32 devices in a mesh: grp: 4 (over y, core), dev: 8 (over z, x).
Axes of the slice: x: 2, y: 2, z: 4, core: 2. Of those that a mesh axis runs over, the one named last changes fastest.
Arguments:
- old_fine: float32 [512, 9, 64, 128], P('dev', None, 'grp'), may hold values from -6 to 6
- old_ids: int32 [4, 512], P('grp', 'dev'), may hold values from -1 to 511, as said below
- old_coarse: float32 [256, 9, 32, 64], P('dev', None, 'grp'), may hold values from -6 to 6
- coarse_ids: int32 [4, 256], P('grp', 'dev'), may hold values from 0 to 255, as said below
- velocity: float32 [512, 3, 64, 128], P('dev', None, 'grp'), may hold values from -0.12 to 0.12
- diffusion: float32 [9], replicated, may hold values from 0.01 to 0.1
Outputs:
- species_out: float32 [512, 9, 64, 128], P('dev', None, 'grp')
The draws below stay inside these ranges and needn't reach their ends.
Inputs may be any that keep to these rules, and one draw needn't show every extreme that they name: `old_ids`: row g names, for each old fine slot k of group g (on dev index k // 64), the x-plane that the slot holds, or -1 for an empty slot whose rows of old_fine are ignored. No plane is named twice; planes named nowhere are newly refined. The slots of one device hold at most 16 planes of any one new box, box e holding planes e * 64 to e * 64 + 63. `coarse_ids`: each row is a permutation. The slots of one device hold at most 8 of the coarse planes e * 32 to e * 32 + 31 of any one new box e.
All inputs are finite; a program needn't handle non-finite values.
Results may differ from the reference program's by a relative error of at most 0.000092.
Values sent between devices are 32-bit elements; how exact they have to be, the bound alone decides.
A program may use at most 192 MiB of HBM per device.

```python
import math
import jax
import jax.numpy as jnp

S = 9
BX = 64
BY = 16
BZ = 128
ITERS = 2
CAP = 16
CBX = 32
CCAP = 8
NX = 512
NY = 64
CX = 256
CY = 32
CZ = 64
N_GRP = 4
N_DEV = 8


def regrid_map(key, block_len, capacity, with_empty):
    rows_out = []
    for group_index in range(N_GRP):
        group_key = jax.random.fold_in(key, group_index)
        key_order = jax.random.fold_in(group_key, 1)
        key_offset = jax.random.fold_in(group_key, 2)
        key_slots = jax.random.fold_in(group_key, 3)
        key_level = jax.random.fold_in(group_key, 4)
        key_rolls = jax.random.fold_in(group_key, 5)
        placing = jax.random.permutation(key_order, N_DEV)
        shuffled = jax.random.permutation(key_offset, capacity * N_DEV) // capacity
        first_value = shuffled[0]
        scores = jnp.where(shuffled == first_value, 1, 0).astype(jnp.int32)
        reorder = jnp.argsort(scores, stable=True)
        rest_values = shuffled[reorder][:block_len - capacity]
        offsets = jnp.concatenate([jnp.full((capacity,), first_value, jnp.int32), rest_values.astype(jnp.int32)])
        slot_order = jax.random.permutation(key_slots, block_len)
        boxes = jnp.arange(N_DEV, dtype=jnp.int32)[:, None]
        planes = jnp.arange(block_len, dtype=jnp.int32)[None, :]
        holder = (placing[:, None] + offsets[None, :]) % N_DEV
        positions = holder * block_len + slot_order[None, :]
        values = boxes * block_len + planes
        if with_empty:
            levels = jax.random.randint(key_level, (N_DEV,), 0, 5)
            rolls = jax.random.randint(key_rolls, (N_DEV, block_len), 0, 8)
            fresh_mask = (rolls < levels[:, None]) & jnp.logical_not((boxes == 0) & (planes < capacity))
            values = jnp.where(fresh_mask, -1, values)
        row_values = jnp.zeros((N_DEV * block_len,), jnp.int32).at[positions.reshape(-1)].set(values.reshape(-1).astype(jnp.int32))
        rows_out.append(row_values)
    return jnp.stack(rows_out, axis=0)


def draw_old_ids(key, part):
    return regrid_map(jax.random.fold_in(key, 11), BX, CAP, True)


def draw_coarse_ids(key, part):
    return regrid_map(jax.random.fold_in(key, 23), CBX, CCAP, False)


def level_of(stream_key, shape, split, smallest, high):
    loudness, own = 1.0, jax.random.fold_in(stream_key, 6)
    for axis_at, parts in split:
        heights = jnp.exp(jax.random.uniform(jax.random.fold_in(own, axis_at), (parts,), jnp.float32, smallest / len(split), high / len(split)))
        loudness = loudness * jnp.repeat(heights, shape[axis_at] // parts).reshape([-1 if axis == axis_at else 1 for axis in range(len(shape))])
    return loudness


def gaussian(own_key, dims, spread, reach, cuts=(), kind=jnp.bfloat16):
    loudness = level_of(own_key, dims, cuts, -0.22, 0.18) if cuts else 1.0
    array = jax.random.normal(own_key, dims, jnp.float32) * spread * loudness
    return jnp.minimum(jnp.maximum(array, -reach), reach).astype(kind)


def setup_inputs(seed: int = 0) -> dict:
    arg_keys = jax.random.split(jax.random.key(seed), 7)
    old_fine = gaussian(arg_keys[0], (NX, S, NY, BZ), 1.0, 6.0, ((0, 8), (2, 4)), jnp.float32)
    old_ids = draw_old_ids(jax.random.fold_in(arg_keys[6], 71), 0)
    old_coarse = gaussian(arg_keys[2], (CX, S, CY, CZ), 1.0, 6.0, ((0, 8), (2, 4)), jnp.float32)
    coarse_ids = draw_coarse_ids(jax.random.fold_in(arg_keys[6], 71), 0)
    velocity = gaussian(arg_keys[4], (NX, 3, NY, BZ), 0.045, 0.12, ((0, 8), (2, 4)), jnp.float32)
    diffusion = jnp.clip(jnp.exp(jax.random.uniform(arg_keys[5], (S,), jnp.float32, math.log(0.01), math.log(0.1))), 0.01, 0.1)
    return dict(old_fine=old_fine, old_ids=old_ids, old_coarse=old_coarse, coarse_ids=coarse_ids, velocity=velocity, diffusion=diffusion)


def refine(coarse):
    extent = coarse.shape
    ypadded = jnp.concatenate([coarse[:, :, :1], coarse, coarse[:, :, -1:]], axis=2)
    zpadded = jnp.concatenate([coarse[..., :1], coarse, coarse[..., -1:]], axis=3)
    slope_y = 0.5 * (ypadded[:, :, 2:] - ypadded[:, :, :-2])
    slope_z = 0.5 * (zpadded[..., 2:] - zpadded[..., :-2])
    row_parts = []
    for row_half in range(2):
        col_parts = [coarse + (0.5 * row_half - 0.25) * slope_y + (0.5 * col_half - 0.25) * slope_z for col_half in range(2)]
        row_parts.append(jnp.stack(col_parts, axis=-1))
    children = jnp.stack(row_parts, axis=3)
    refined = children.reshape(extent[0], extent[1], 2 * extent[2], 2 * extent[3])
    return jnp.repeat(refined, 2, axis=0)


def advance(padded, flow_field, diffusion):
    center = padded[1:-1, :, 1:-1]
    zpadded = jnp.concatenate([center[..., :1], center, center[..., -1:]], axis=3)
    minus_side = [padded[:-2, :, 1:-1], padded[1:-1, :, :-2], zpadded[..., :-2]]
    plus_side = [padded[2:, :, 1:-1], padded[1:-1, :, 2:], zpadded[..., 2:]]
    laplace = minus_side[0] + plus_side[0] + minus_side[1] + plus_side[1] + minus_side[2] + plus_side[2] - 6.0 * center
    transport = jnp.zeros_like(center)
    for direction in range(3):
        speed_part = flow_field[:, direction:direction + 1]
        transport = transport + jnp.maximum(speed_part, 0.0) * (center - minus_side[direction]) + jnp.minimum(speed_part, 0.0) * (plus_side[direction] - center)
    return center + diffusion[None, :, None, None] * laplace - transport


def reference(old_fine, old_ids, old_coarse, coarse_ids, velocity, diffusion):
    pieces = []
    half_rows = BY // 2
    for group_index in range(N_GRP):
        labels = old_ids[group_index]
        target = jnp.where(labels >= 0, labels, NX).astype(jnp.int32)
        source = jnp.full((NX,), -1, jnp.int32).at[target].set(jnp.arange(NX, dtype=jnp.int32), mode="drop")
        moved_rows = old_fine[jnp.maximum(source, 0).astype(jnp.int32), :, group_index * BY:(group_index + 1) * BY]
        coarse_source = jnp.zeros((CX,), jnp.int32).at[coarse_ids[group_index].astype(jnp.int32)].set(jnp.arange(CX, dtype=jnp.int32))
        parents = old_coarse[coarse_source, :, group_index * half_rows:(group_index + 1) * half_rows]
        interp = refine(parents)
        pieces.append(jnp.where((source < 0)[:, None, None, None], interp, moved_rows))
    species_state = jnp.concatenate(pieces, axis=2)
    for repeat in range(ITERS):
        padded = jnp.pad(species_state, ((1, 1), (0, 0), (1, 1), (0, 0)))
        species_state = advance(padded, velocity, diffusion)
    return species_state
```

```python
import functools

import jax
import jax.numpy as jnp
from jax import lax
from jax.experimental import pallas as pl
from jax.experimental.pallas import tpu as pltpu
from jax.sharding import PartitionSpec as P

CROSS = (8, 9, 10)
VMEM_LIMIT = 48 * 1024 * 1024
MESH = pl.DeviceIdType.MESH


def params(**more):
    return pltpu.CompilerParams(vmem_limit_bytes=VMEM_LIMIT, **more)


def earlier_count(mask):
    count = mask.shape[-1]
    lower = jnp.arange(count)[None, :] < jnp.arange(count)[:, None]
    return jnp.sum((mask[..., None, :] & lower).astype(jnp.int32), axis=-1)


def send_table(labels, block_len, devices, capacity):
    target = jnp.where(labels >= 0, labels // block_len, -1)
    count = labels.shape[0]
    same = target[None, :] == target[:, None]
    lower = jnp.arange(count)[None, :] < jnp.arange(count)[:, None]
    rank = jnp.sum((same & lower).astype(jnp.int32), axis=1)
    slot = jnp.where(labels >= 0, target * capacity + rank, -1)
    hits = slot[None, :] == jnp.arange(devices * capacity)[:, None]
    return jnp.max(jnp.where(hits, jnp.arange(count)[None, :], 0), axis=1)


def receive_table(labels_all, block_len, capacity, me):
    devices, count = labels_all.shape
    within = labels_all - me * block_len
    valid = (within >= 0) & (within < block_len)
    slot = jnp.arange(devices)[:, None] * capacity + earlier_count(valid)
    flat_within = jnp.where(valid, within, -1).reshape(-1)
    hits = flat_within[None, :] == jnp.arange(block_len)[:, None]
    return jnp.max(jnp.where(hits, slot.reshape(-1)[None, :], -1), axis=1)


def pair_count(same):
    count = same.shape[-1]
    lower = jnp.arange(count)[None, :] < jnp.arange(count)[:, None]
    return jnp.sum((same & lower).astype(jnp.int32), axis=-1)


def slot_caps(devices, cross, inner):
    half = jnp.arange(devices) // (devices // 2)
    return jnp.where(half[:, None] != half[None, :], cross, inner)


def cross_need(labels, block_len):
    devices = labels.shape[0]
    part = devices // 2
    half = jnp.where(labels >= 0, labels // block_len // part, -1)
    away = 1 - jnp.arange(devices) // part
    load = jnp.sum((half == away[:, None]).astype(jnp.int32), axis=1)
    return jnp.max((load + part - 1) // part)


def exchange_plan(labels, block_len, stride, caps, second_cap):
    devices = labels.shape[0]
    part = devices // 2
    owners = jnp.arange(devices)
    valid = labels >= 0
    owner = jnp.where(valid, labels // block_len, -1)
    rank = pair_count(owner[:, None, :] == owner[:, :, None])
    mine = owner[:, :, None] == owners
    limit = jnp.sum(jnp.where(mine, caps[:, None, :], 0), axis=-1)
    over = valid & (rank >= limit)
    half = owner // part
    order = pair_count(over[:, None, :] & (half[:, None, :] == half[:, :, None]))
    counts = jnp.sum(mine.astype(jnp.int32), axis=1)
    spot = jnp.arange(stride)
    free = ((spot >= counts[:, :, None]) & (spot < caps[:, :, None])).astype(jnp.int32)
    by_half = free.reshape(devices, 2, part, stride)
    level = jnp.sum(by_half, axis=2)
    higher = jnp.sum(jnp.where(spot[None, :] > spot[:, None], level[:, :, None, :], 0), axis=-1)
    member = jnp.arange(part)
    beside = jnp.sum(
        jnp.where((member[None, :] < member[:, None])[:, :, None], by_half[:, :, None], 0), axis=3
    )
    at = jnp.where(by_half > 0, higher[:, :, None, :] + beside, -1)
    at = at.reshape(devices, 1, devices * stride)
    spots = jnp.arange(devices * stride)
    match = (at == order[:, :, None]) & ((spots // stride) // part == half[:, :, None])
    borrowed = jnp.max(jnp.where(match, spots, -1), axis=-1)
    slot = jnp.where(valid, jnp.where(over, borrowed, owner * stride + rank), -1)
    via = slot // stride
    relayed = over & (via != owner)
    lane = jnp.where(relayed, via * part + owner % part, -1)
    within = pair_count(lane[:, None, :] == lane[:, :, None])
    lanes = jnp.arange(devices * part)
    per_source = jnp.sum((lane[:, :, None] == lanes).astype(jnp.int32), axis=1)
    ahead = jnp.sum(
        jnp.where((owners[None, :] < owners[:, None])[:, :, None], per_source[None], 0), axis=1
    )
    second = within + jnp.sum(jnp.where(lane[:, :, None] == lanes, ahead[:, None, :], 0), axis=-1)
    fits = jnp.all(jnp.where(over, borrowed >= 0, True))
    fits = fits & jnp.all(jnp.sum(per_source, axis=0) <= second_cap)
    return owner, slot, relayed, second, fits


def block_of(here, there, part):
    turn = (there - here) % part
    return jnp.where(here // part != there // part, turn, part + turn)


def plan_tables(labels, plan, block_len, stride, second_cap, me):
    owner, slot, relayed, second = plan
    devices, count = labels.shape
    part = devices // 2
    via, spot = slot // stride, slot % stride
    source = jnp.arange(devices)[:, None]
    mine = jnp.where(source == me, slot, -1)
    mine = jnp.where(mine >= 0, block_of(me, via, part) * stride + spot, -1)
    mine = jnp.max(mine, axis=0)
    spots = jnp.arange(devices * stride)
    send = jnp.max(jnp.where(mine[None] == spots[:, None], jnp.arange(count)[None], 0), axis=1)
    arrive = block_of(source, me, part) * stride + spot
    lane = (owner - me) % part - 1
    handed = jnp.where(relayed & (via == me), lane * second_cap + second, -1).reshape(-1)
    hops = jnp.arange((part - 1) * second_cap)
    relay = jnp.max(
        jnp.where(handed[None] == hops[:, None], arrive.reshape(-1)[None], 0), axis=1
    )
    indirect = devices * stride + ((me - via) % part - 1) * second_cap + second
    where = jnp.where(relayed, indirect, arrive).reshape(-1)
    inside = jnp.where(owner == me, labels - me * block_len, -1).reshape(-1)
    hits = inside[None] == jnp.arange(block_len)[:, None]
    return send, relay, jnp.max(jnp.where(hits, where[None], -1), axis=1)


def pack_fine_kernel(table, source, out, sem):
    def send(i, carry):
        pltpu.make_async_copy(source.at[table[i]], out.at[i], sem).start()
        return carry

    lax.fori_loop(0, out.shape[0], send, 0)
    pltpu.make_async_copy(out, out, sem).wait()


def pack_fine(table, fine):
    return pl.pallas_call(
        pack_fine_kernel,
        out_shape=jax.ShapeDtypeStruct((table.shape[0],) + fine.shape[1:], fine.dtype),
        in_specs=[
            pl.BlockSpec(memory_space=pltpu.SMEM),
            pl.BlockSpec(memory_space=pltpu.VMEM),
        ],
        out_specs=pl.BlockSpec(memory_space=pl.ANY),
        scratch_shapes=[pltpu.SemaphoreType.DMA],
        compiler_params=params(),
        name="pack_fine",
    )(table, fine)


def pack_coarse_kernel(table, source, out):
    half = source.shape[-1]

    def step(i, carry):
        out[i, :, :, 0:half] = source[table[2 * i]]
        out[i, :, :, half : 2 * half] = source[table[2 * i + 1]]
        return carry

    lax.fori_loop(0, out.shape[0], step, 0)


def pack_coarse(table, coarse):
    shape = (table.shape[0] // 2,) + coarse.shape[1:3] + (2 * coarse.shape[3],)
    return pl.pallas_call(
        pack_coarse_kernel,
        out_shape=jax.ShapeDtypeStruct(shape, coarse.dtype),
        in_specs=[
            pl.BlockSpec(memory_space=pltpu.SMEM),
            pl.BlockSpec(memory_space=pltpu.VMEM),
        ],
        out_specs=pl.BlockSpec(memory_space=pltpu.VMEM),
        compiler_params=params(),
        name="pack_coarse",
    )(table, coarse)


def refine_into(table, pairs, weights, out, offset, count):
    species, rows, depth = pairs.shape[1:]
    half = depth // 2
    lane = lax.broadcasted_iota(jnp.int32, (species * rows, depth), 1)
    row = lax.broadcasted_iota(jnp.int32, (species, rows, depth), 1)

    def step(c, carry):
        slot = jnp.maximum(table[c], 0)
        block = pairs[slot // 2].reshape(species * rows, depth)
        odd = slot % 2
        block = jnp.where((lane >= half).astype(jnp.int32) == odd, block, 0.0)
        spread = jnp.dot(
            block, weights[...], precision=lax.Precision.HIGHEST,
            preferred_element_type=jnp.float32,
        )
        plain = spread[:, :depth].reshape(species, rows, depth)
        sloped = spread[:, depth:].reshape(species, rows, depth)
        below = jnp.where(row == 0, plain, pltpu.roll(plain, 1, 1))
        above = jnp.where(row == rows - 1, plain, pltpu.roll(plain, rows - 1, 1))
        slope = 0.125 * (above - below)
        for s in range(species):
            out[offset + c, s, pl.ds(0, rows, 2), :] = sloped[s] - slope[s]
            out[offset + c, s, pl.ds(1, rows, 2), :] = sloped[s] + slope[s]
        return carry

    lax.fori_loop(0, count, step, 0)


def refine_kernel(table, pairs, weights, out):
    refine_into(table, pairs, weights, out, 0, out.shape[0])


def spread_weights(half):
    depth = 2 * half
    coarse = jnp.arange(half)[:, None]
    fine = jnp.arange(depth)[None, :]
    centre = (fine // 2 == coarse).astype(jnp.float32)
    up = (jnp.minimum(fine // 2 + 1, half - 1) == coarse).astype(jnp.float32)
    down = (jnp.maximum(fine // 2 - 1, 0) == coarse).astype(jnp.float32)
    side = jnp.where(fine % 2 == 1, 0.125, -0.125)
    both = jnp.concatenate([centre, centre + side * (up - down)], axis=1)
    return jnp.concatenate([both, both], axis=0)


def refine(table, pairs, weights):
    species, rows, depth = pairs.shape[1:]
    return pl.pallas_call(
        refine_kernel,
        out_shape=jax.ShapeDtypeStruct(
            (table.shape[0], species, 2 * rows, depth), pairs.dtype
        ),
        in_specs=[
            pl.BlockSpec(memory_space=pltpu.SMEM),
            pl.BlockSpec(memory_space=pltpu.VMEM),
            pl.BlockSpec(memory_space=pltpu.VMEM),
        ],
        out_specs=pl.BlockSpec(memory_space=pltpu.VMEM),
        compiler_params=params(),
        cost_estimate=pl.CostEstimate(
            flops=40_000_000, bytes_accessed=30_000_000, transcendentals=0
        ),
        name="refine",
    )(table, pairs, weights)


def assemble_kernel(table, arrived, interp, out, sem):
    def fetch(p, carry):
        slot = table[p]

        @pl.when(slot >= 0)
        def _():
            pltpu.make_async_copy(arrived.at[slot], out.at[p], sem).start()

        @pl.when(slot < 0)
        def _():
            pltpu.make_async_copy(interp.at[p // 2], out.at[p], sem).start()

        return carry

    lax.fori_loop(0, out.shape[0], fetch, 0)
    pltpu.make_async_copy(out, out, sem).wait()


def assemble(table, arrived, interp):
    return pl.pallas_call(
        assemble_kernel,
        out_shape=jax.ShapeDtypeStruct((table.shape[0],) + arrived.shape[1:], arrived.dtype),
        in_specs=[
            pl.BlockSpec(memory_space=pltpu.SMEM),
            pl.BlockSpec(memory_space=pl.ANY),
            pl.BlockSpec(memory_space=pl.ANY),
        ],
        out_specs=pl.BlockSpec(memory_space=pltpu.VMEM),
        scratch_shapes=[pltpu.SemaphoreType.DMA],
        compiler_params=params(),
        name="assemble",
    )(table, arrived, interp)


def gather_kernel(groups, devices, mine, out, send_sems, recv_sems):
    total = groups * devices
    me = lax.axis_index("grp") * devices + lax.axis_index("dev")
    barrier = pltpu.get_barrier_semaphore()

    def place(k):
        to = lax.rem(me + k, total)
        return {"grp": to // devices, "dev": lax.rem(to, devices)}

    def greet(k, carry):
        pl.semaphore_signal(barrier, inc=1, device_id=place(k), device_id_type=MESH)
        return carry

    lax.fori_loop(1, total, greet, 0)
    pl.semaphore_wait(barrier, total - 1)

    def copy(k):
        return pltpu.make_async_remote_copy(
            src_ref=mine,
            dst_ref=out.at[me],
            send_sem=send_sems.at[k],
            recv_sem=recv_sems.at[k],
            device_id=place(k),
            device_id_type=MESH,
        )

    def start(k, carry):
        copy(k).start()
        return carry

    def finish(k, carry):
        copy(k).wait_send()
        source = lax.rem(me + total - k, total)
        pltpu.make_async_remote_copy(
            src_ref=mine,
            dst_ref=out.at[source],
            send_sem=send_sems.at[k],
            recv_sem=recv_sems.at[k],
            device_id=place(k),
            device_id_type=MESH,
        ).wait_recv()
        return carry

    lax.fori_loop(1, total, start, 0)
    out[me] = mine[...]
    lax.fori_loop(1, total, finish, 0)


def gather_ids(both, groups, devices):
    width = both.shape[0]
    padded = -(-width // 128) * 128
    mine = jnp.pad(both, (0, padded - width))[None]
    total = groups * devices
    out = pl.pallas_call(
        functools.partial(gather_kernel, groups, devices),
        out_shape=jax.ShapeDtypeStruct((total, 1, padded), both.dtype),
        in_specs=[pl.BlockSpec(memory_space=pltpu.VMEM)],
        out_specs=pl.BlockSpec(memory_space=pltpu.VMEM),
        scratch_shapes=[
            pltpu.SemaphoreType.DMA((total,)),
            pltpu.SemaphoreType.DMA((total,)),
        ],
        compiler_params=pltpu.CompilerParams(collective_id=0, has_side_effects=True),
        name="gather_ids",
    )(mine)
    return out.reshape(groups, devices, padded)[:, :, :width]


def coefficients(flow, x):
    v = [flow[x, k] for k in range(3)]
    plus = [jnp.maximum(w, 0.0) for w in v]
    minus = [jnp.maximum(-w, 0.0) for w in v]
    rest = 1.0
    for k in range(3):
        rest = rest - plus[k] - minus[k]
    return plus, minus, rest


def update(d, coeffs, c, lo, hi, below, above, row, lane):
    rows, depth = c.shape
    plus, minus, rest = coeffs
    ylo = jnp.where(row == 0, below, pltpu.roll(c, 1, 0))
    yhi = jnp.where(row == rows - 1, above, pltpu.roll(c, rows - 1, 0))
    zlo = jnp.where(lane == 0, c, pltpu.roll(c, 1, 1))
    zhi = jnp.where(lane == depth - 1, c, pltpu.roll(c, depth - 1, 1))
    total = (rest - 6.0 * d) * c
    total = total + (plus[0] + d) * lo + (minus[0] + d) * hi
    total = total + (plus[1] + d) * ylo + (minus[1] + d) * yhi
    return total + (plus[2] + d) * zlo + (minus[2] + d) * zhi


def regrid_kernel(
    cross, inner, stride, hops,
    send_table, relay_table, final_table, coarse_table, diffusion,
    fine, pairs, weights, flow,
    out, first_out, last_out, below_out, above_out,
    send, pool, handed, passed_in, state, low, high, below, above,
    low_next, high_next, below_next, above_next, first_next, last_next,
    send_sems, recv_sems, relay_send, relay_recv, edge_send, edge_recv, row_send, row_recv,
):
    planes, species, rows, depth = fine.shape
    groups, devices = lax.axis_size("grp"), lax.axis_size("dev")
    part = devices // 2
    g, me = lax.axis_index("grp"), lax.axis_index("dev")
    base = (me // part) * part
    other = part - base
    spot = lax.rem(me, part)
    barrier = pltpu.get_barrier_semaphore()

    def across(k):
        return {"dev": other + lax.rem(spot + k, part)}

    def within(k):
        return {"dev": base + lax.rem(spot + k, part)}

    def greet(to):
        pl.semaphore_signal(barrier, inc=1, device_id=to, device_id_type=MESH)

    for k in range(part):
        greet(across(k))
    for k in range(1, part):
        greet(within(k))
    greet({"grp": lax.rem(g + 1, groups)})
    greet({"grp": lax.rem(g + groups - 1, groups)})
    pl.semaphore_wait(barrier, devices + 1)

    def pack(block, count, into, offset):
        def step(k, carry):
            into[offset + k] = fine[send_table[block * stride + k]]
            return carry

        lax.fori_loop(0, count, step, 0)

    def block_copy(block, count, to):
        at = pl.ds(block * stride, count)
        return pltpu.make_async_remote_copy(
            src_ref=send.at[at],
            dst_ref=pool.at[at],
            send_sem=send_sems.at[block],
            recv_sem=recv_sems.at[block],
            device_id=to,
            device_id_type=MESH,
        )

    moves = []
    for k in range(part):
        pack(k, cross, send, k * stride)
        moves.append(block_copy(k, cross, across(k)))
        moves[-1].start()
    for k in range(1, part):
        pack(part + k, inner, send, (part + k) * stride)
        moves.append(block_copy(part + k, inner, within(k)))
        moves[-1].start()
    pack(part, inner, pool, part * stride)

    arrivals = devices * stride
    passed = (part - 1) * hops
    fill = arrivals + passed
    refine_into(coarse_table, pairs, weights, pool, fill, coarse_table.shape[0])

    for move in moves:
        move.wait_recv()

    def relay(k, carry):
        handed[k] = pool[relay_table[k]]
        return carry

    lax.fori_loop(0, passed, relay, 0)
    relays = []
    for k in range(1, part):
        relays.append(
            pltpu.make_async_remote_copy(
                src_ref=handed.at[pl.ds((k - 1) * hops, hops)],
                dst_ref=passed_in.at[pl.ds((k - 1) * hops, hops)],
                send_sem=relay_send.at[k],
                recv_sem=relay_recv.at[k],
                device_id=within(k),
                device_id_type=MESH,
            )
        )
        relays[-1].start()
    for move in relays:
        move.wait_recv()

    def settle_relay(k, carry):
        pool[arrivals + k] = passed_in[k]
        return carry

    lax.fori_loop(0, passed, settle_relay, 0)

    def assemble(p, carry):
        at = final_table[p]
        for s in range(species):
            value = pool[at, s]
            state[p + 1, s] = value
            low[s, pl.ds(p, 1), :] = value[0:1]
            high[s, pl.ds(p, 1), :] = value[rows - 1 : rows]
        return carry

    lax.fori_loop(0, planes, assemble, 0)

    def edge_copy(source, target, at, to):
        return pltpu.make_async_remote_copy(
            src_ref=source,
            dst_ref=target,
            send_sem=edge_send.at[at],
            recv_sem=edge_recv.at[at],
            device_id=to,
            device_id_type=MESH,
        )

    def row_copy(source, target, b, at, to):
        cut = pl.ds(pl.multiple_of(b * 8, 8), 8)
        return pltpu.make_async_remote_copy(
            src_ref=source.at[:, cut],
            dst_ref=target.at[:, cut],
            send_sem=row_send.at[at, b],
            recv_sem=row_recv.at[at, b],
            device_id=to,
            device_id_type=MESH,
        )

    left, right = {"dev": me - 1}, {"dev": me + 1}
    down, up = {"grp": g - 1}, {"grp": g + 1}
    ahead = edge_copy(state.at[pl.ds(planes, 1)], state.at[pl.ds(0, 1)], 0, right)
    back = edge_copy(state.at[pl.ds(1, 1)], state.at[pl.ds(planes + 1, 1)], 1, left)
    rise = edge_copy(high, below, 2, up)
    sink = edge_copy(low, above, 3, down)
    has_left, has_right = me > 0, me < devices - 1
    has_down, has_up = g > 0, g < groups - 1

    @pl.when(has_up)
    def _():
        rise.start()

    @pl.when(has_down)
    def _():
        sink.start()

    @pl.when(has_right)
    def _():
        ahead.start()

    @pl.when(has_left)
    def _():
        back.start()

    for move in moves + relays:
        move.wait_send()

    @pl.when(has_left)
    def _():
        ahead.wait_recv()

    @pl.when(has_right)
    def _():
        back.wait_recv()

    @pl.when(has_down)
    def _():
        rise.wait_recv()

    @pl.when(has_up)
    def _():
        sink.wait_recv()

    @pl.when(has_right)
    def _():
        ahead.wait_send()

    @pl.when(has_left)
    def _():
        back.wait_send()

    @pl.when(has_up)
    def _():
        rise.wait_send()

    @pl.when(has_down)
    def _():
        sink.wait_send()

    @pl.when(me == 0)
    def _():
        state[0] = jnp.zeros(state.shape[1:], state.dtype)

    @pl.when(me == devices - 1)
    def _():
        state[planes + 1] = jnp.zeros(state.shape[1:], state.dtype)

    @pl.when(g == 0)
    def _():
        below[...] = jnp.zeros(below.shape, below.dtype)

    @pl.when(g == groups - 1)
    def _():
        above[...] = jnp.zeros(above.shape, above.dtype)

    row = lax.broadcasted_iota(jnp.int32, (rows, depth), 0)
    lane = lax.broadcasted_iota(jnp.int32, (rows, depth), 1)


    next_ahead = edge_copy(out.at[pl.ds(planes - 1, 1)], first_next, 4, right)
    next_back = edge_copy(out.at[pl.ds(0, 1)], last_next, 5, left)
    blocks = planes // 8

    def advance_block(turn, carry):
        b = lax.rem(turn + blocks - 1, blocks)

        def advance_plane(k, carry):
            p = b * 8 + k
            coeffs = coefficients(flow, p)
            for s in range(species):
                total = update(
                    diffusion[s], coeffs, state[p + 1, s], state[p, s], state[p + 2, s],
                    below[s, pl.ds(p, 1), :], above[s, pl.ds(p, 1), :], row, lane,
                )
                out[p, s] = total
                low_next[s, pl.ds(p, 1), :] = total[0:1]
                high_next[s, pl.ds(p, 1), :] = total[rows - 1 : rows]
            return carry

        lax.fori_loop(0, 8, advance_plane, 0)

        @pl.when(has_up)
        def _():
            row_copy(high_next, below_next, b, 0, up).start()

        @pl.when(has_down)
        def _():
            row_copy(low_next, above_next, b, 1, down).start()

        @pl.when((turn == 0) & has_right)
        def _():
            next_ahead.start()

        @pl.when((turn == 1) & has_left)
        def _():
            next_back.start()

        return carry

    lax.fori_loop(0, blocks, advance_block, 0)

    def settle(b, carry):
        @pl.when(has_down)
        def _():
            row_copy(high_next, below_next, b, 0, up).wait_recv()
            row_copy(low_next, above_next, b, 1, down).wait_send()

        @pl.when(has_up)
        def _():
            row_copy(low_next, above_next, b, 1, down).wait_recv()
            row_copy(high_next, below_next, b, 0, up).wait_send()

        return carry

    lax.fori_loop(0, blocks, settle, 0)

    @pl.when(has_left)
    def _():
        next_ahead.wait_recv()
        next_back.wait_send()
        first_out[...] = first_next[...]

    @pl.when(has_right)
    def _():
        next_back.wait_recv()
        next_ahead.wait_send()
        last_out[...] = last_next[...]

    @pl.when(has_down)
    def _():
        below_out[...] = below_next[...]

    @pl.when(has_up)
    def _():
        above_out[...] = above_next[...]

    @pl.when(me == 0)
    def _():
        first_out[...] = jnp.zeros(first_out.shape, first_out.dtype)

    @pl.when(me == devices - 1)
    def _():
        last_out[...] = jnp.zeros(last_out.shape, last_out.dtype)

    @pl.when(g == 0)
    def _():
        below_out[...] = jnp.zeros(below_out.shape, below_out.dtype)

    @pl.when(g == groups - 1)
    def _():
        above_out[...] = jnp.zeros(above_out.shape, above_out.dtype)


def regrid(cross, inner, stride, hops, ident, devices, tables, diffusion, fine, pairs, weights, flow):
    planes, species, rows, depth = fine.shape
    part = devices // 2
    kept = jax.ShapeDtypeStruct(fine.shape, fine.dtype)
    plane = jax.ShapeDtypeStruct((1,) + fine.shape[1:], fine.dtype)
    edge = jax.ShapeDtypeStruct((species, planes, depth), fine.dtype)
    pool = devices * stride + (part - 1) * hops + planes // 2
    vmem = pl.BlockSpec(memory_space=pltpu.VMEM)
    smem = pl.BlockSpec(memory_space=pltpu.SMEM)

    def held(count):
        return pltpu.VMEM((count,) + fine.shape[1:], fine.dtype)

    rim = pltpu.VMEM(edge.shape, edge.dtype)
    return pl.pallas_call(
        functools.partial(regrid_kernel, cross, inner, stride, hops),
        out_shape=(kept, plane, plane, edge, edge),
        in_specs=[smem] * 5 + [vmem] * 4,
        out_specs=(vmem,) * 5,
        scratch_shapes=[
            held(devices * stride), held(pool), held((part - 1) * hops), held((part - 1) * hops),
            held(planes + 2),
            rim, rim, rim, rim, rim, rim, rim, rim, held(1), held(1),
            pltpu.SemaphoreType.DMA((devices,)),
            pltpu.SemaphoreType.DMA((devices,)),
            pltpu.SemaphoreType.DMA((part,)),
            pltpu.SemaphoreType.DMA((part,)),
            pltpu.SemaphoreType.DMA((6,)),
            pltpu.SemaphoreType.DMA((6,)),
            pltpu.SemaphoreType.DMA((2, planes // 8)),
            pltpu.SemaphoreType.DMA((2, planes // 8)),
        ],
        compiler_params=params(collective_id=ident, has_side_effects=True),
        name="regrid",
    )(*tables, diffusion, fine, pairs, weights, flow)


def advance_kernel(steps, diffusion, u, before, after, first, last, below, above, flow, out):
    i = pl.program_id(0)
    block, species, rows, depth = u.shape
    row = lax.broadcasted_iota(jnp.int32, (rows, depth), 0)
    lane = lax.broadcasted_iota(jnp.int32, (rows, depth), 1)
    for x in range(block):
        coeffs = coefficients(flow, x)
        for s in range(species):
            if x > 0:
                lo = u[x - 1, s]
            else:
                lo = jnp.where(i == 0, first[0, s], before[0, s])
            if x < block - 1:
                hi = u[x + 1, s]
            else:
                hi = jnp.where(i == steps - 1, last[0, s], after[0, s])
            out[x, s] = update(
                diffusion[s], coeffs, u[x, s], lo, hi,
                below[s, pl.ds(x, 1), :], above[s, pl.ds(x, 1), :], row, lane,
            )


def advance(diffusion, u, first, last, below, above, flow):
    planes, species, rows, depth = u.shape
    block = 8 if planes % 8 == 0 else planes
    steps = planes // block
    edge_spec = pl.BlockSpec((species, block, depth), lambda i: (0, i, 0))
    plane_spec = pl.BlockSpec((1, species, rows, depth), lambda i: (0, 0, 0, 0))
    block_spec = pl.BlockSpec((block, species, rows, depth), lambda i: (i, 0, 0, 0))
    return pl.pallas_call(
        functools.partial(advance_kernel, steps),
        grid=(steps,),
        out_shape=jax.ShapeDtypeStruct(u.shape, u.dtype),
        in_specs=[
            pl.BlockSpec(memory_space=pltpu.SMEM),
            block_spec,
            pl.BlockSpec(
                (1, species, rows, depth), lambda i: (jnp.maximum(i * block - 1, 0), 0, 0, 0)
            ),
            pl.BlockSpec(
                (1, species, rows, depth),
                lambda i: (jnp.minimum(i * block + block, planes - 1), 0, 0, 0),
            ),
            plane_spec,
            plane_spec,
            edge_spec,
            edge_spec,
            pl.BlockSpec((block, 3, rows, depth), lambda i: (i, 0, 0, 0)),
        ],
        out_specs=block_spec,
        compiler_params=params(),
        name="advance",
    )(diffusion, u, u, u, first, last, below, above, flow)


def shift_up(value, axis):
    size = lax.axis_size(axis)
    return lax.ppermute(value, axis, [(i, i + 1) for i in range(size - 1)])


def shift_down(value, axis):
    size = lax.axis_size(axis)
    return lax.ppermute(value, axis, [(i + 1, i) for i in range(size - 1)])


def rims(u):
    rows = u.shape[2]
    below = shift_up(jnp.swapaxes(u[:, :, rows - 1], 0, 1), "grp")
    above = shift_down(jnp.swapaxes(u[:, :, 0], 0, 1), "grp")
    return shift_up(u[-1:], "dev"), shift_down(u[:1], "dev"), below, above


def on_device(old_fine, old_ids, old_coarse, coarse_ids, velocity, diffusion):
    devices = lax.axis_size("dev")
    group_count = lax.axis_size("grp")
    me = lax.axis_index("dev")
    planes = old_fine.shape[0]
    coarse_planes = old_coarse.shape[0]
    capacity = max(2, 2 * planes // devices)
    coarse_capacity = max(2, 2 * coarse_planes // devices)
    both = jnp.concatenate([old_ids[0], coarse_ids[0]])
    relaying = capacity >= 16 and devices % 2 == 0 and planes % 8 == 0 and group_count > 2
    if relaying:
        groups = gather_ids(both, group_count, devices)
    else:
        groups = lax.all_gather(both, ("grp", "dev")).reshape(group_count, devices, -1)
    here = (jnp.arange(group_count) == lax.axis_index("grp"))[:, None, None]
    both_all = jnp.max(jnp.where(here, groups, -1), axis=0)
    labels = both_all[:, :planes]
    own = jnp.max(jnp.where((jnp.arange(devices) == me)[:, None], both_all, -1), axis=0)
    coarse_send = send_table(own[planes:], coarse_planes, devices, coarse_capacity)
    coarse_table = receive_table(both_all[:, planes:], coarse_planes, coarse_capacity, me)
    weights = spread_weights(old_coarse.shape[3])
    coarse_out = pack_coarse(coarse_send, old_coarse)
    coarse_in = lax.all_to_all(coarse_out, "dev", split_axis=0, concat_axis=0, tiled=True)

    def padded(fine, coarse):
        send = send_table(own[:planes], planes, devices, capacity)
        table = receive_table(labels, planes, capacity, me)
        arrived = lax.all_to_all(pack_fine(send, fine), "dev", split_axis=0, concat_axis=0, tiled=True)
        interp = refine(coarse_table, coarse, weights)
        u = assemble(table, arrived, interp)
        u = advance(diffusion, u, *rims(u), velocity)
        return (u,) + rims(u)

    if relaying:
        choices = [capacity * k // 16 for k in CROSS]
        inner, stride, hops = 11 * capacity // 16, 11 * capacity // 16, capacity // 4
        need = jnp.max(jax.vmap(functools.partial(cross_need, block_len=planes))(groups[:, :, :planes]))
        pick = jnp.sum((need > jnp.array(choices)).astype(jnp.int32))
        cross = jnp.sum(jnp.where(jnp.arange(len(choices)) == pick, jnp.array(choices), 0))
        caps = slot_caps(devices, cross, inner)
        plan = functools.partial(
            exchange_plan, block_len=planes, stride=stride, caps=caps, second_cap=hops
        )
        plans = jax.vmap(plan)(groups[:, :, :planes])
        pick = jnp.where(jnp.all(plans[4]), pick, len(choices))
        mine = [jnp.max(jnp.where(here, value.astype(jnp.int32), -1), axis=0) for value in plans[:4]]
        mine[2] = mine[2] > 0
        send, relay, table = plan_tables(labels, mine, planes, stride, hops, me)
        fill = devices * stride + (devices // 2 - 1) * hops
        table = jnp.where(table >= 0, table, fill + jnp.arange(planes) // 2)
        tables = (send, relay, table, coarse_table)

        def relayed(count, ident, fine, coarse):
            return regrid(
                count, inner, stride, hops, ident, devices, tables, diffusion, fine, coarse,
                weights, velocity,
            )

        branches = [
            functools.partial(relayed, count, 1 + k) for k, count in enumerate(choices)
        ]
        state = lax.switch(pick, branches + [padded], old_fine, coarse_in)
    else:
        state = padded(old_fine, coarse_in)
    return advance(diffusion, *state, velocity)


def solution(mesh):
    in_specs = (
        P("dev", None, "grp", None),
        P("grp", "dev"),
        P("dev", None, "grp", None),
        P("grp", "dev"),
        P("dev", None, "grp", None),
        P(),
    )
    out_specs = P("dev", None, "grp", None)
    return jax.shard_map(
        on_device, mesh=mesh, in_specs=in_specs, out_specs=out_specs, check_vma=False
    )
```

```python
import functools

import jax
import jax.numpy as jnp
from jax import lax
from jax.experimental import pallas as pl
from jax.experimental.pallas import tpu as pltpu
from jax.sharding import PartitionSpec as P

CROSS = (34, 36, 38, 40, 44)
FINE = (10, 11, 6, 6)
COARSE = (4, 2, 6, 6, 4)
VMEM_LIMIT = 48 * 1024 * 1024
MESH = pl.DeviceIdType.MESH


def params(**more):
    return pltpu.CompilerParams(vmem_limit_bytes=VMEM_LIMIT, **more)


def earlier_count(mask):
    count = mask.shape[-1]
    lower = jnp.arange(count)[None, :] < jnp.arange(count)[:, None]
    return jnp.sum((mask[..., None, :] & lower).astype(jnp.int32), axis=-1)


def send_table(labels, block_len, devices, capacity):
    target = jnp.where(labels >= 0, labels // block_len, -1)
    count = labels.shape[0]
    same = target[None, :] == target[:, None]
    lower = jnp.arange(count)[None, :] < jnp.arange(count)[:, None]
    rank = jnp.sum((same & lower).astype(jnp.int32), axis=1)
    slot = jnp.where(labels >= 0, target * capacity + rank, -1)
    hits = slot[None, :] == jnp.arange(devices * capacity)[:, None]
    return jnp.max(jnp.where(hits, jnp.arange(count)[None, :], 0), axis=1)


def receive_table(labels_all, block_len, capacity, me):
    devices, count = labels_all.shape
    within = labels_all - me * block_len
    valid = (within >= 0) & (within < block_len)
    slot = jnp.arange(devices)[:, None] * capacity + earlier_count(valid)
    flat_within = jnp.where(valid, within, -1).reshape(-1)
    hits = flat_within[None, :] == jnp.arange(block_len)[:, None]
    return jnp.max(jnp.where(hits, slot.reshape(-1)[None, :], -1), axis=1)


def same_dim(a, b):
    return lax.dot_general(
        a, b, (((1,), (1,)), ((), ())), precision=lax.Precision.HIGHEST,
        preferred_element_type=jnp.float32,
    )


def plain_dot(a, b):
    return jnp.dot(a, b, preferred_element_type=jnp.float32)


def as_float(mask):
    return jnp.where(mask, 1.0, 0.0)


def stacked(masks, right):
    out = plain_dot(jnp.concatenate(masks, axis=0), right)
    size = masks[0].shape[0]
    return [out[i * size : (i + 1) * size] for i in range(len(masks))]


def route(owner, devices, base, extra, step, inner, stride, depth, hops):
    shape = owner.shape
    rows, count = shape
    part = devices // 2
    src = lax.rem(lax.broadcasted_iota(jnp.int32, shape, 0), devices)
    home, spot0 = src // part, lax.rem(src, part)
    first = lax.broadcasted_iota(jnp.int32, (count, count), 0)
    second = lax.broadcasted_iota(jnp.int32, (count, count), 1)
    before = as_float(first < second)
    ones = jnp.ones((count, count), jnp.float32)
    masks = [as_float(owner == e) for e in range(devices)]
    ranks = stacked(masks, before)
    counts = [c.astype(jnp.int32) for c in stacked(masks, ones)]
    rank = sum(m * r for m, r in zip(masks, ranks)).astype(jnp.int32)
    caps = []
    for v in range(devices):
        turn = lax.rem(v + part - spot0, part)
        wide = base + jnp.where(turn < extra, step, 0)
        caps.append(jnp.where(home != v // part, wide, inner))
    limit = sum(jnp.where(owner == v, caps[v], 0) for v in range(devices))
    valid = owner >= 0
    over = valid & (rank >= limit)
    side = jnp.where(valid, owner // part, -1)
    orders = stacked([as_float(over & (side == h)) for h in range(2)], before)
    order = jnp.where(side == 0, orders[0], orders[1]).astype(jnp.int32)
    lent_via = jnp.full(shape, -1, jnp.int32)
    lent_spot = jnp.zeros(shape, jnp.int32)
    for h in range(2):
        passed = jnp.zeros(shape, jnp.int32)
        seek = jnp.where(over & (side == h), order, -1)
        for l in range(stride - 1, -1, -1):
            for v in range(h * part, (h + 1) * part):
                free = (counts[v] <= l) & (caps[v] > l)
                hit = free & (seek == passed)
                lent_via = jnp.where(hit, v, lent_via)
                lent_spot = jnp.where(hit, l, lent_spot)
                passed = passed + jnp.where(free, 1, 0)
    via = jnp.where(over, lent_via, owner)
    spot = jnp.where(over, lent_spot, rank)
    relayed = over & (via >= 0) & (via != owner)
    limit_via = sum(jnp.where(via == v, caps[v], 0) for v in range(devices))
    deep = relayed & (spot < limit_via - depth)
    bad = (over & (lent_via < 0)) | deep
    lanes = [
        (v, e) for v in range(devices) for e in range(devices)
        if v != e and v // part == e // part
    ]
    hops_at = [as_float(relayed & (via == v) & (owner == e)) for v, e in lanes]
    inside = stacked(hops_at, before)
    total = stacked(hops_at, jnp.ones((count, 128), jnp.float32))
    lane = lax.broadcasted_iota(jnp.int32, (rows, 128), 1)
    table = sum(jnp.where(lane == i, t, 0.0) for i, t in enumerate(total))
    up = lax.broadcasted_iota(jnp.int32, (rows, rows), 0)
    across = lax.broadcasted_iota(jnp.int32, (rows, rows), 1)
    earlier = as_float((up // devices == across // devices) & (across < up))
    ahead = plain_dot(earlier, table)
    index = jnp.zeros(shape, jnp.float32)
    for i, m in enumerate(hops_at):
        index = index + m * (inside[i] + ahead[:, i : i + 1])
    crowded = jnp.max(ahead + table, axis=(0, 1), keepdims=True) > hops
    fault = jnp.max(as_float(bad), axis=(0, 1), keepdims=True) > 0.0
    return via, spot, relayed, index.astype(jnp.int32), caps, crowded | fault


def widest_load(owner, devices):
    part = devices // 2
    src = lax.rem(lax.broadcasted_iota(jnp.int32, owner.shape, 0), devices)
    away = (owner >= 0) & (owner // part != src // part)
    load = jnp.sum(as_float(away), axis=1, keepdims=True)
    return jnp.max(load, axis=0, keepdims=True)


def plan_kernel(
    groups, devices, block_len, coarse_len, sizes, choices,
    place, fine_ids, coarse_ids, out, via_ref, where_ref, kind_ref, owner_ref, inner_ref,
):
    inner, stride, depth, hops, base_c, extra_c, step_c, inner_c, stride_c, hops_c = sizes
    part = devices // 2
    g, me = place[0], place[1]
    fine, coarse = fine_ids[...], coarse_ids[...]
    rows, count = fine.shape
    count_c = coarse.shape[1]
    width = out.shape[1]
    owner = jnp.where(fine >= 0, fine // block_len, -1)
    load = widest_load(owner, devices)
    pick = sum(jnp.where(load > float(c), 1, 0) for c in choices)
    wide = sum(jnp.where(pick == i, c, 0) for i, c in enumerate(choices))
    base, extra = wide // part, lax.rem(wide, part)

    both = jnp.where(fine >= 0, lax.rem(fine, block_len) // 2, -1)
    kind = lax.broadcasted_iota(jnp.int32, (devices, count), 0)
    cell = lax.broadcasted_iota(jnp.int32, (coarse_len, count), 0)
    cell_c = lax.broadcasted_iota(jnp.int32, (coarse_len, count_c), 0)
    kind_c = lax.broadcasted_iota(jnp.int32, (devices, count_c), 0)
    owner_c = coarse // coarse_len
    within_c = lax.rem(coarse, coarse_len)
    needed = []
    for k in range(groups):
        held = jnp.zeros((devices, coarse_len), jnp.float32)
        for s in range(devices):
            r = k * devices + s
            held = held + same_dim(
                as_float(owner[r : r + 1] == kind), as_float(both[r : r + 1] == cell)
            )
        for s in range(devices):
            r = k * devices + s
            seen = jnp.dot(
                held, as_float(within_c[r : r + 1] == cell_c),
                precision=lax.Precision.HIGHEST, preferred_element_type=jnp.float32,
            )
            seen = jnp.where(owner_c[r : r + 1] == kind_c, seen, 0.0)
            needed.append(jnp.sum(seen, axis=0, keepdims=True))
    needed = jnp.concatenate(needed, axis=0) < 1.5
    owner_c = jnp.where(needed, owner_c, -1)

    def tables(owner, ids, length, stride, hops, depth, base, extra, step, inner, start):
        via, spot, relayed, index, caps, fault = route(
            owner, devices, base, extra, step, inner, stride, depth, hops
        )
        n = owner.shape[1]
        src = lax.rem(lax.broadcasted_iota(jnp.int32, owner.shape, 0), devices)
        turn = lax.rem(lax.rem(via, part) + part - lax.rem(src, part), part)
        block = jnp.where(via // part != src // part, turn, part + turn)
        cap = sum(jnp.where(via == v, caps[v], 0) for v in range(devices))
        late = stride - depth
        early = spot >= cap - depth
        flat = jnp.where(
            early, devices * late + block * depth + spot - (cap - depth), block * late + spot
        )
        flat = jnp.where(via >= 0, flat, -1)
        arrivals = devices * stride
        via_ref[:, 0:n] = jnp.where(relayed, via, -1)
        where_ref[:, 0:n] = flat
        kind_ref[:, 0:n] = index
        owner_ref[:, 0:n] = owner
        inner_ref[:, 0:n] = ids - me * length
        mine = pl.ds(pl.multiple_of(g * devices, devices), devices)
        via_g = via_ref[mine, 0:n]
        flat_g = where_ref[mine, 0:n]
        index_g = kind_ref[mine, 0:n]
        owner_g = owner_ref[mine, 0:n]
        inner_g = inner_ref[mine, 0:n]
        source = lax.broadcasted_iota(jnp.int32, (devices, n), 0)
        own = jnp.max(jnp.where(source == me, flat_g, -1), axis=0, keepdims=True)
        slots = lax.broadcasted_iota(jnp.int32, (width, n), 0)
        place_at = lax.broadcasted_iota(jnp.int32, (devices, n), 1).astype(jnp.float32)
        send = same_dim(place_at, as_float(own == slots))
        lane = lax.rem(owner_g + 2 * part - lax.rem(me, part), part) - 1
        handed = jnp.where(via_g == me, lane * hops + index_g, -1)
        back = lax.rem(lax.rem(me, part) + part - lax.rem(jnp.maximum(via_g, 0), part), part) - 1
        spot_at = jnp.where(via_g >= 0, arrivals + back * hops + index_g, flat_g)
        inside = jnp.where(owner_g == me, inner_g, -1)
        flat_f = flat_g.astype(jnp.float32)
        spot_f = spot_at.astype(jnp.float32) + 1.0
        relay = jnp.zeros((devices, width), jnp.float32)
        final = jnp.zeros((devices, width), jnp.float32)
        for s in range(devices):
            relay = relay + same_dim(
                jnp.broadcast_to(flat_f[s : s + 1], (devices, n)),
                as_float(handed[s : s + 1] == slots),
            )
            final = final + same_dim(
                jnp.broadcast_to(spot_f[s : s + 1], (devices, n)),
                as_float(inside[s : s + 1] == slots),
            )
        at = lax.broadcasted_iota(jnp.int32, (devices, width), 1)
        whole = (final + 0.5).astype(jnp.int32)
        missing = start + (at // 2 if start else 0)
        whole = jnp.where(whole > 0, whole - 1, missing)
        send = (send + 0.5).astype(jnp.int32)
        relay = (relay + 0.5).astype(jnp.int32)
        return send, relay, whole, fault

    fill = devices * stride + (part - 1) * hops
    send, relay, final, fault = tables(
        owner, fine, block_len, stride, hops, depth, base, extra, 1, inner, fill
    )
    send_c, relay_c, final_c, fault_c = tables(
        owner_c, coarse, coarse_len, stride_c, hops_c, stride_c, base_c, extra_c, step_c, inner_c, 0
    )
    pick = jnp.where(fault | fault_c, len(choices), pick)
    parts = (send, relay, final, send_c, relay_c, final_c)
    for i, value in enumerate(parts):
        out[i : i + 1] = value[0:1]
    out[len(parts) : len(parts) + 1] = jnp.broadcast_to(pick, (1, width)).astype(jnp.int32)


def plan(place, fine_ids, coarse_ids, groups, devices, block_len, coarse_len, sizes, choices):
    rows, count = fine_ids.shape
    longest = max(devices * sizes[1], devices * sizes[8], count, (devices // 2) * max(sizes[3], sizes[9]))
    width = -(-longest // 128) * 128
    cells = pltpu.VMEM((rows, max(count, coarse_ids.shape[1])), jnp.int32)
    return pl.pallas_call(
        functools.partial(
            plan_kernel, groups, devices, block_len, coarse_len, sizes, choices
        ),
        out_shape=jax.ShapeDtypeStruct((8, width), jnp.int32),
        in_specs=[
            pl.BlockSpec(memory_space=pltpu.SMEM),
            pl.BlockSpec(memory_space=pltpu.VMEM),
            pl.BlockSpec(memory_space=pltpu.VMEM),
        ],
        out_specs=pl.BlockSpec(memory_space=pltpu.VMEM),
        scratch_shapes=[cells] * 5,
        compiler_params=params(),
        name="plan",
    )(place, fine_ids, coarse_ids)


def pack_fine_kernel(table, source, out, sem):
    def send(i, carry):
        pltpu.make_async_copy(source.at[table[i]], out.at[i], sem).start()
        return carry

    lax.fori_loop(0, out.shape[0], send, 0)
    pltpu.make_async_copy(out, out, sem).wait()


def pack_fine(table, fine):
    return pl.pallas_call(
        pack_fine_kernel,
        out_shape=jax.ShapeDtypeStruct((table.shape[0],) + fine.shape[1:], fine.dtype),
        in_specs=[
            pl.BlockSpec(memory_space=pltpu.SMEM),
            pl.BlockSpec(memory_space=pltpu.VMEM),
        ],
        out_specs=pl.BlockSpec(memory_space=pl.ANY),
        scratch_shapes=[pltpu.SemaphoreType.DMA],
        compiler_params=params(),
        name="pack_fine",
    )(table, fine)


def pack_coarse_kernel(table, source, out):
    half = source.shape[-1]

    def step(i, carry):
        out[i, :, :, 0:half] = source[table[2 * i]]
        out[i, :, :, half : 2 * half] = source[table[2 * i + 1]]
        return carry

    lax.fori_loop(0, out.shape[0], step, 0)


def pack_coarse(table, coarse):
    shape = (table.shape[0] // 2,) + coarse.shape[1:3] + (2 * coarse.shape[3],)
    return pl.pallas_call(
        pack_coarse_kernel,
        out_shape=jax.ShapeDtypeStruct(shape, coarse.dtype),
        in_specs=[
            pl.BlockSpec(memory_space=pltpu.SMEM),
            pl.BlockSpec(memory_space=pltpu.VMEM),
        ],
        out_specs=pl.BlockSpec(memory_space=pltpu.VMEM),
        compiler_params=params(),
        name="pack_coarse",
    )(table, coarse)


def refine_into(table, which, pairs, weights, out, offset, count):
    species, rows, depth = pairs.shape[1:]
    half = depth // 2
    lane = lax.broadcasted_iota(jnp.int32, (species * rows, depth), 1)
    row = lax.broadcasted_iota(jnp.int32, (species, rows, depth), 1)

    def step(c, carry):
        slot = jnp.maximum(table[which, c], 0)
        block = pairs[slot // 2].reshape(species * rows, depth)
        odd = slot % 2
        block = jnp.where((lane >= half).astype(jnp.int32) == odd, block, 0.0)
        spread = jnp.dot(
            block, weights[...], precision=lax.Precision.HIGHEST,
            preferred_element_type=jnp.float32,
        )
        plain = spread[:, :depth].reshape(species, rows, depth)
        sloped = spread[:, depth:].reshape(species, rows, depth)
        below = jnp.where(row == 0, plain, pltpu.roll(plain, 1, 1))
        above = jnp.where(row == rows - 1, plain, pltpu.roll(plain, rows - 1, 1))
        slope = 0.125 * (above - below)
        for s in range(species):
            out[offset + c, s, pl.ds(0, rows, 2), :] = sloped[s] - slope[s]
            out[offset + c, s, pl.ds(1, rows, 2), :] = sloped[s] + slope[s]
        return carry

    lax.fori_loop(0, count, step, 0)


def refine_kernel(table, pairs, weights, out):
    refine_into(table, 0, pairs, weights, out, 0, out.shape[0])


def spread_weights(half):
    depth = 2 * half
    coarse = jnp.arange(half)[:, None]
    fine = jnp.arange(depth)[None, :]
    centre = (fine // 2 == coarse).astype(jnp.float32)
    up = (jnp.minimum(fine // 2 + 1, half - 1) == coarse).astype(jnp.float32)
    down = (jnp.maximum(fine // 2 - 1, 0) == coarse).astype(jnp.float32)
    side = jnp.where(fine % 2 == 1, 0.125, -0.125)
    both = jnp.concatenate([centre, centre + side * (up - down)], axis=1)
    return jnp.concatenate([both, both], axis=0)


def refine(table, pairs, weights):
    species, rows, depth = pairs.shape[1:]
    return pl.pallas_call(
        refine_kernel,
        out_shape=jax.ShapeDtypeStruct(
            (table.shape[1], species, 2 * rows, depth), pairs.dtype
        ),
        in_specs=[
            pl.BlockSpec(memory_space=pltpu.SMEM),
            pl.BlockSpec(memory_space=pltpu.VMEM),
            pl.BlockSpec(memory_space=pltpu.VMEM),
        ],
        out_specs=pl.BlockSpec(memory_space=pltpu.VMEM),
        compiler_params=params(),
        cost_estimate=pl.CostEstimate(
            flops=40_000_000, bytes_accessed=30_000_000, transcendentals=0
        ),
        name="refine",
    )(table, pairs, weights)


def assemble_kernel(table, arrived, interp, out, sem):
    def fetch(p, carry):
        slot = table[p]

        @pl.when(slot >= 0)
        def _():
            pltpu.make_async_copy(arrived.at[slot], out.at[p], sem).start()

        @pl.when(slot < 0)
        def _():
            pltpu.make_async_copy(interp.at[p // 2], out.at[p], sem).start()

        return carry

    lax.fori_loop(0, out.shape[0], fetch, 0)
    pltpu.make_async_copy(out, out, sem).wait()


def assemble(table, arrived, interp):
    return pl.pallas_call(
        assemble_kernel,
        out_shape=jax.ShapeDtypeStruct((table.shape[0],) + arrived.shape[1:], arrived.dtype),
        in_specs=[
            pl.BlockSpec(memory_space=pltpu.SMEM),
            pl.BlockSpec(memory_space=pl.ANY),
            pl.BlockSpec(memory_space=pl.ANY),
        ],
        out_specs=pl.BlockSpec(memory_space=pltpu.VMEM),
        scratch_shapes=[pltpu.SemaphoreType.DMA],
        compiler_params=params(),
        name="assemble",
    )(table, arrived, interp)


def gather_kernel(groups, devices, mine, out, send_sems, recv_sems):
    total = groups * devices
    me = lax.axis_index("grp") * devices + lax.axis_index("dev")
    barrier = pltpu.get_barrier_semaphore()

    def place(k):
        to = lax.rem(me + k, total)
        return {"grp": to // devices, "dev": lax.rem(to, devices)}

    def greet(k, carry):
        pl.semaphore_signal(barrier, inc=1, device_id=place(k), device_id_type=MESH)
        return carry

    lax.fori_loop(1, total, greet, 0)
    pl.semaphore_wait(barrier, total - 1)

    def copy(k):
        return pltpu.make_async_remote_copy(
            src_ref=mine,
            dst_ref=out.at[me],
            send_sem=send_sems.at[k],
            recv_sem=recv_sems.at[k],
            device_id=place(k),
            device_id_type=MESH,
        )

    def start(k, carry):
        copy(k).start()
        return carry

    def finish(k, carry):
        copy(k).wait_send()
        source = lax.rem(me + total - k, total)
        pltpu.make_async_remote_copy(
            src_ref=mine,
            dst_ref=out.at[source],
            send_sem=send_sems.at[k],
            recv_sem=recv_sems.at[k],
            device_id=place(k),
            device_id_type=MESH,
        ).wait_recv()
        return carry

    lax.fori_loop(1, total, start, 0)
    out[me] = mine[...]
    lax.fori_loop(1, total, finish, 0)


def gather_ids(both, groups, devices):
    width = both.shape[0]
    padded = -(-width // 128) * 128
    mine = jnp.pad(both, (0, padded - width))[None]
    total = groups * devices
    out = pl.pallas_call(
        functools.partial(gather_kernel, groups, devices),
        out_shape=jax.ShapeDtypeStruct((total, 1, padded), both.dtype),
        in_specs=[pl.BlockSpec(memory_space=pltpu.VMEM)],
        out_specs=pl.BlockSpec(memory_space=pltpu.VMEM),
        scratch_shapes=[
            pltpu.SemaphoreType.DMA((total,)),
            pltpu.SemaphoreType.DMA((total,)),
        ],
        compiler_params=pltpu.CompilerParams(collective_id=0, has_side_effects=True),
        name="gather_ids",
    )(mine)
    return out.reshape(groups, devices, padded)[:, :, :width]


def coefficients(flow, x):
    v = [flow[x, k] for k in range(3)]
    plus = [jnp.maximum(w, 0.0) for w in v]
    minus = [jnp.maximum(-w, 0.0) for w in v]
    rest = 1.0
    for k in range(3):
        rest = rest - plus[k] - minus[k]
    return plus, minus, rest


def update(d, coeffs, c, lo, hi, below, above, row, lane):
    rows, depth = c.shape
    plus, minus, rest = coeffs
    ylo = jnp.where(row == 0, below, pltpu.roll(c, 1, 0))
    yhi = jnp.where(row == rows - 1, above, pltpu.roll(c, rows - 1, 0))
    zlo = jnp.where(lane == 0, c, pltpu.roll(c, 1, 1))
    zhi = jnp.where(lane == depth - 1, c, pltpu.roll(c, depth - 1, 1))
    total = (rest - 6.0 * d) * c
    total = total + (plus[0] + d) * lo + (minus[0] + d) * hi
    total = total + (plus[1] + d) * ylo + (minus[1] + d) * yhi
    return total + (plus[2] + d) * zlo + (minus[2] + d) * zhi


def regrid_kernel(
    cross, sizes, tables, diffusion, fine, coarse, weights, flow,
    out, first_out, last_out, below_out, above_out,
    send, send_c, pool, pool_c, near, handed, handed_c, passed_in, passed_c,
    state, low, high, below, above,
    low_next, high_next, below_next, above_next, first_next, last_next,
    send_sems, recv_sems, relay_send, relay_recv, edge_send, edge_recv, row_send, row_recv,
):
    inner, stride, depth, hops, base_c, extra_c, step_c, inner_c, stride_c, hops_c = sizes
    planes, species, rows, depth_z = fine.shape
    half_z = depth_z // 2
    groups, devices = lax.axis_size("grp"), lax.axis_size("dev")
    part = devices // 2
    late = stride - depth
    wide = [cross // part + (1 if k < cross % part else 0) for k in range(part)]
    wide_c = [base_c + (step_c if k < extra_c else 0) for k in range(part)]
    caps = wide + [inner] * part
    caps_c = wide_c + [inner_c] * part
    g, me = lax.axis_index("grp"), lax.axis_index("dev")
    base = (me // part) * part
    other = part - base
    seat = lax.rem(me, part)
    barrier = pltpu.get_barrier_semaphore()
    lane_c = lax.broadcasted_iota(jnp.int32, send_c.shape[1:], 2)

    def target(b):
        if b < part:
            return {"dev": other + lax.rem(seat + b, part)}
        return {"dev": base + lax.rem(seat + b - part, part)}

    def greet(to):
        pl.semaphore_signal(barrier, inc=1, device_id=to, device_id_type=MESH)

    peers = list(range(part)) + list(range(part + 1, devices))
    for b in peers:
        greet(target(b))
    greet({"grp": lax.rem(g + 1, groups)})
    greet({"grp": lax.rem(g + groups - 1, groups)})
    pl.semaphore_wait(barrier, devices + 1)

    def remote(source, into, sems, at, to):
        return pltpu.make_async_remote_copy(
            src_ref=source,
            dst_ref=into,
            send_sem=sems[0].at[at],
            recv_sem=sems[1].at[at],
            device_id=to,
            device_id_type=MESH,
        )

    def pack(first, count, into, offset):
        def step(k, carry):
            into[offset + k] = fine[tables[0, first + k]]
            return carry

        lax.fori_loop(0, count, step, 0)

    def pack_coarse_pairs(first, count, into):
        def step(k, carry):
            into[first + k, :, :, 0:half_z] = coarse[tables[3, 2 * (first + k)]]
            into[first + k, :, :, half_z:depth_z] = coarse[tables[3, 2 * (first + k) + 1]]
            return carry

        lax.fori_loop(0, count, step, 0)

    sems = (send_sems, recv_sems)
    pairs_c = stride_c // 2
    coarse_moves, early_moves, late_moves = [], [], []
    for b in peers:
        count = caps_c[b] // 2
        first = b * pairs_c + pairs_c - count
        pack_coarse_pairs(first, count, send_c)
        cut = pl.ds(first, count)
        coarse_moves.append(remote(send_c.at[cut], pool_c.at[cut], sems, b, target(b)))
        coarse_moves[-1].start()
    begin = devices * late
    for b in peers:
        pack(begin + b * depth, depth, send, begin + b * depth)
        early_moves.append(
            remote(
                send.at[pl.ds(begin + b * depth, depth)], near.at[pl.ds(b * depth, depth)],
                sems, devices + b, target(b),
            )
        )
        early_moves[-1].start()

    def pack_late(b, first, count, turn):
        at = b * late + first
        pack(at, count, send, at)
        cut = pl.ds(at, count)
        late_moves.append(
            remote(send.at[cut], pool.at[cut], sems, (2 + turn) * devices + b, target(b))
        )
        late_moves[-1].start()

    pack_coarse_pairs(part * pairs_c + pairs_c - inner_c // 2, inner_c // 2, pool_c)
    pack(begin + part * depth, depth, near, part * depth)
    pack(part * late, inner - depth, pool, part * late)
    for move in coarse_moves:
        move.wait_recv()

    def half_of(slot, odd):
        value = pool_c[slot // 2]
        turned = pltpu.roll(value, half_z, 2)
        return jnp.where(slot % 2 == odd, value, turned)

    def relay_coarse(k, carry):
        left = half_of(tables[4, 2 * k], 0)
        right = half_of(tables[4, 2 * k + 1], 1)
        handed_c[k] = jnp.where(lane_c < half_z, left, right)
        return carry

    sends_c = hops_c // 2
    relay_sems = (relay_send, relay_recv)
    lax.fori_loop(0, (part - 1) * sends_c, relay_coarse, 0)
    relays_c = []
    for k in range(1, part):
        cut = pl.ds((k - 1) * sends_c, sends_c)
        relays_c.append(remote(handed_c.at[cut], passed_c.at[cut], relay_sems, k, target(part + k)))
        relays_c[-1].start()
    for b in peers:
        pack_late(b, 1, caps[b] - depth - 1, 0)
    for move in early_moves:
        move.wait_recv()

    passed = (part - 1) * hops

    def relay(k, carry):
        handed[k] = near[jnp.maximum(tables[1, k] - begin, 0)]
        return carry

    lax.fori_loop(0, passed, relay, 0)
    relays = []
    for k in range(1, part):
        cut = pl.ds((k - 1) * hops, hops)
        relays.append(
            remote(handed.at[cut], passed_in.at[cut], relay_sems, part + k, target(part + k))
        )
        relays[-1].start()
    for b in peers:
        pack_late(b, 0, 1, 1)

    def keep_near(k, carry):
        pool[begin + k] = near[k]
        return carry

    lax.fori_loop(0, devices * depth, keep_near, 0)
    for move in relays_c:
        move.wait_recv()

    def keep_coarse(k, carry):
        pool_c[devices * pairs_c + k] = passed_c[k]
        return carry

    lax.fori_loop(0, (part - 1) * sends_c, keep_coarse, 0)
    arrivals = devices * stride
    refine_into(tables, 5, pool_c, weights, pool, arrivals + passed, coarse.shape[0])
    for move in late_moves + relays:
        move.wait_recv()

    def keep_passed(k, carry):
        pool[arrivals + k] = passed_in[k]
        return carry

    lax.fori_loop(0, passed, keep_passed, 0)

    def assemble(p, carry):
        at = tables[2, p]
        for s in range(species):
            value = pool[at, s]
            state[p + 1, s] = value
            low[s, pl.ds(p, 1), :] = value[0:1]
            high[s, pl.ds(p, 1), :] = value[rows - 1 : rows]
        return carry

    lax.fori_loop(0, planes, assemble, 0)

    def edge_copy(source, target, at, to):
        return pltpu.make_async_remote_copy(
            src_ref=source,
            dst_ref=target,
            send_sem=edge_send.at[at],
            recv_sem=edge_recv.at[at],
            device_id=to,
            device_id_type=MESH,
        )

    def row_copy(source, target, b, at, to):
        cut = pl.ds(pl.multiple_of(b * 8, 8), 8)
        return pltpu.make_async_remote_copy(
            src_ref=source.at[:, cut],
            dst_ref=target.at[:, cut],
            send_sem=row_send.at[at, b],
            recv_sem=row_recv.at[at, b],
            device_id=to,
            device_id_type=MESH,
        )

    left, right = {"dev": me - 1}, {"dev": me + 1}
    down, up = {"grp": g - 1}, {"grp": g + 1}
    ahead = edge_copy(state.at[pl.ds(planes, 1)], state.at[pl.ds(0, 1)], 0, right)
    back = edge_copy(state.at[pl.ds(1, 1)], state.at[pl.ds(planes + 1, 1)], 1, left)
    rise = edge_copy(high, below, 2, up)
    sink = edge_copy(low, above, 3, down)
    has_left, has_right = me > 0, me < devices - 1
    has_down, has_up = g > 0, g < groups - 1

    @pl.when(has_up)
    def _():
        rise.start()

    @pl.when(has_down)
    def _():
        sink.start()

    @pl.when(has_right)
    def _():
        ahead.start()

    @pl.when(has_left)
    def _():
        back.start()

    for move in coarse_moves + relays_c + early_moves + late_moves + relays:
        move.wait_send()

    @pl.when(has_left)
    def _():
        ahead.wait_recv()

    @pl.when(has_right)
    def _():
        back.wait_recv()

    @pl.when(has_down)
    def _():
        rise.wait_recv()

    @pl.when(has_up)
    def _():
        sink.wait_recv()

    @pl.when(has_right)
    def _():
        ahead.wait_send()

    @pl.when(has_left)
    def _():
        back.wait_send()

    @pl.when(has_up)
    def _():
        rise.wait_send()

    @pl.when(has_down)
    def _():
        sink.wait_send()

    @pl.when(me == 0)
    def _():
        state[0] = jnp.zeros(state.shape[1:], state.dtype)

    @pl.when(me == devices - 1)
    def _():
        state[planes + 1] = jnp.zeros(state.shape[1:], state.dtype)

    @pl.when(g == 0)
    def _():
        below[...] = jnp.zeros(below.shape, below.dtype)

    @pl.when(g == groups - 1)
    def _():
        above[...] = jnp.zeros(above.shape, above.dtype)

    row = lax.broadcasted_iota(jnp.int32, (rows, depth_z), 0)
    lane = lax.broadcasted_iota(jnp.int32, (rows, depth_z), 1)


    next_ahead = edge_copy(out.at[pl.ds(planes - 1, 1)], first_next, 4, right)
    next_back = edge_copy(out.at[pl.ds(0, 1)], last_next, 5, left)
    blocks = planes // 8

    def advance_block(turn, carry):
        b = lax.rem(turn + blocks - 1, blocks)

        def advance_plane(k, carry):
            p = b * 8 + k
            coeffs = coefficients(flow, p)
            for s in range(species):
                total = update(
                    diffusion[s], coeffs, state[p + 1, s], state[p, s], state[p + 2, s],
                    below[s, pl.ds(p, 1), :], above[s, pl.ds(p, 1), :], row, lane,
                )
                out[p, s] = total
                low_next[s, pl.ds(p, 1), :] = total[0:1]
                high_next[s, pl.ds(p, 1), :] = total[rows - 1 : rows]
            return carry

        lax.fori_loop(0, 8, advance_plane, 0)

        @pl.when(has_up)
        def _():
            row_copy(high_next, below_next, b, 0, up).start()

        @pl.when(has_down)
        def _():
            row_copy(low_next, above_next, b, 1, down).start()

        @pl.when((turn == 0) & has_right)
        def _():
            next_ahead.start()

        @pl.when((turn == 1) & has_left)
        def _():
            next_back.start()

        return carry

    lax.fori_loop(0, blocks, advance_block, 0)

    def settle(b, carry):
        @pl.when(has_down)
        def _():
            row_copy(high_next, below_next, b, 0, up).wait_recv()
            row_copy(low_next, above_next, b, 1, down).wait_send()

        @pl.when(has_up)
        def _():
            row_copy(low_next, above_next, b, 1, down).wait_recv()
            row_copy(high_next, below_next, b, 0, up).wait_send()

        return carry

    lax.fori_loop(0, blocks, settle, 0)

    @pl.when(has_left)
    def _():
        next_ahead.wait_recv()
        next_back.wait_send()
        first_out[...] = first_next[...]

    @pl.when(has_right)
    def _():
        next_back.wait_recv()
        next_ahead.wait_send()
        last_out[...] = last_next[...]

    @pl.when(has_down)
    def _():
        below_out[...] = below_next[...]

    @pl.when(has_up)
    def _():
        above_out[...] = above_next[...]

    @pl.when(me == 0)
    def _():
        first_out[...] = jnp.zeros(first_out.shape, first_out.dtype)

    @pl.when(me == devices - 1)
    def _():
        last_out[...] = jnp.zeros(last_out.shape, last_out.dtype)

    @pl.when(g == 0)
    def _():
        below_out[...] = jnp.zeros(below_out.shape, below_out.dtype)

    @pl.when(g == groups - 1)
    def _():
        above_out[...] = jnp.zeros(above_out.shape, above_out.dtype)


def regrid(cross, sizes, ident, devices, tables, diffusion, fine, coarse, weights, flow):
    inner, stride, depth, hops, base_c, extra_c, step_c, inner_c, stride_c, hops_c = sizes
    planes, species, rows, depth_z = fine.shape
    part = devices // 2
    kept = jax.ShapeDtypeStruct(fine.shape, fine.dtype)
    plane = jax.ShapeDtypeStruct((1,) + fine.shape[1:], fine.dtype)
    edge = jax.ShapeDtypeStruct((species, planes, depth_z), fine.dtype)
    pool = devices * stride + (part - 1) * hops + planes // 2
    pool_c = (devices * stride_c + (part - 1) * hops_c) // 2
    vmem = pl.BlockSpec(memory_space=pltpu.VMEM)
    smem = pl.BlockSpec(memory_space=pltpu.SMEM)

    def held(count):
        return pltpu.VMEM((count,) + fine.shape[1:], fine.dtype)

    def held_c(count):
        return pltpu.VMEM((count, species, rows // 2, depth_z), fine.dtype)

    def sems(*shape):
        return [pltpu.SemaphoreType.DMA(shape)] * 2

    rim = pltpu.VMEM(edge.shape, edge.dtype)
    passed, passed_c = (part - 1) * hops, (part - 1) * hops_c // 2
    return pl.pallas_call(
        functools.partial(regrid_kernel, cross, sizes),
        out_shape=(kept, plane, plane, edge, edge),
        in_specs=[smem] * 2 + [vmem] * 4,
        out_specs=(vmem,) * 5,
        scratch_shapes=[
            held(devices * stride), held_c(devices * stride_c // 2), held(pool), held_c(pool_c),
            held(devices * depth), held(passed), held_c(passed_c), held(passed), held_c(passed_c),
            held(planes + 2), rim, rim, rim, rim, rim, rim, rim, rim, held(1), held(1),
            *sems(4 * devices), *sems(2 * part), *sems(6), *sems(2, planes // 8),
        ],
        compiler_params=params(collective_id=ident, has_side_effects=True),
        name="regrid",
    )(tables, diffusion, fine, coarse, weights, flow)


def advance_kernel(steps, diffusion, u, before, after, first, last, below, above, flow, out):
    i = pl.program_id(0)
    block, species, rows, depth = u.shape
    row = lax.broadcasted_iota(jnp.int32, (rows, depth), 0)
    lane = lax.broadcasted_iota(jnp.int32, (rows, depth), 1)
    for x in range(block):
        coeffs = coefficients(flow, x)
        for s in range(species):
            if x > 0:
                lo = u[x - 1, s]
            else:
                lo = jnp.where(i == 0, first[0, s], before[0, s])
            if x < block - 1:
                hi = u[x + 1, s]
            else:
                hi = jnp.where(i == steps - 1, last[0, s], after[0, s])
            out[x, s] = update(
                diffusion[s], coeffs, u[x, s], lo, hi,
                below[s, pl.ds(x, 1), :], above[s, pl.ds(x, 1), :], row, lane,
            )


def advance(diffusion, u, first, last, below, above, flow):
    planes, species, rows, depth = u.shape
    block = 8 if planes % 8 == 0 else planes
    steps = planes // block
    edge_spec = pl.BlockSpec((species, block, depth), lambda i: (0, i, 0))
    plane_spec = pl.BlockSpec((1, species, rows, depth), lambda i: (0, 0, 0, 0))
    block_spec = pl.BlockSpec((block, species, rows, depth), lambda i: (i, 0, 0, 0))
    return pl.pallas_call(
        functools.partial(advance_kernel, steps),
        grid=(steps,),
        out_shape=jax.ShapeDtypeStruct(u.shape, u.dtype),
        in_specs=[
            pl.BlockSpec(memory_space=pltpu.SMEM),
            block_spec,
            pl.BlockSpec(
                (1, species, rows, depth), lambda i: (jnp.maximum(i * block - 1, 0), 0, 0, 0)
            ),
            pl.BlockSpec(
                (1, species, rows, depth),
                lambda i: (jnp.minimum(i * block + block, planes - 1), 0, 0, 0),
            ),
            plane_spec,
            plane_spec,
            edge_spec,
            edge_spec,
            pl.BlockSpec((block, 3, rows, depth), lambda i: (i, 0, 0, 0)),
        ],
        out_specs=block_spec,
        compiler_params=params(),
        name="advance",
    )(diffusion, u, u, u, first, last, below, above, flow)


def shift_up(value, axis):
    size = lax.axis_size(axis)
    return lax.ppermute(value, axis, [(i, i + 1) for i in range(size - 1)])


def shift_down(value, axis):
    size = lax.axis_size(axis)
    return lax.ppermute(value, axis, [(i + 1, i) for i in range(size - 1)])


def rims(u):
    rows = u.shape[2]
    below = shift_up(jnp.swapaxes(u[:, :, rows - 1], 0, 1), "grp")
    above = shift_down(jnp.swapaxes(u[:, :, 0], 0, 1), "grp")
    return shift_up(u[-1:], "dev"), shift_down(u[:1], "dev"), below, above


def on_device(old_fine, old_ids, old_coarse, coarse_ids, velocity, diffusion):
    devices = lax.axis_size("dev")
    group_count = lax.axis_size("grp")
    me = lax.axis_index("dev")
    planes = old_fine.shape[0]
    coarse_planes = old_coarse.shape[0]
    capacity = max(2, 2 * planes // devices)
    coarse_capacity = max(2, 2 * coarse_planes // devices)
    both = jnp.concatenate([old_ids[0], coarse_ids[0]])
    relaying = capacity >= 16 and devices % 2 == 0 and planes % 8 == 0 and group_count > 2
    if relaying:
        groups = gather_ids(both, group_count, devices)
    else:
        groups = lax.all_gather(both, ("grp", "dev")).reshape(group_count, devices, -1)
    weights = spread_weights(old_coarse.shape[3])

    def padded(fine, coarse):
        here = (jnp.arange(group_count) == lax.axis_index("grp"))[:, None, None]
        both_all = jnp.max(jnp.where(here, groups, -1), axis=0)
        own = jnp.max(jnp.where((jnp.arange(devices) == me)[:, None], both_all, -1), axis=0)
        coarse_send = send_table(own[planes:], coarse_planes, devices, coarse_capacity)
        coarse_table = receive_table(both_all[:, planes:], coarse_planes, coarse_capacity, me)
        coarse_out = pack_coarse(coarse_send, coarse)
        coarse_in = lax.all_to_all(coarse_out, "dev", split_axis=0, concat_axis=0, tiled=True)
        send = send_table(own[:planes], planes, devices, capacity)
        table = receive_table(both_all[:, :planes], planes, capacity, me)
        arrived = lax.all_to_all(pack_fine(send, fine), "dev", split_axis=0, concat_axis=0, tiled=True)
        interp = refine(coarse_table[None], coarse_in, weights)
        u = assemble(table, arrived, interp)
        u = advance(diffusion, u, *rims(u), velocity)
        return (u,) + rims(u)

    if relaying:
        choices = [capacity * k // 16 for k in CROSS]
        sizes = tuple(capacity * k // 16 for k in FINE) + tuple(coarse_capacity * k // 8 for k in COARSE)
        sizes = sizes[:5] + (1,) + sizes[5:]
        rows = group_count * devices
        flat = groups.reshape(rows, -1)
        place = jnp.stack([lax.axis_index("grp"), me]).astype(jnp.int32)
        tables = plan(
            place, flat[:, :planes], flat[:, planes:], group_count, devices, planes,
            coarse_planes, sizes, choices,
        )

        def relayed(count, ident, fine, coarse):
            return regrid(
                count, sizes, ident, devices, tables, diffusion, fine, coarse, weights, velocity
            )

        branches = [
            functools.partial(relayed, count, 1 + k) for k, count in enumerate(choices)
        ]
        state = lax.switch(tables[6, 0], branches + [padded], old_fine, old_coarse)
    else:
        state = padded(old_fine, old_coarse)
    return advance(diffusion, *state, velocity)


def solution(mesh):
    in_specs = (
        P("dev", None, "grp", None),
        P("grp", "dev"),
        P("dev", None, "grp", None),
        P("grp", "dev"),
        P("dev", None, "grp", None),
        P(),
    )
    out_specs = P("dev", None, "grp", None)
    return jax.shard_map(
        on_device, mesh=mesh, in_specs=in_specs, out_specs=out_specs, check_vma=False
    )
```

```python
import functools

import jax
import jax.numpy as jnp
from jax import lax
from jax.experimental import pallas as pl
from jax.experimental.pallas import tpu as pltpu
from jax.sharding import PartitionSpec as P

CROSS = (34, 36, 38, 40, 44)
FINE = (10, 11, 6, 6)
COARSE = (4, 2, 6, 6, 4)
VMEM_LIMIT = 48 * 1024 * 1024
MESH = pl.DeviceIdType.MESH


def params(**more):
    return pltpu.CompilerParams(vmem_limit_bytes=VMEM_LIMIT, **more)


def earlier_count(mask):
    count = mask.shape[-1]
    lower = jnp.arange(count)[None, :] < jnp.arange(count)[:, None]
    return jnp.sum((mask[..., None, :] & lower).astype(jnp.int32), axis=-1)


def send_table(labels, block_len, devices, capacity):
    target = jnp.where(labels >= 0, labels // block_len, -1)
    count = labels.shape[0]
    same = target[None, :] == target[:, None]
    lower = jnp.arange(count)[None, :] < jnp.arange(count)[:, None]
    rank = jnp.sum((same & lower).astype(jnp.int32), axis=1)
    slot = jnp.where(labels >= 0, target * capacity + rank, -1)
    hits = slot[None, :] == jnp.arange(devices * capacity)[:, None]
    return jnp.max(jnp.where(hits, jnp.arange(count)[None, :], 0), axis=1)


def receive_table(labels_all, block_len, capacity, me):
    devices, count = labels_all.shape
    within = labels_all - me * block_len
    valid = (within >= 0) & (within < block_len)
    slot = jnp.arange(devices)[:, None] * capacity + earlier_count(valid)
    flat_within = jnp.where(valid, within, -1).reshape(-1)
    hits = flat_within[None, :] == jnp.arange(block_len)[:, None]
    return jnp.max(jnp.where(hits, slot.reshape(-1)[None, :], -1), axis=1)


def same_dim(a, b, exact=None):
    return lax.dot_general(
        a, b, (((1,), (1,)), ((), ())), precision=exact,
        preferred_element_type=jnp.float32,
    )


def plain_dot(a, b):
    return jnp.dot(a, b, preferred_element_type=jnp.float32)


def as_float(mask):
    return jnp.where(mask, 1.0, 0.0)


def stacked(masks, right):
    out = plain_dot(jnp.concatenate(masks, axis=0), right)
    size = masks[0].shape[0]
    return [out[i * size : (i + 1) * size] for i in range(len(masks))]


def route(owner, devices, base, extra, step, inner, stride, depth, hops):
    shape = owner.shape
    rows, count = shape
    part = devices // 2
    src = lax.rem(lax.broadcasted_iota(jnp.int32, shape, 0), devices)
    home, spot0 = src // part, lax.rem(src, part)
    first = lax.broadcasted_iota(jnp.int32, (count, count), 0)
    second = lax.broadcasted_iota(jnp.int32, (count, count), 1)
    before = as_float(first < second)
    ones = jnp.ones((count, count), jnp.float32)
    masks = [as_float(owner == e) for e in range(devices)]
    ranks = stacked(masks, before)
    counts = [c.astype(jnp.int32) for c in stacked(masks, ones)]
    rank = sum(m * r for m, r in zip(masks, ranks)).astype(jnp.int32)
    caps = []
    for v in range(devices):
        turn = lax.rem(v + part - spot0, part)
        wide = base + jnp.where(turn < extra, step, 0)
        caps.append(jnp.where(home != v // part, wide, inner))
    limit = sum(jnp.where(owner == v, caps[v], 0) for v in range(devices))
    valid = owner >= 0
    over = valid & (rank >= limit)
    side = jnp.where(valid, owner // part, -1)
    orders = stacked([as_float(over & (side == h)) for h in range(2)], before)
    order = jnp.where(side == 0, orders[0], orders[1]).astype(jnp.int32)
    lent_via = jnp.full(shape, -1, jnp.int32)
    lent_spot = jnp.zeros(shape, jnp.int32)
    for h in range(2):
        passed = jnp.zeros(shape, jnp.int32)
        seek = jnp.where(over & (side == h), order, -1)
        for l in range(stride - 1, -1, -1):
            for v in range(h * part, (h + 1) * part):
                free = (counts[v] <= l) & (caps[v] > l)
                hit = free & (seek == passed)
                lent_via = jnp.where(hit, v, lent_via)
                lent_spot = jnp.where(hit, l, lent_spot)
                passed = passed + jnp.where(free, 1, 0)
    via = jnp.where(over, lent_via, owner)
    spot = jnp.where(over, lent_spot, rank)
    relayed = over & (via >= 0) & (via != owner)
    limit_via = sum(jnp.where(via == v, caps[v], 0) for v in range(devices))
    deep = relayed & (spot < limit_via - depth)
    bad = (over & (lent_via < 0)) | deep
    lanes = [
        (v, e) for v in range(devices) for e in range(devices)
        if v != e and v // part == e // part
    ]
    hops_at = [as_float(relayed & (via == v) & (owner == e)) for v, e in lanes]
    inside = stacked(hops_at, before)
    total = stacked(hops_at, jnp.ones((count, 128), jnp.float32))
    lane = lax.broadcasted_iota(jnp.int32, (rows, 128), 1)
    table = sum(jnp.where(lane == i, t, 0.0) for i, t in enumerate(total))
    up = lax.broadcasted_iota(jnp.int32, (rows, rows), 0)
    across = lax.broadcasted_iota(jnp.int32, (rows, rows), 1)
    earlier = as_float((up // devices == across // devices) & (across < up))
    ahead = plain_dot(earlier, table)
    index = jnp.zeros(shape, jnp.float32)
    for i, m in enumerate(hops_at):
        index = index + m * (inside[i] + ahead[:, i : i + 1])
    crowded = jnp.max(ahead + table, axis=(0, 1), keepdims=True) > hops
    fault = jnp.max(as_float(bad), axis=(0, 1), keepdims=True) > 0.0
    return via, spot, relayed, index.astype(jnp.int32), caps, crowded | fault


def widest_load(owner, devices):
    part = devices // 2
    src = lax.rem(lax.broadcasted_iota(jnp.int32, owner.shape, 0), devices)
    away = (owner >= 0) & (owner // part != src // part)
    load = jnp.sum(as_float(away), axis=1, keepdims=True)
    return jnp.max(load, axis=0, keepdims=True)


def plan_kernel(
    groups, devices, block_len, coarse_len, sizes, choices,
    place, fine_ids, coarse_ids, out, via_ref, where_ref, kind_ref, owner_ref, inner_ref,
):
    inner, stride, depth, hops, base_c, extra_c, step_c, inner_c, stride_c, hops_c = sizes
    part = devices // 2
    g, me = place[0], place[1]
    fine, coarse = fine_ids[...], coarse_ids[...]
    rows, count = fine.shape
    count_c = coarse.shape[1]
    width = out.shape[1]
    owner = jnp.where(fine >= 0, fine // block_len, -1)
    load = widest_load(owner, devices)
    pick = sum(jnp.where(load > float(c), 1, 0) for c in choices)
    wide = sum(jnp.where(pick == i, c, 0) for i, c in enumerate(choices))
    base, extra = wide // part, lax.rem(wide, part)

    both = jnp.where(fine >= 0, lax.rem(fine, block_len) // 2, -1)
    kind = lax.broadcasted_iota(jnp.int32, (devices, count), 0)
    cell = lax.broadcasted_iota(jnp.int32, (coarse_len, count), 0)
    cell_c = lax.broadcasted_iota(jnp.int32, (coarse_len, count_c), 0)
    kind_c = lax.broadcasted_iota(jnp.int32, (devices, count_c), 0)
    owner_c = coarse // coarse_len
    within_c = lax.rem(coarse, coarse_len)
    needed = []
    for k in range(groups):
        held = jnp.zeros((devices, coarse_len), jnp.float32)
        for s in range(devices):
            r = k * devices + s
            held = held + same_dim(
                as_float(owner[r : r + 1] == kind), as_float(both[r : r + 1] == cell)
            )
        for s in range(devices):
            r = k * devices + s
            seen = plain_dot(held, as_float(within_c[r : r + 1] == cell_c))
            seen = jnp.where(owner_c[r : r + 1] == kind_c, seen, 0.0)
            needed.append(jnp.sum(seen, axis=0, keepdims=True))
    needed = jnp.concatenate(needed, axis=0) < 1.5
    owner_c = jnp.where(needed, owner_c, -1)

    def tables(owner, ids, length, stride, hops, depth, base, extra, step, inner, start):
        via, spot, relayed, index, caps, fault = route(
            owner, devices, base, extra, step, inner, stride, depth, hops
        )
        n = owner.shape[1]
        src = lax.rem(lax.broadcasted_iota(jnp.int32, owner.shape, 0), devices)
        turn = lax.rem(lax.rem(via, part) + part - lax.rem(src, part), part)
        block = jnp.where(via // part != src // part, turn, part + turn)
        cap = sum(jnp.where(via == v, caps[v], 0) for v in range(devices))
        late = stride - depth
        early = spot >= cap - depth
        flat = jnp.where(
            early, devices * late + block * depth + spot - (cap - depth), block * late + spot
        )
        flat = jnp.where(via >= 0, flat, -1)
        arrivals = devices * stride
        small = max(n, arrivals + (part - 1) * hops + 1) <= 256
        exact = None if small else lax.Precision.HIGHEST
        via_ref[:, 0:n] = jnp.where(relayed, via, -1)
        where_ref[:, 0:n] = flat
        kind_ref[:, 0:n] = index
        owner_ref[:, 0:n] = owner
        inner_ref[:, 0:n] = ids - me * length
        mine = pl.ds(pl.multiple_of(g * devices, devices), devices)
        via_g = via_ref[mine, 0:n]
        flat_g = where_ref[mine, 0:n]
        index_g = kind_ref[mine, 0:n]
        owner_g = owner_ref[mine, 0:n]
        inner_g = inner_ref[mine, 0:n]
        source = lax.broadcasted_iota(jnp.int32, (devices, n), 0)
        own = jnp.max(jnp.where(source == me, flat_g, -1), axis=0, keepdims=True)
        slots = lax.broadcasted_iota(jnp.int32, (width, n), 0)
        place_at = lax.broadcasted_iota(jnp.int32, (devices, n), 1).astype(jnp.float32)
        send = same_dim(place_at, as_float(own == slots), exact)
        lane = lax.rem(owner_g + 2 * part - lax.rem(me, part), part) - 1
        handed = jnp.where(via_g == me, lane * hops + index_g, -1)
        back = lax.rem(lax.rem(me, part) + part - lax.rem(jnp.maximum(via_g, 0), part), part) - 1
        spot_at = jnp.where(via_g >= 0, arrivals + back * hops + index_g, flat_g)
        inside = jnp.where(owner_g == me, inner_g, -1)
        flat_f = flat_g.astype(jnp.float32)
        spot_f = spot_at.astype(jnp.float32) + 1.0
        relay = jnp.zeros((devices, width), jnp.float32)
        final = jnp.zeros((devices, width), jnp.float32)
        for s in range(devices):
            relay = relay + same_dim(
                jnp.broadcast_to(flat_f[s : s + 1], (devices, n)),
                as_float(handed[s : s + 1] == slots), exact,
            )
            final = final + same_dim(
                jnp.broadcast_to(spot_f[s : s + 1], (devices, n)),
                as_float(inside[s : s + 1] == slots), exact,
            )
        at = lax.broadcasted_iota(jnp.int32, (devices, width), 1)
        whole = (final + 0.5).astype(jnp.int32)
        missing = start + (at // 2 if start else 0)
        whole = jnp.where(whole > 0, whole - 1, missing)
        send = (send + 0.5).astype(jnp.int32)
        relay = (relay + 0.5).astype(jnp.int32)
        return send, relay, whole, fault

    fill = devices * stride + (part - 1) * hops
    send, relay, final, fault = tables(
        owner, fine, block_len, stride, hops, depth, base, extra, 1, inner, fill
    )
    send_c, relay_c, final_c, fault_c = tables(
        owner_c, coarse, coarse_len, stride_c, hops_c, stride_c, base_c, extra_c, step_c, inner_c, 0
    )
    pick = jnp.where(fault | fault_c, len(choices), pick)
    parts = (send, relay, final, send_c, relay_c, final_c)
    for i, value in enumerate(parts):
        out[i : i + 1] = value[0:1]
    out[len(parts) : len(parts) + 1] = jnp.broadcast_to(pick, (1, width)).astype(jnp.int32)


def plan(place, fine_ids, coarse_ids, groups, devices, block_len, coarse_len, sizes, choices):
    rows, count = fine_ids.shape
    longest = max(devices * sizes[1], devices * sizes[8], count, (devices // 2) * max(sizes[3], sizes[9]))
    width = -(-longest // 128) * 128
    cells = pltpu.VMEM((rows, max(count, coarse_ids.shape[1])), jnp.int32)
    return pl.pallas_call(
        functools.partial(
            plan_kernel, groups, devices, block_len, coarse_len, sizes, choices
        ),
        out_shape=jax.ShapeDtypeStruct((8, width), jnp.int32),
        in_specs=[
            pl.BlockSpec(memory_space=pltpu.SMEM),
            pl.BlockSpec(memory_space=pltpu.VMEM),
            pl.BlockSpec(memory_space=pltpu.VMEM),
        ],
        out_specs=pl.BlockSpec(memory_space=pltpu.VMEM),
        scratch_shapes=[cells] * 5,
        compiler_params=params(),
        name="plan",
    )(place, fine_ids, coarse_ids)


def pack_fine_kernel(table, source, out, sem):
    def send(i, carry):
        pltpu.make_async_copy(source.at[table[i]], out.at[i], sem).start()
        return carry

    lax.fori_loop(0, out.shape[0], send, 0)
    pltpu.make_async_copy(out, out, sem).wait()


def pack_fine(table, fine):
    return pl.pallas_call(
        pack_fine_kernel,
        out_shape=jax.ShapeDtypeStruct((table.shape[0],) + fine.shape[1:], fine.dtype),
        in_specs=[
            pl.BlockSpec(memory_space=pltpu.SMEM),
            pl.BlockSpec(memory_space=pltpu.VMEM),
        ],
        out_specs=pl.BlockSpec(memory_space=pl.ANY),
        scratch_shapes=[pltpu.SemaphoreType.DMA],
        compiler_params=params(),
        name="pack_fine",
    )(table, fine)


def pack_coarse_kernel(table, source, out):
    half = source.shape[-1]

    def step(i, carry):
        out[i, :, :, 0:half] = source[table[2 * i]]
        out[i, :, :, half : 2 * half] = source[table[2 * i + 1]]
        return carry

    lax.fori_loop(0, out.shape[0], step, 0)


def pack_coarse(table, coarse):
    shape = (table.shape[0] // 2,) + coarse.shape[1:3] + (2 * coarse.shape[3],)
    return pl.pallas_call(
        pack_coarse_kernel,
        out_shape=jax.ShapeDtypeStruct(shape, coarse.dtype),
        in_specs=[
            pl.BlockSpec(memory_space=pltpu.SMEM),
            pl.BlockSpec(memory_space=pltpu.VMEM),
        ],
        out_specs=pl.BlockSpec(memory_space=pltpu.VMEM),
        compiler_params=params(),
        name="pack_coarse",
    )(table, coarse)


def refine_into(table, which, pairs, weights, out, offset, count):
    species, rows, depth = pairs.shape[1:]
    half = depth // 2
    lane = lax.broadcasted_iota(jnp.int32, (species * rows, depth), 1)
    row = lax.broadcasted_iota(jnp.int32, (species, rows, depth), 1)

    def step(c, carry):
        slot = jnp.maximum(table[which, c], 0)
        block = pairs[slot // 2].reshape(species * rows, depth)
        odd = slot % 2
        block = jnp.where((lane >= half).astype(jnp.int32) == odd, block, 0.0)
        spread = jnp.dot(
            block, weights[...], precision=lax.Precision.HIGHEST,
            preferred_element_type=jnp.float32,
        )
        plain = spread[:, :depth].reshape(species, rows, depth)
        sloped = spread[:, depth:].reshape(species, rows, depth)
        below = jnp.where(row == 0, plain, pltpu.roll(plain, 1, 1))
        above = jnp.where(row == rows - 1, plain, pltpu.roll(plain, rows - 1, 1))
        slope = 0.125 * (above - below)
        for s in range(species):
            out[offset + c, s, pl.ds(0, rows, 2), :] = sloped[s] - slope[s]
            out[offset + c, s, pl.ds(1, rows, 2), :] = sloped[s] + slope[s]
        return carry

    lax.fori_loop(0, count, step, 0)


def refine_kernel(table, pairs, weights, out):
    refine_into(table, 0, pairs, weights, out, 0, out.shape[0])


def spread_weights(half):
    depth = 2 * half
    coarse = jnp.arange(half)[:, None]
    fine = jnp.arange(depth)[None, :]
    centre = (fine // 2 == coarse).astype(jnp.float32)
    up = (jnp.minimum(fine // 2 + 1, half - 1) == coarse).astype(jnp.float32)
    down = (jnp.maximum(fine // 2 - 1, 0) == coarse).astype(jnp.float32)
    side = jnp.where(fine % 2 == 1, 0.125, -0.125)
    both = jnp.concatenate([centre, centre + side * (up - down)], axis=1)
    return jnp.concatenate([both, both], axis=0)


def refine(table, pairs, weights):
    species, rows, depth = pairs.shape[1:]
    return pl.pallas_call(
        refine_kernel,
        out_shape=jax.ShapeDtypeStruct(
            (table.shape[1], species, 2 * rows, depth), pairs.dtype
        ),
        in_specs=[
            pl.BlockSpec(memory_space=pltpu.SMEM),
            pl.BlockSpec(memory_space=pltpu.VMEM),
            pl.BlockSpec(memory_space=pltpu.VMEM),
        ],
        out_specs=pl.BlockSpec(memory_space=pltpu.VMEM),
        compiler_params=params(),
        cost_estimate=pl.CostEstimate(
            flops=40_000_000, bytes_accessed=30_000_000, transcendentals=0
        ),
        name="refine",
    )(table, pairs, weights)


def assemble_kernel(table, arrived, interp, out, sem):
    def fetch(p, carry):
        slot = table[p]

        @pl.when(slot >= 0)
        def _():
            pltpu.make_async_copy(arrived.at[slot], out.at[p], sem).start()

        @pl.when(slot < 0)
        def _():
            pltpu.make_async_copy(interp.at[p // 2], out.at[p], sem).start()

        return carry

    lax.fori_loop(0, out.shape[0], fetch, 0)
    pltpu.make_async_copy(out, out, sem).wait()


def assemble(table, arrived, interp):
    return pl.pallas_call(
        assemble_kernel,
        out_shape=jax.ShapeDtypeStruct((table.shape[0],) + arrived.shape[1:], arrived.dtype),
        in_specs=[
            pl.BlockSpec(memory_space=pltpu.SMEM),
            pl.BlockSpec(memory_space=pl.ANY),
            pl.BlockSpec(memory_space=pl.ANY),
        ],
        out_specs=pl.BlockSpec(memory_space=pltpu.VMEM),
        scratch_shapes=[pltpu.SemaphoreType.DMA],
        compiler_params=params(),
        name="assemble",
    )(table, arrived, interp)


def gather_kernel(groups, devices, mine, out, send_sems, recv_sems):
    total = groups * devices
    me = lax.axis_index("grp") * devices + lax.axis_index("dev")
    barrier = pltpu.get_barrier_semaphore()

    def place(k):
        to = lax.rem(me + k, total)
        return {"grp": to // devices, "dev": lax.rem(to, devices)}

    def greet(k, carry):
        pl.semaphore_signal(barrier, inc=1, device_id=place(k), device_id_type=MESH)
        return carry

    lax.fori_loop(1, total, greet, 0)
    pl.semaphore_wait(barrier, total - 1)

    def copy(k):
        return pltpu.make_async_remote_copy(
            src_ref=mine,
            dst_ref=out.at[me],
            send_sem=send_sems.at[k],
            recv_sem=recv_sems.at[k],
            device_id=place(k),
            device_id_type=MESH,
        )

    def start(k, carry):
        copy(k).start()
        return carry

    def finish(k, carry):
        copy(k).wait_send()
        source = lax.rem(me + total - k, total)
        pltpu.make_async_remote_copy(
            src_ref=mine,
            dst_ref=out.at[source],
            send_sem=send_sems.at[k],
            recv_sem=recv_sems.at[k],
            device_id=place(k),
            device_id_type=MESH,
        ).wait_recv()
        return carry

    lax.fori_loop(1, total, start, 0)
    out[me] = mine[...]
    lax.fori_loop(1, total, finish, 0)


def gather_ids(both, groups, devices):
    width = both.shape[0]
    padded = -(-width // 128) * 128
    mine = jnp.pad(both, (0, padded - width))[None]
    total = groups * devices
    out = pl.pallas_call(
        functools.partial(gather_kernel, groups, devices),
        out_shape=jax.ShapeDtypeStruct((total, 1, padded), both.dtype),
        in_specs=[pl.BlockSpec(memory_space=pltpu.VMEM)],
        out_specs=pl.BlockSpec(memory_space=pltpu.VMEM),
        scratch_shapes=[
            pltpu.SemaphoreType.DMA((total,)),
            pltpu.SemaphoreType.DMA((total,)),
        ],
        compiler_params=pltpu.CompilerParams(collective_id=0, has_side_effects=True),
        name="gather_ids",
    )(mine)
    return out.reshape(groups, devices, padded)[:, :, :width]


def coefficients(flow, x):
    v = [flow[x, k] for k in range(3)]
    plus = [jnp.maximum(w, 0.0) for w in v]
    minus = [jnp.maximum(-w, 0.0) for w in v]
    rest = 1.0
    for k in range(3):
        rest = rest - plus[k] - minus[k]
    return plus, minus, rest


def update(d, coeffs, c, lo, hi, below, above, row, lane):
    rows, depth = c.shape
    plus, minus, rest = coeffs
    ylo = jnp.where(row == 0, below, pltpu.roll(c, 1, 0))
    yhi = jnp.where(row == rows - 1, above, pltpu.roll(c, rows - 1, 0))
    zlo = jnp.where(lane == 0, c, pltpu.roll(c, 1, 1))
    zhi = jnp.where(lane == depth - 1, c, pltpu.roll(c, depth - 1, 1))
    total = (rest - 6.0 * d) * c
    total = total + (plus[0] + d) * lo + (minus[0] + d) * hi
    total = total + (plus[1] + d) * ylo + (minus[1] + d) * yhi
    return total + (plus[2] + d) * zlo + (minus[2] + d) * zhi


def regrid_kernel(
    cross, sizes, tables, diffusion, fine_hbm, coarse_hbm, weights, flow_hbm,
    out_hbm, first_out, last_out, below_out, above_out,
    fine, coarse, flow, out, load_sems, save_sems, send, send_c, pool, pool_c, near, handed, handed_c, passed_in, passed_c,
    state, low, high, below, above,
    low_next, high_next, below_next, above_next, first_next, last_next,
    send_sems, recv_sems, relay_send, relay_recv, edge_send, edge_recv, row_send, row_recv,
):
    inner, stride, depth, hops, base_c, extra_c, step_c, inner_c, stride_c, hops_c = sizes
    planes, species, rows, depth_z = fine.shape
    half_z = depth_z // 2
    groups, devices = lax.axis_size("grp"), lax.axis_size("dev")
    part = devices // 2
    late = stride - depth
    wide = [cross // part + (1 if k < cross % part else 0) for k in range(part)]
    wide_c = [base_c + (step_c if k < extra_c else 0) for k in range(part)]
    caps = wide + [inner] * part
    caps_c = wide_c + [inner_c] * part
    g, me = lax.axis_index("grp"), lax.axis_index("dev")
    base = (me // part) * part
    other = part - base
    seat = lax.rem(me, part)
    barrier = pltpu.get_barrier_semaphore()
    lane_c = lax.broadcasted_iota(jnp.int32, send_c.shape[1:], 2)

    def target(b):
        if b < part:
            return {"dev": other + lax.rem(seat + b, part)}
        return {"dev": base + lax.rem(seat + b - part, part)}

    def greet(to):
        pl.semaphore_signal(barrier, inc=1, device_id=to, device_id_type=MESH)

    loads = [
        pltpu.make_async_copy(source, into, load_sems.at[i])
        for i, (source, into) in enumerate(((fine_hbm, fine), (coarse_hbm, coarse), (flow_hbm, flow)))
    ]
    for load in loads:
        load.start()
    peers = list(range(part + 1, devices)) + list(range(part))
    for b in peers:
        greet(target(b))
    greet({"grp": lax.rem(g + 1, groups)})
    greet({"grp": lax.rem(g + groups - 1, groups)})
    pl.semaphore_wait(barrier, devices + 1)

    def remote(source, into, sems, at, to):
        return pltpu.make_async_remote_copy(
            src_ref=source,
            dst_ref=into,
            send_sem=sems[0].at[at],
            recv_sem=sems[1].at[at],
            device_id=to,
            device_id_type=MESH,
        )

    def pack(first, count, into, offset):
        def step(k, carry):
            into[offset + k] = fine[tables[0, first + k]]
            return carry

        lax.fori_loop(0, count, step, 0)

    def pack_coarse_pairs(first, count, into):
        def step(k, carry):
            into[first + k, :, :, 0:half_z] = coarse[tables[3, 2 * (first + k)]]
            into[first + k, :, :, half_z:depth_z] = coarse[tables[3, 2 * (first + k) + 1]]
            return carry

        lax.fori_loop(0, count, step, 0)

    sems = (send_sems, recv_sems)
    pairs_c = stride_c // 2
    coarse_moves, early_moves = [], []
    begin = devices * late
    near_by, far = peers[: part - 1], peers[part - 1 :]

    def send_coarse(b):
        count = caps_c[b] // 2
        first = b * pairs_c + pairs_c - count
        pack_coarse_pairs(first, count, send_c)
        cut = pl.ds(first, count)
        coarse_moves.append(remote(send_c.at[cut], pool_c.at[cut], sems, b, target(b)))
        coarse_moves[-1].start()

    def send_early(b):
        pack(begin + b * depth, depth, send, begin + b * depth)
        early_moves.append(
            remote(
                send.at[pl.ds(begin + b * depth, depth)], near.at[pl.ds(b * depth, depth)],
                sems, devices + b, target(b),
            )
        )
        early_moves[-1].start()

    def late_copy(b):
        cut = pl.ds(b * late, caps[b] - depth)
        return remote(send.at[cut], pool.at[cut], sems, 2 * devices + b, target(b))

    loads[0].wait()
    for b in far[:1]:
        send_early(b)
    loads[1].wait()
    for b in far:
        send_coarse(b)
    for b in far[1:]:
        send_early(b)
    for b in near_by:
        send_coarse(b)
        send_early(b)
        pack(b * late, inner - depth, send, b * late)
        late_copy(b).start()
    pack_coarse_pairs(part * pairs_c + pairs_c - inner_c // 2, inner_c // 2, pool_c)
    pack(begin + part * depth, depth, near, part * depth)
    pack(part * late, inner - depth, pool, part * late)
    for move in coarse_moves:
        move.wait_recv()

    def half_of(slot, odd):
        value = pool_c[slot // 2]
        turned = pltpu.roll(value, half_z, 2)
        return jnp.where(slot % 2 == odd, value, turned)

    def relay_coarse(k, carry):
        left = half_of(tables[4, 2 * k], 0)
        right = half_of(tables[4, 2 * k + 1], 1)
        handed_c[k] = jnp.where(lane_c < half_z, left, right)
        return carry

    sends_c = hops_c // 2
    relay_sems = (relay_send, relay_recv)
    lax.fori_loop(0, (part - 1) * sends_c, relay_coarse, 0)
    relays_c = []
    for k in range(1, part):
        cut = pl.ds((k - 1) * sends_c, sends_c)
        relays_c.append(remote(handed_c.at[cut], passed_c.at[cut], relay_sems, k, target(part + k)))
        relays_c[-1].start()
    for b in far:
        pack(b * late, caps[b] - depth, send, b * late)
    outer = (me < part // 2) | (me >= devices - part // 2)

    @pl.when(jnp.logical_not(outer))
    def _():
        for b in far:
            late_copy(b).start()

    for move in early_moves:
        move.wait_recv()

    passed = (part - 1) * hops

    def relay(k, carry):
        handed[k] = near[jnp.maximum(tables[1, k] - begin, 0)]
        return carry

    lax.fori_loop(0, passed, relay, 0)
    relays = []
    for k in range(1, part):
        cut = pl.ds((k - 1) * hops, hops)
        relays.append(
            remote(handed.at[cut], passed_in.at[cut], relay_sems, part + k, target(part + k))
        )
        relays[-1].start()

    @pl.when(outer)
    def _():
        for b in far:
            late_copy(b).start()

    late_moves = [late_copy(b) for b in peers]

    def keep_near(k, carry):
        pool[begin + k] = near[k]
        return carry

    lax.fori_loop(0, devices * depth, keep_near, 0)
    for move in relays_c:
        move.wait_recv()

    def keep_coarse(k, carry):
        pool_c[devices * pairs_c + k] = passed_c[k]
        return carry

    lax.fori_loop(0, (part - 1) * sends_c, keep_coarse, 0)
    arrivals = devices * stride
    refine_into(tables, 5, pool_c, weights, pool, arrivals + passed, coarse.shape[0])
    for move in late_moves + relays:
        move.wait_recv()

    def keep_passed(k, carry):
        pool[arrivals + k] = passed_in[k]
        return carry

    lax.fori_loop(0, passed, keep_passed, 0)

    def assemble(p, carry):
        at = tables[2, p]
        for s in range(species):
            value = pool[at, s]
            state[p + 1, s] = value
            low[s, pl.ds(p, 1), :] = value[0:1]
            high[s, pl.ds(p, 1), :] = value[rows - 1 : rows]
        return carry

    lax.fori_loop(0, planes, assemble, 0)

    def edge_copy(source, target, at, to):
        return pltpu.make_async_remote_copy(
            src_ref=source,
            dst_ref=target,
            send_sem=edge_send.at[at],
            recv_sem=edge_recv.at[at],
            device_id=to,
            device_id_type=MESH,
        )

    def row_copy(source, target, b, at, to):
        cut = pl.ds(pl.multiple_of(b * 8, 8), 8)
        return pltpu.make_async_remote_copy(
            src_ref=source.at[:, cut],
            dst_ref=target.at[:, cut],
            send_sem=row_send.at[at, b],
            recv_sem=row_recv.at[at, b],
            device_id=to,
            device_id_type=MESH,
        )

    left, right = {"dev": me - 1}, {"dev": me + 1}
    down, up = {"grp": g - 1}, {"grp": g + 1}
    ahead = edge_copy(state.at[pl.ds(planes, 1)], state.at[pl.ds(0, 1)], 0, right)
    back = edge_copy(state.at[pl.ds(1, 1)], state.at[pl.ds(planes + 1, 1)], 1, left)
    rise = edge_copy(high, below, 2, up)
    sink = edge_copy(low, above, 3, down)
    has_left, has_right = me > 0, me < devices - 1
    has_down, has_up = g > 0, g < groups - 1

    @pl.when(has_up)
    def _():
        rise.start()

    @pl.when(has_down)
    def _():
        sink.start()

    @pl.when(has_right)
    def _():
        ahead.start()

    @pl.when(has_left)
    def _():
        back.start()

    for move in coarse_moves + relays_c + early_moves + late_moves + relays:
        move.wait_send()

    @pl.when(has_left)
    def _():
        ahead.wait_recv()

    @pl.when(has_right)
    def _():
        back.wait_recv()

    @pl.when(has_down)
    def _():
        rise.wait_recv()

    @pl.when(has_up)
    def _():
        sink.wait_recv()

    @pl.when(has_right)
    def _():
        ahead.wait_send()

    @pl.when(has_left)
    def _():
        back.wait_send()

    @pl.when(has_up)
    def _():
        rise.wait_send()

    @pl.when(has_down)
    def _():
        sink.wait_send()

    @pl.when(me == 0)
    def _():
        state[0] = jnp.zeros(state.shape[1:], state.dtype)

    @pl.when(me == devices - 1)
    def _():
        state[planes + 1] = jnp.zeros(state.shape[1:], state.dtype)

    @pl.when(g == 0)
    def _():
        below[...] = jnp.zeros(below.shape, below.dtype)

    @pl.when(g == groups - 1)
    def _():
        above[...] = jnp.zeros(above.shape, above.dtype)

    row = lax.broadcasted_iota(jnp.int32, (rows, depth_z), 0)
    lane = lax.broadcasted_iota(jnp.int32, (rows, depth_z), 1)


    loads[2].wait()
    next_ahead = edge_copy(out.at[pl.ds(planes - 1, 1)], first_next, 4, right)
    next_back = edge_copy(out.at[pl.ds(0, 1)], last_next, 5, left)
    blocks = planes // 8

    def save(b):
        cut = pl.ds(b * 8, 8)
        return pltpu.make_async_copy(out.at[cut], out_hbm.at[cut], save_sems.at[b])

    def advance_block(turn, carry):
        b = lax.rem(turn + blocks - 1, blocks)

        def advance_plane(k, carry):
            p = b * 8 + k
            coeffs = coefficients(flow, p)
            for s in range(species):
                total = update(
                    diffusion[s], coeffs, state[p + 1, s], state[p, s], state[p + 2, s],
                    below[s, pl.ds(p, 1), :], above[s, pl.ds(p, 1), :], row, lane,
                )
                out[p, s] = total
                low_next[s, pl.ds(p, 1), :] = total[0:1]
                high_next[s, pl.ds(p, 1), :] = total[rows - 1 : rows]
            return carry

        lax.fori_loop(0, 8, advance_plane, 0)
        save(b).start()

        @pl.when(has_up)
        def _():
            row_copy(high_next, below_next, b, 0, up).start()

        @pl.when(has_down)
        def _():
            row_copy(low_next, above_next, b, 1, down).start()

        @pl.when((turn == 0) & has_right)
        def _():
            next_ahead.start()

        @pl.when((turn == 1) & has_left)
        def _():
            next_back.start()

        return carry

    lax.fori_loop(0, blocks, advance_block, 0)

    def settle(b, carry):
        save(b).wait()

        @pl.when(has_down)
        def _():
            row_copy(high_next, below_next, b, 0, up).wait_recv()
            row_copy(low_next, above_next, b, 1, down).wait_send()

        @pl.when(has_up)
        def _():
            row_copy(low_next, above_next, b, 1, down).wait_recv()
            row_copy(high_next, below_next, b, 0, up).wait_send()

        return carry

    lax.fori_loop(0, blocks, settle, 0)

    @pl.when(has_left)
    def _():
        next_ahead.wait_recv()
        next_back.wait_send()
        first_out[...] = first_next[...]

    @pl.when(has_right)
    def _():
        next_back.wait_recv()
        next_ahead.wait_send()
        last_out[...] = last_next[...]

    @pl.when(has_down)
    def _():
        below_out[...] = below_next[...]

    @pl.when(has_up)
    def _():
        above_out[...] = above_next[...]

    @pl.when(me == 0)
    def _():
        first_out[...] = jnp.zeros(first_out.shape, first_out.dtype)

    @pl.when(me == devices - 1)
    def _():
        last_out[...] = jnp.zeros(last_out.shape, last_out.dtype)

    @pl.when(g == 0)
    def _():
        below_out[...] = jnp.zeros(below_out.shape, below_out.dtype)

    @pl.when(g == groups - 1)
    def _():
        above_out[...] = jnp.zeros(above_out.shape, above_out.dtype)


def regrid(cross, sizes, ident, devices, tables, diffusion, fine, coarse, weights, flow):
    inner, stride, depth, hops, base_c, extra_c, step_c, inner_c, stride_c, hops_c = sizes
    planes, species, rows, depth_z = fine.shape
    part = devices // 2
    kept = jax.ShapeDtypeStruct(fine.shape, fine.dtype)
    plane = jax.ShapeDtypeStruct((1,) + fine.shape[1:], fine.dtype)
    edge = jax.ShapeDtypeStruct((species, planes, depth_z), fine.dtype)
    pool = devices * stride + (part - 1) * hops + planes // 2
    pool_c = (devices * stride_c + (part - 1) * hops_c) // 2
    vmem = pl.BlockSpec(memory_space=pltpu.VMEM)
    smem = pl.BlockSpec(memory_space=pltpu.SMEM)
    hbm = pl.BlockSpec(memory_space=pl.ANY)

    def held(count):
        return pltpu.VMEM((count,) + fine.shape[1:], fine.dtype)

    def held_c(count):
        return pltpu.VMEM((count, species, rows // 2, depth_z), fine.dtype)

    def sems(*shape):
        return [pltpu.SemaphoreType.DMA(shape)] * 2

    rim = pltpu.VMEM(edge.shape, edge.dtype)
    passed, passed_c = (part - 1) * hops, (part - 1) * hops_c // 2
    return pl.pallas_call(
        functools.partial(regrid_kernel, cross, sizes),
        out_shape=(kept, plane, plane, edge, edge),
        in_specs=[smem] * 2 + [hbm, hbm, vmem, hbm],
        out_specs=(hbm,) + (vmem,) * 4,
        scratch_shapes=[
            held(planes), pltpu.VMEM(coarse.shape, coarse.dtype), pltpu.VMEM(flow.shape, flow.dtype),
            held(planes), pltpu.SemaphoreType.DMA((3,)), pltpu.SemaphoreType.DMA((planes // 8,)),
            held(devices * stride), held_c(devices * stride_c // 2), held(pool), held_c(pool_c),
            held(devices * depth), held(passed), held_c(passed_c), held(passed), held_c(passed_c),
            held(planes + 2), rim, rim, rim, rim, rim, rim, rim, rim, held(1), held(1),
            *sems(3 * devices), *sems(2 * part), *sems(6), *sems(2, planes // 8),
        ],
        compiler_params=params(collective_id=ident, has_side_effects=True),
        name="regrid",
    )(tables, diffusion, fine, coarse, weights, flow)


def advance_kernel(steps, diffusion, u, before, after, first, last, below, above, flow, out):
    i = pl.program_id(0)
    block, species, rows, depth = u.shape
    row = lax.broadcasted_iota(jnp.int32, (rows, depth), 0)
    lane = lax.broadcasted_iota(jnp.int32, (rows, depth), 1)
    for x in range(block):
        coeffs = coefficients(flow, x)
        for s in range(species):
            if x > 0:
                lo = u[x - 1, s]
            else:
                lo = jnp.where(i == 0, first[0, s], before[0, s])
            if x < block - 1:
                hi = u[x + 1, s]
            else:
                hi = jnp.where(i == steps - 1, last[0, s], after[0, s])
            out[x, s] = update(
                diffusion[s], coeffs, u[x, s], lo, hi,
                below[s, pl.ds(x, 1), :], above[s, pl.ds(x, 1), :], row, lane,
            )


def advance(diffusion, u, first, last, below, above, flow):
    planes, species, rows, depth = u.shape
    block = 16 if planes % 16 == 0 else planes
    steps = planes // block
    edge_spec = pl.BlockSpec((species, block, depth), lambda i: (0, i, 0))
    plane_spec = pl.BlockSpec((1, species, rows, depth), lambda i: (0, 0, 0, 0))
    block_spec = pl.BlockSpec((block, species, rows, depth), lambda i: (i, 0, 0, 0))
    return pl.pallas_call(
        functools.partial(advance_kernel, steps),
        grid=(steps,),
        out_shape=jax.ShapeDtypeStruct(u.shape, u.dtype),
        in_specs=[
            pl.BlockSpec(memory_space=pltpu.SMEM),
            block_spec,
            pl.BlockSpec(
                (1, species, rows, depth), lambda i: (jnp.maximum(i * block - 1, 0), 0, 0, 0)
            ),
            pl.BlockSpec(
                (1, species, rows, depth),
                lambda i: (jnp.minimum(i * block + block, planes - 1), 0, 0, 0),
            ),
            plane_spec,
            plane_spec,
            edge_spec,
            edge_spec,
            pl.BlockSpec((block, 3, rows, depth), lambda i: (i, 0, 0, 0)),
        ],
        out_specs=block_spec,
        compiler_params=params(),
        name="advance",
    )(diffusion, u, u, u, first, last, below, above, flow)


def shift_up(value, axis):
    size = lax.axis_size(axis)
    return lax.ppermute(value, axis, [(i, i + 1) for i in range(size - 1)])


def shift_down(value, axis):
    size = lax.axis_size(axis)
    return lax.ppermute(value, axis, [(i + 1, i) for i in range(size - 1)])


def rims(u):
    rows = u.shape[2]
    below = shift_up(jnp.swapaxes(u[:, :, rows - 1], 0, 1), "grp")
    above = shift_down(jnp.swapaxes(u[:, :, 0], 0, 1), "grp")
    return shift_up(u[-1:], "dev"), shift_down(u[:1], "dev"), below, above


def on_device(old_fine, old_ids, old_coarse, coarse_ids, velocity, diffusion):
    devices = lax.axis_size("dev")
    group_count = lax.axis_size("grp")
    me = lax.axis_index("dev")
    planes = old_fine.shape[0]
    coarse_planes = old_coarse.shape[0]
    capacity = max(2, 2 * planes // devices)
    coarse_capacity = max(2, 2 * coarse_planes // devices)
    both = jnp.concatenate([old_ids[0], coarse_ids[0]])
    relaying = capacity >= 16 and devices % 2 == 0 and planes % 8 == 0 and group_count > 2
    if relaying:
        groups = gather_ids(both, group_count, devices)
    else:
        groups = lax.all_gather(both, ("grp", "dev")).reshape(group_count, devices, -1)
    weights = spread_weights(old_coarse.shape[3])

    def padded(fine, coarse):
        here = (jnp.arange(group_count) == lax.axis_index("grp"))[:, None, None]
        both_all = jnp.max(jnp.where(here, groups, -1), axis=0)
        own = jnp.max(jnp.where((jnp.arange(devices) == me)[:, None], both_all, -1), axis=0)
        coarse_send = send_table(own[planes:], coarse_planes, devices, coarse_capacity)
        coarse_table = receive_table(both_all[:, planes:], coarse_planes, coarse_capacity, me)
        coarse_out = pack_coarse(coarse_send, coarse)
        coarse_in = lax.all_to_all(coarse_out, "dev", split_axis=0, concat_axis=0, tiled=True)
        send = send_table(own[:planes], planes, devices, capacity)
        table = receive_table(both_all[:, :planes], planes, capacity, me)
        arrived = lax.all_to_all(pack_fine(send, fine), "dev", split_axis=0, concat_axis=0, tiled=True)
        interp = refine(coarse_table[None], coarse_in, weights)
        u = assemble(table, arrived, interp)
        u = advance(diffusion, u, *rims(u), velocity)
        return (u,) + rims(u)

    if relaying:
        choices = [capacity * k // 16 for k in CROSS]
        sizes = tuple(capacity * k // 16 for k in FINE) + tuple(coarse_capacity * k // 8 for k in COARSE)
        sizes = sizes[:5] + (1,) + sizes[5:]
        rows = group_count * devices
        flat = groups.reshape(rows, -1)
        place = jnp.stack([lax.axis_index("grp"), me]).astype(jnp.int32)
        tables = plan(
            place, flat[:, :planes], flat[:, planes:], group_count, devices, planes,
            coarse_planes, sizes, choices,
        )

        def relayed(count, ident, fine, coarse):
            return regrid(
                count, sizes, ident, devices, tables, diffusion, fine, coarse, weights, velocity
            )

        branches = [
            functools.partial(relayed, count, 1 + k) for k, count in enumerate(choices)
        ]
        state = lax.switch(tables[6, 0], branches + [padded], old_fine, old_coarse)
    else:
        state = padded(old_fine, old_coarse)
    return advance(diffusion, *state, velocity)


def solution(mesh):
    in_specs = (
        P("dev", None, "grp", None),
        P("grp", "dev"),
        P("dev", None, "grp", None),
        P("grp", "dev"),
        P("dev", None, "grp", None),
        P(),
    )
    out_specs = P("dev", None, "grp", None)
    return jax.shard_map(
        on_device, mesh=mesh, in_specs=in_specs, out_specs=out_specs, check_vma=False
    )
```

```python
import functools

import jax
import jax.numpy as jnp
from jax import lax
from jax.experimental import pallas as pl
from jax.experimental.pallas import tpu as pltpu
from jax.sharding import PartitionSpec as P

CROSS = (32, 33, 34, 35, 36, 37, 38, 40, 44)
LOOSE = 40
FINE = (10, 11, 6, 6)
COARSE = (4, 2, 6, 6, 4)
VMEM_LIMIT = 48 * 1024 * 1024
MESH = pl.DeviceIdType.MESH


def params(**more):
    return pltpu.CompilerParams(vmem_limit_bytes=VMEM_LIMIT, **more)


def earlier_count(mask):
    count = mask.shape[-1]
    lower = jnp.arange(count)[None, :] < jnp.arange(count)[:, None]
    return jnp.sum((mask[..., None, :] & lower).astype(jnp.int32), axis=-1)


def send_table(labels, block_len, devices, capacity):
    target = jnp.where(labels >= 0, labels // block_len, -1)
    count = labels.shape[0]
    same = target[None, :] == target[:, None]
    lower = jnp.arange(count)[None, :] < jnp.arange(count)[:, None]
    rank = jnp.sum((same & lower).astype(jnp.int32), axis=1)
    slot = jnp.where(labels >= 0, target * capacity + rank, -1)
    hits = slot[None, :] == jnp.arange(devices * capacity)[:, None]
    return jnp.max(jnp.where(hits, jnp.arange(count)[None, :], 0), axis=1)


def receive_table(labels_all, block_len, capacity, me):
    devices, count = labels_all.shape
    within = labels_all - me * block_len
    valid = (within >= 0) & (within < block_len)
    slot = jnp.arange(devices)[:, None] * capacity + earlier_count(valid)
    flat_within = jnp.where(valid, within, -1).reshape(-1)
    hits = flat_within[None, :] == jnp.arange(block_len)[:, None]
    return jnp.max(jnp.where(hits, slot.reshape(-1)[None, :], -1), axis=1)


def same_dim(a, b, exact=None):
    return lax.dot_general(
        a, b, (((1,), (1,)), ((), ())), precision=exact,
        preferred_element_type=jnp.float32,
    )


def plain_dot(a, b):
    return jnp.dot(a, b, preferred_element_type=jnp.float32)


def as_float(mask):
    return jnp.where(mask, 1.0, 0.0)


def stacked(masks, right):
    out = plain_dot(jnp.concatenate(masks, axis=0), right)
    size = masks[0].shape[0]
    return [out[i * size : (i + 1) * size] for i in range(len(masks))]


def route(owner, devices, base, extra, step, inner, stride, depth, hops):
    shape = owner.shape
    rows, count = shape
    part = devices // 2
    src = lax.rem(lax.broadcasted_iota(jnp.int32, shape, 0), devices)
    home, spot0 = src // part, lax.rem(src, part)
    first = lax.broadcasted_iota(jnp.int32, (count, count), 0)
    second = lax.broadcasted_iota(jnp.int32, (count, count), 1)
    before = as_float(first < second)
    ones = jnp.ones((count, count), jnp.float32)
    masks = [as_float(owner == e) for e in range(devices)]
    ranks = stacked(masks, before)
    counts = [c.astype(jnp.int32) for c in stacked(masks, ones)]
    rank = sum(m * r for m, r in zip(masks, ranks)).astype(jnp.int32)
    caps = []
    for v in range(devices):
        turn = lax.rem(v + part - spot0, part)
        wide = base + jnp.where(turn < extra, step, 0)
        caps.append(jnp.where(home != v // part, wide, inner))
    limit = sum(jnp.where(owner == v, caps[v], 0) for v in range(devices))
    valid = owner >= 0
    over = valid & (rank >= limit)
    side = jnp.where(valid, owner // part, -1)
    orders = stacked([as_float(over & (side == h)) for h in range(2)], before)
    order = jnp.where(side == 0, orders[0], orders[1]).astype(jnp.int32)
    lent_via = jnp.full(shape, -1, jnp.int32)
    lent_spot = jnp.zeros(shape, jnp.int32)
    for h in range(2):
        passed = jnp.zeros(shape, jnp.int32)
        seek = jnp.where(over & (side == h), order, -1)
        for l in range(stride - 1, -1, -1):
            for v in range(h * part, (h + 1) * part):
                free = (counts[v] <= l) & (caps[v] > l)
                hit = free & (seek == passed)
                lent_via = jnp.where(hit, v, lent_via)
                lent_spot = jnp.where(hit, l, lent_spot)
                passed = passed + jnp.where(free, 1, 0)
    via = jnp.where(over, lent_via, owner)
    spot = jnp.where(over, lent_spot, rank)
    relayed = over & (via >= 0) & (via != owner)
    limit_via = sum(jnp.where(via == v, caps[v], 0) for v in range(devices))
    deep = relayed & (spot < limit_via - depth)
    bad = (over & (lent_via < 0)) | deep
    lanes = [
        (v, e) for v in range(devices) for e in range(devices)
        if v != e and v // part == e // part
    ]
    hops_at = [as_float(relayed & (via == v) & (owner == e)) for v, e in lanes]
    inside = stacked(hops_at, before)
    total = stacked(hops_at, jnp.ones((count, 128), jnp.float32))
    lane = lax.broadcasted_iota(jnp.int32, (rows, 128), 1)
    table = sum(jnp.where(lane == i, t, 0.0) for i, t in enumerate(total))
    up = lax.broadcasted_iota(jnp.int32, (rows, rows), 0)
    across = lax.broadcasted_iota(jnp.int32, (rows, rows), 1)
    earlier = as_float((up // devices == across // devices) & (across < up))
    ahead = plain_dot(earlier, table)
    index = jnp.zeros(shape, jnp.float32)
    for i, m in enumerate(hops_at):
        index = index + m * (inside[i] + ahead[:, i : i + 1])
    crowded = jnp.max(ahead + table, axis=(0, 1), keepdims=True) > float(hops)
    fault = jnp.max(as_float(bad), axis=(0, 1), keepdims=True) > 0.0
    broken = jnp.where(crowded | fault, 1, 0)
    return via, spot, relayed, index.astype(jnp.int32), caps, broken


def widest_load(owner, devices):
    part = devices // 2
    src = lax.rem(lax.broadcasted_iota(jnp.int32, owner.shape, 0), devices)
    away = (owner >= 0) & (owner // part != src // part)
    load = jnp.sum(as_float(away), axis=1, keepdims=True)
    return jnp.max(load, axis=0, keepdims=True)


def plan_kernel(
    groups, devices, block_len, coarse_len, sizes, choices, loose,
    place, fine_ids, coarse_ids, out, via_ref, where_ref, kind_ref, owner_ref, inner_ref,
):
    inner, stride, depth, hops, base_c, extra_c, step_c, inner_c, stride_c, hops_c = sizes
    part = devices // 2
    g, me = place[0], place[1]
    fine, coarse = fine_ids[...], coarse_ids[...]
    rows, count = fine.shape
    count_c = coarse.shape[1]
    width = out.shape[1]
    owner = jnp.where(fine >= 0, fine // block_len, -1)
    load = widest_load(owner, devices)
    pick = sum(jnp.where(load > float(c), 1, 0) for c in choices)[0, 0]

    both = jnp.where(fine >= 0, lax.rem(fine, block_len) // 2, -1)
    kind = lax.broadcasted_iota(jnp.int32, (devices, count), 0)
    cell = lax.broadcasted_iota(jnp.int32, (coarse_len, count), 0)
    cell_c = lax.broadcasted_iota(jnp.int32, (coarse_len, count_c), 0)
    kind_c = lax.broadcasted_iota(jnp.int32, (devices, count_c), 0)
    owner_c = coarse // coarse_len
    within_c = lax.rem(coarse, coarse_len)
    needed = []
    for k in range(groups):
        held = jnp.zeros((devices, coarse_len), jnp.float32)
        for s in range(devices):
            r = k * devices + s
            held = held + same_dim(
                as_float(owner[r : r + 1] == kind), as_float(both[r : r + 1] == cell)
            )
        for s in range(devices):
            r = k * devices + s
            seen = plain_dot(held, as_float(within_c[r : r + 1] == cell_c))
            seen = jnp.where(owner_c[r : r + 1] == kind_c, seen, 0.0)
            needed.append(jnp.sum(seen, axis=0, keepdims=True))
    needed = jnp.concatenate(needed, axis=0) < 1.5
    owner_c = jnp.where(needed, owner_c, -1)

    def assign(owner, ids, length, stride, hops, depth, base, extra, step, inner):
        via, spot, relayed, index, caps, broken = route(
            owner, devices, base, extra, step, inner, stride, depth, hops
        )
        n = owner.shape[1]
        src = lax.rem(lax.broadcasted_iota(jnp.int32, owner.shape, 0), devices)
        turn = lax.rem(lax.rem(via, part) + part - lax.rem(src, part), part)
        block = jnp.where(via // part != src // part, turn, part + turn)
        cap = sum(jnp.where(via == v, caps[v], 0) for v in range(devices))
        late = stride - depth
        early = spot >= cap - depth
        flat = jnp.where(
            early, devices * late + block * depth + spot - (cap - depth), block * late + spot
        )
        via_ref[:, 0:n] = jnp.where(relayed, via, -1)
        where_ref[:, 0:n] = jnp.where(via >= 0, flat, -1)
        kind_ref[:, 0:n] = index
        owner_ref[:, 0:n] = owner
        inner_ref[:, 0:n] = ids - me * length
        return broken

    def tables(n, stride, hops, start):
        arrivals = devices * stride
        passed = (part - 1) * hops
        small = max(n, arrivals + passed + 1) <= 256
        exact = None if small else lax.Precision.HIGHEST
        mine = pl.ds(pl.multiple_of(g * devices, devices), devices)
        via_g = via_ref[mine, 0:n]
        flat_g = where_ref[mine, 0:n]
        index_g = kind_ref[mine, 0:n]
        owner_g = owner_ref[mine, 0:n]
        inner_g = inner_ref[mine, 0:n]
        source = lax.broadcasted_iota(jnp.int32, (devices, n), 0)
        own = jnp.max(jnp.where(source == me, flat_g, -1), axis=0, keepdims=True)
        slots = lax.broadcasted_iota(jnp.int32, (width, n), 0)
        place_at = lax.broadcasted_iota(jnp.int32, (devices, n), 1).astype(jnp.float32)
        send = same_dim(place_at, as_float(own == slots), exact)
        seat = lax.rem(me, part)
        lane = lax.rem(owner_g + 2 * part - seat, part) - 1
        handed = jnp.where(via_g == me, lane * hops + index_g, -1)
        back = lax.rem(seat + part - lax.rem(jnp.maximum(via_g, 0), part), part) - 1
        spot_at = jnp.where(via_g >= 0, arrivals + back * hops + index_g, flat_g)
        inside = jnp.where(owner_g == me, inner_g, -1)
        flat_f = flat_g.astype(jnp.float32)
        spot_f = spot_at.astype(jnp.float32) + 1.0
        relay = jnp.zeros((devices, width), jnp.float32)
        final = jnp.zeros((devices, width), jnp.float32)
        for s in range(devices):
            relay = relay + same_dim(
                jnp.broadcast_to(flat_f[s : s + 1], (devices, n)),
                as_float(handed[s : s + 1] == slots), exact,
            )
            final = final + same_dim(
                jnp.broadcast_to(spot_f[s : s + 1], (devices, n)),
                as_float(inside[s : s + 1] == slots), exact,
            )
        at = lax.broadcasted_iota(jnp.int32, (devices, width), 1)
        whole = (final + 0.5).astype(jnp.int32)
        missing = start + (at // 2 if start else 0)
        whole = jnp.where(whole > 0, whole - 1, missing)
        return [(send + 0.5).astype(jnp.int32), (relay + 0.5).astype(jnp.int32), whole]

    broken_c = assign(
        owner_c, coarse, coarse_len, stride_c, hops_c, stride_c, base_c, extra_c, step_c, inner_c,
    )
    parts_c = tables(count_c, stride_c, hops_c, 0)

    def attempt(carry):
        pick, _ = carry
        wide = sum(jnp.where(pick == i, c, 0) for i, c in enumerate(choices))
        broken = assign(
            owner, fine, block_len, stride, hops, depth, wide // part, lax.rem(wide, part), 1,
            inner + jnp.where(wide >= loose, 1, 0),
        )
        return pick + 1, broken[0, 0]

    def again(carry):
        return (carry[1] > 0) & (carry[0] < len(choices))

    after, broken = lax.while_loop(again, attempt, (pick, jnp.int32(1)))
    fill = devices * stride + (part - 1) * hops
    parts = tables(count, stride, hops, fill)
    pick = jnp.where((broken > 0) | (broken_c[0, 0] > 0), len(choices), after - 1)
    parts = parts + parts_c
    for i, value in enumerate(parts):
        out[i : i + 1] = value[0:1]
    out[len(parts) : len(parts) + 1] = jnp.zeros((1, width), jnp.int32) + pick


def plan(place, fine_ids, coarse_ids, groups, devices, block_len, coarse_len, sizes, choices, loose):
    rows, count = fine_ids.shape
    longest = max(devices * sizes[1], devices * sizes[8], count, (devices // 2) * max(sizes[3], sizes[9]))
    width = -(-longest // 128) * 128
    cells = pltpu.VMEM((rows, max(count, coarse_ids.shape[1])), jnp.int32)
    return pl.pallas_call(
        functools.partial(
            plan_kernel, groups, devices, block_len, coarse_len, sizes, choices, loose
        ),
        out_shape=jax.ShapeDtypeStruct((8, width), jnp.int32),
        in_specs=[
            pl.BlockSpec(memory_space=pltpu.SMEM),
            pl.BlockSpec(memory_space=pltpu.VMEM),
            pl.BlockSpec(memory_space=pltpu.VMEM),
        ],
        out_specs=pl.BlockSpec(memory_space=pltpu.VMEM),
        scratch_shapes=[cells] * 5,
        compiler_params=params(),
        name="plan",
    )(place, fine_ids, coarse_ids)


def pack_fine_kernel(table, source, out, sem):
    def send(i, carry):
        pltpu.make_async_copy(source.at[table[i]], out.at[i], sem).start()
        return carry

    lax.fori_loop(0, out.shape[0], send, 0)
    pltpu.make_async_copy(out, out, sem).wait()


def pack_fine(table, fine):
    return pl.pallas_call(
        pack_fine_kernel,
        out_shape=jax.ShapeDtypeStruct((table.shape[0],) + fine.shape[1:], fine.dtype),
        in_specs=[
            pl.BlockSpec(memory_space=pltpu.SMEM),
            pl.BlockSpec(memory_space=pltpu.VMEM),
        ],
        out_specs=pl.BlockSpec(memory_space=pl.ANY),
        scratch_shapes=[pltpu.SemaphoreType.DMA],
        compiler_params=params(),
        name="pack_fine",
    )(table, fine)


def pack_coarse_kernel(table, source, out):
    half = source.shape[-1]

    def step(i, carry):
        out[i, :, :, 0:half] = source[table[2 * i]]
        out[i, :, :, half : 2 * half] = source[table[2 * i + 1]]
        return carry

    lax.fori_loop(0, out.shape[0], step, 0)


def pack_coarse(table, coarse):
    shape = (table.shape[0] // 2,) + coarse.shape[1:3] + (2 * coarse.shape[3],)
    return pl.pallas_call(
        pack_coarse_kernel,
        out_shape=jax.ShapeDtypeStruct(shape, coarse.dtype),
        in_specs=[
            pl.BlockSpec(memory_space=pltpu.SMEM),
            pl.BlockSpec(memory_space=pltpu.VMEM),
        ],
        out_specs=pl.BlockSpec(memory_space=pltpu.VMEM),
        compiler_params=params(),
        name="pack_coarse",
    )(table, coarse)


def refine_into(table, which, pairs, weights, out, offset, count):
    species, rows, depth = pairs.shape[1:]
    half = depth // 2
    lane = lax.broadcasted_iota(jnp.int32, (species * rows, depth), 1)
    row = lax.broadcasted_iota(jnp.int32, (species, rows, depth), 1)

    def step(c, carry):
        slot = jnp.maximum(table[which, c], 0)
        block = pairs[slot // 2].reshape(species * rows, depth)
        odd = slot % 2
        block = jnp.where((lane >= half).astype(jnp.int32) == odd, block, 0.0)
        spread = jnp.dot(
            block, weights[...], precision=lax.Precision.HIGHEST,
            preferred_element_type=jnp.float32,
        )
        plain = spread[:, :depth].reshape(species, rows, depth)
        sloped = spread[:, depth:].reshape(species, rows, depth)
        below = jnp.where(row == 0, plain, pltpu.roll(plain, 1, 1))
        above = jnp.where(row == rows - 1, plain, pltpu.roll(plain, rows - 1, 1))
        slope = 0.125 * (above - below)
        for s in range(species):
            out[offset + c, s, pl.ds(0, rows, 2), :] = sloped[s] - slope[s]
            out[offset + c, s, pl.ds(1, rows, 2), :] = sloped[s] + slope[s]
        return carry

    lax.fori_loop(0, count, step, 0)


def refine_kernel(table, pairs, weights, out):
    refine_into(table, 0, pairs, weights, out, 0, out.shape[0])


def spread_weights(half):
    depth = 2 * half
    coarse = jnp.arange(half)[:, None]
    fine = jnp.arange(depth)[None, :]
    centre = (fine // 2 == coarse).astype(jnp.float32)
    up = (jnp.minimum(fine // 2 + 1, half - 1) == coarse).astype(jnp.float32)
    down = (jnp.maximum(fine // 2 - 1, 0) == coarse).astype(jnp.float32)
    side = jnp.where(fine % 2 == 1, 0.125, -0.125)
    both = jnp.concatenate([centre, centre + side * (up - down)], axis=1)
    return jnp.concatenate([both, both], axis=0)


def refine(table, pairs, weights):
    species, rows, depth = pairs.shape[1:]
    return pl.pallas_call(
        refine_kernel,
        out_shape=jax.ShapeDtypeStruct(
            (table.shape[1], species, 2 * rows, depth), pairs.dtype
        ),
        in_specs=[
            pl.BlockSpec(memory_space=pltpu.SMEM),
            pl.BlockSpec(memory_space=pltpu.VMEM),
            pl.BlockSpec(memory_space=pltpu.VMEM),
        ],
        out_specs=pl.BlockSpec(memory_space=pltpu.VMEM),
        compiler_params=params(),
        cost_estimate=pl.CostEstimate(
            flops=40_000_000, bytes_accessed=30_000_000, transcendentals=0
        ),
        name="refine",
    )(table, pairs, weights)


def assemble_kernel(table, arrived, interp, out, sem):
    def fetch(p, carry):
        slot = table[p]

        @pl.when(slot >= 0)
        def _():
            pltpu.make_async_copy(arrived.at[slot], out.at[p], sem).start()

        @pl.when(slot < 0)
        def _():
            pltpu.make_async_copy(interp.at[p // 2], out.at[p], sem).start()

        return carry

    lax.fori_loop(0, out.shape[0], fetch, 0)
    pltpu.make_async_copy(out, out, sem).wait()


def assemble(table, arrived, interp):
    return pl.pallas_call(
        assemble_kernel,
        out_shape=jax.ShapeDtypeStruct((table.shape[0],) + arrived.shape[1:], arrived.dtype),
        in_specs=[
            pl.BlockSpec(memory_space=pltpu.SMEM),
            pl.BlockSpec(memory_space=pl.ANY),
            pl.BlockSpec(memory_space=pl.ANY),
        ],
        out_specs=pl.BlockSpec(memory_space=pltpu.VMEM),
        scratch_shapes=[pltpu.SemaphoreType.DMA],
        compiler_params=params(),
        name="assemble",
    )(table, arrived, interp)


def gather_kernel(groups, devices, mine, out, send_sems, recv_sems):
    total = groups * devices
    me = lax.axis_index("grp") * devices + lax.axis_index("dev")
    barrier = pltpu.get_barrier_semaphore()

    def place(k):
        to = lax.rem(me + k, total)
        return {"grp": to // devices, "dev": lax.rem(to, devices)}

    def greet(k, carry):
        pl.semaphore_signal(barrier, inc=1, device_id=place(k), device_id_type=MESH)
        return carry

    lax.fori_loop(1, total, greet, 0)
    pl.semaphore_wait(barrier, total - 1)

    def copy(k):
        return pltpu.make_async_remote_copy(
            src_ref=mine,
            dst_ref=out.at[me],
            send_sem=send_sems.at[k],
            recv_sem=recv_sems.at[k],
            device_id=place(k),
            device_id_type=MESH,
        )

    def start(k, carry):
        copy(k).start()
        return carry

    def finish(k, carry):
        copy(k).wait_send()
        source = lax.rem(me + total - k, total)
        pltpu.make_async_remote_copy(
            src_ref=mine,
            dst_ref=out.at[source],
            send_sem=send_sems.at[k],
            recv_sem=recv_sems.at[k],
            device_id=place(k),
            device_id_type=MESH,
        ).wait_recv()
        return carry

    lax.fori_loop(1, total, start, 0)
    out[me] = mine[...]
    lax.fori_loop(1, total, finish, 0)


def gather_ids(both, groups, devices):
    width = both.shape[0]
    padded = -(-width // 128) * 128
    mine = jnp.pad(both, (0, padded - width))[None]
    total = groups * devices
    out = pl.pallas_call(
        functools.partial(gather_kernel, groups, devices),
        out_shape=jax.ShapeDtypeStruct((total, 1, padded), both.dtype),
        in_specs=[pl.BlockSpec(memory_space=pltpu.VMEM)],
        out_specs=pl.BlockSpec(memory_space=pltpu.VMEM),
        scratch_shapes=[
            pltpu.SemaphoreType.DMA((total,)),
            pltpu.SemaphoreType.DMA((total,)),
        ],
        compiler_params=pltpu.CompilerParams(collective_id=0, has_side_effects=True),
        name="gather_ids",
    )(mine)
    return out.reshape(groups, devices, padded)[:, :, :width]


def coefficients(flow, x):
    v = [flow[x, k] for k in range(3)]
    plus = [jnp.maximum(w, 0.0) for w in v]
    minus = [jnp.maximum(-w, 0.0) for w in v]
    rest = 1.0
    for k in range(3):
        rest = rest - plus[k] - minus[k]
    return plus, minus, rest


def update(d, coeffs, c, lo, hi, below, above, row, lane):
    rows, depth = c.shape
    plus, minus, rest = coeffs
    ylo = jnp.where(row == 0, below, pltpu.roll(c, 1, 0))
    yhi = jnp.where(row == rows - 1, above, pltpu.roll(c, rows - 1, 0))
    zlo = jnp.where(lane == 0, c, pltpu.roll(c, 1, 1))
    zhi = jnp.where(lane == depth - 1, c, pltpu.roll(c, depth - 1, 1))
    total = (rest - 6.0 * d) * c
    total = total + (plus[0] + d) * lo + (minus[0] + d) * hi
    total = total + (plus[1] + d) * ylo + (minus[1] + d) * yhi
    return total + (plus[2] + d) * zlo + (minus[2] + d) * zhi


def regrid_kernel(
    cross, sizes, tables, diffusion, fine_hbm, coarse_hbm, weights, flow_hbm,
    out_hbm, first_out, last_out, below_out, above_out,
    fine, coarse, flow, out, load_sems, save_sems, send, send_c, pool, pool_c, near, handed, handed_c, passed_in, passed_c,
    state, low, high, below, above,
    low_next, high_next, below_next, above_next, first_next, last_next,
    send_sems, recv_sems, relay_send, relay_recv, edge_send, edge_recv, row_send, row_recv,
):
    inner, stride, depth, hops, base_c, extra_c, step_c, inner_c, stride_c, hops_c = sizes
    planes, species, rows, depth_z = fine.shape
    half_z = depth_z // 2
    groups, devices = lax.axis_size("grp"), lax.axis_size("dev")
    part = devices // 2
    late = stride - depth
    wide = [cross // part + (1 if k < cross % part else 0) for k in range(part)]
    wide_c = [base_c + (step_c if k < extra_c else 0) for k in range(part)]
    caps = wide + [inner] * part
    caps_c = wide_c + [inner_c] * part
    g, me = lax.axis_index("grp"), lax.axis_index("dev")
    base = (me // part) * part
    other = part - base
    seat = lax.rem(me, part)
    barrier = pltpu.get_barrier_semaphore()
    lane_c = lax.broadcasted_iota(jnp.int32, send_c.shape[1:], 2)

    def target(b):
        if b < part:
            return {"dev": other + lax.rem(seat + b, part)}
        return {"dev": base + lax.rem(seat + b - part, part)}

    def greet(to):
        pl.semaphore_signal(barrier, inc=1, device_id=to, device_id_type=MESH)

    loads = [
        pltpu.make_async_copy(source, into, load_sems.at[i])
        for i, (source, into) in enumerate(((fine_hbm, fine), (coarse_hbm, coarse), (flow_hbm, flow)))
    ]
    for load in loads:
        load.start()
    peers = list(range(part + 1, devices)) + list(range(part))
    for b in peers:
        greet(target(b))
    greet({"grp": lax.rem(g + 1, groups)})
    greet({"grp": lax.rem(g + groups - 1, groups)})
    pl.semaphore_wait(barrier, devices + 1)

    def remote(source, into, sems, at, to):
        return pltpu.make_async_remote_copy(
            src_ref=source,
            dst_ref=into,
            send_sem=sems[0].at[at],
            recv_sem=sems[1].at[at],
            device_id=to,
            device_id_type=MESH,
        )

    def pack(first, count, into, offset):
        def step(k, carry):
            into[offset + k] = fine[tables[0, first + k]]
            return carry

        lax.fori_loop(0, count, step, 0)

    def pack_coarse_pairs(first, count, into):
        def step(k, carry):
            into[first + k, :, :, 0:half_z] = coarse[tables[3, 2 * (first + k)]]
            into[first + k, :, :, half_z:depth_z] = coarse[tables[3, 2 * (first + k) + 1]]
            return carry

        lax.fori_loop(0, count, step, 0)

    sems = (send_sems, recv_sems)
    pairs_c = stride_c // 2
    coarse_moves, early_moves = [], []
    begin = devices * late
    near_by, far = peers[: part - 1], peers[part - 1 :]

    def send_coarse(b):
        count = caps_c[b] // 2
        first = b * pairs_c + pairs_c - count
        pack_coarse_pairs(first, count, send_c)
        cut = pl.ds(first, count)
        coarse_moves.append(remote(send_c.at[cut], pool_c.at[cut], sems, b, target(b)))
        coarse_moves[-1].start()

    def send_early(b):
        pack(begin + b * depth, depth, send, begin + b * depth)
        early_moves.append(
            remote(
                send.at[pl.ds(begin + b * depth, depth)], near.at[pl.ds(b * depth, depth)],
                sems, devices + b, target(b),
            )
        )
        early_moves[-1].start()

    def late_copy(b):
        cut = pl.ds(b * late, caps[b] - depth)
        return remote(send.at[cut], pool.at[cut], sems, 2 * devices + b, target(b))

    loads[0].wait()
    for b in far[:1]:
        send_early(b)
    loads[1].wait()
    for b in far:
        send_coarse(b)
    for b in far[1:]:
        send_early(b)
    for b in near_by:
        send_coarse(b)
        send_early(b)
        pack(b * late, inner - depth, send, b * late)
        late_copy(b).start()
    pack_coarse_pairs(part * pairs_c + pairs_c - inner_c // 2, inner_c // 2, pool_c)
    pack(begin + part * depth, depth, near, part * depth)
    pack(part * late, inner - depth, pool, part * late)
    for move in coarse_moves:
        move.wait_recv()

    def half_of(slot, odd):
        value = pool_c[slot // 2]
        turned = pltpu.roll(value, half_z, 2)
        return jnp.where(slot % 2 == odd, value, turned)

    def relay_coarse(k, carry):
        left = half_of(tables[4, 2 * k], 0)
        right = half_of(tables[4, 2 * k + 1], 1)
        handed_c[k] = jnp.where(lane_c < half_z, left, right)
        return carry

    sends_c = hops_c // 2
    relay_sems = (relay_send, relay_recv)
    lax.fori_loop(0, (part - 1) * sends_c, relay_coarse, 0)
    relays_c = []
    for k in range(1, part):
        cut = pl.ds((k - 1) * sends_c, sends_c)
        relays_c.append(remote(handed_c.at[cut], passed_c.at[cut], relay_sems, k, target(part + k)))
        relays_c[-1].start()
    for b in far:
        pack(b * late, caps[b] - depth, send, b * late)
    outer = (me < part // 2) | (me >= devices - part // 2)

    @pl.when(jnp.logical_not(outer))
    def _():
        for b in far:
            late_copy(b).start()

    for move in early_moves:
        move.wait_recv()

    passed = (part - 1) * hops

    def relay(k, carry):
        handed[k] = near[jnp.maximum(tables[1, k] - begin, 0)]
        return carry

    lax.fori_loop(0, passed, relay, 0)
    relays = []
    for k in range(1, part):
        cut = pl.ds((k - 1) * hops, hops)
        relays.append(
            remote(handed.at[cut], passed_in.at[cut], relay_sems, part + k, target(part + k))
        )
        relays[-1].start()

    @pl.when(outer)
    def _():
        for b in far:
            late_copy(b).start()

    late_moves = [late_copy(b) for b in peers]

    def keep_near(k, carry):
        pool[begin + k] = near[k]
        return carry

    lax.fori_loop(0, devices * depth, keep_near, 0)
    for move in relays_c:
        move.wait_recv()

    def keep_coarse(k, carry):
        pool_c[devices * pairs_c + k] = passed_c[k]
        return carry

    lax.fori_loop(0, (part - 1) * sends_c, keep_coarse, 0)
    arrivals = devices * stride
    refine_into(tables, 5, pool_c, weights, pool, arrivals + passed, coarse.shape[0])
    for move in late_moves + relays:
        move.wait_recv()

    def keep_passed(k, carry):
        pool[arrivals + k] = passed_in[k]
        return carry

    lax.fori_loop(0, passed, keep_passed, 0)

    def assemble(p, carry):
        at = tables[2, p]
        for s in range(species):
            value = pool[at, s]
            state[p + 1, s] = value
            low[s, pl.ds(p, 1), :] = value[0:1]
            high[s, pl.ds(p, 1), :] = value[rows - 1 : rows]
        return carry

    lax.fori_loop(0, planes, assemble, 0)

    def edge_copy(source, target, at, to):
        return pltpu.make_async_remote_copy(
            src_ref=source,
            dst_ref=target,
            send_sem=edge_send.at[at],
            recv_sem=edge_recv.at[at],
            device_id=to,
            device_id_type=MESH,
        )

    def row_copy(source, target, b, at, to):
        cut = pl.ds(pl.multiple_of(b * 8, 8), 8)
        return pltpu.make_async_remote_copy(
            src_ref=source.at[:, cut],
            dst_ref=target.at[:, cut],
            send_sem=row_send.at[at, b],
            recv_sem=row_recv.at[at, b],
            device_id=to,
            device_id_type=MESH,
        )

    left, right = {"dev": me - 1}, {"dev": me + 1}
    down, up = {"grp": g - 1}, {"grp": g + 1}
    ahead = edge_copy(state.at[pl.ds(planes, 1)], state.at[pl.ds(0, 1)], 0, right)
    back = edge_copy(state.at[pl.ds(1, 1)], state.at[pl.ds(planes + 1, 1)], 1, left)
    rise = edge_copy(high, below, 2, up)
    sink = edge_copy(low, above, 3, down)
    has_left, has_right = me > 0, me < devices - 1
    has_down, has_up = g > 0, g < groups - 1

    @pl.when(has_up)
    def _():
        rise.start()

    @pl.when(has_down)
    def _():
        sink.start()

    @pl.when(has_right)
    def _():
        ahead.start()

    @pl.when(has_left)
    def _():
        back.start()

    for move in coarse_moves + relays_c + early_moves + late_moves + relays:
        move.wait_send()

    @pl.when(has_left)
    def _():
        ahead.wait_recv()

    @pl.when(has_right)
    def _():
        back.wait_recv()

    @pl.when(has_down)
    def _():
        rise.wait_recv()

    @pl.when(has_up)
    def _():
        sink.wait_recv()

    @pl.when(has_right)
    def _():
        ahead.wait_send()

    @pl.when(has_left)
    def _():
        back.wait_send()

    @pl.when(has_up)
    def _():
        rise.wait_send()

    @pl.when(has_down)
    def _():
        sink.wait_send()

    @pl.when(me == 0)
    def _():
        state[0] = jnp.zeros(state.shape[1:], state.dtype)

    @pl.when(me == devices - 1)
    def _():
        state[planes + 1] = jnp.zeros(state.shape[1:], state.dtype)

    @pl.when(g == 0)
    def _():
        below[...] = jnp.zeros(below.shape, below.dtype)

    @pl.when(g == groups - 1)
    def _():
        above[...] = jnp.zeros(above.shape, above.dtype)

    row = lax.broadcasted_iota(jnp.int32, (rows, depth_z), 0)
    lane = lax.broadcasted_iota(jnp.int32, (rows, depth_z), 1)


    loads[2].wait()
    next_ahead = edge_copy(out.at[pl.ds(planes - 1, 1)], first_next, 4, right)
    next_back = edge_copy(out.at[pl.ds(0, 1)], last_next, 5, left)
    blocks = planes // 8

    def save(b):
        cut = pl.ds(b * 8, 8)
        return pltpu.make_async_copy(out.at[cut], out_hbm.at[cut], save_sems.at[b])

    def advance_block(turn, carry):
        b = lax.rem(turn + blocks - 1, blocks)

        def advance_plane(k, carry):
            p = b * 8 + k
            coeffs = coefficients(flow, p)
            for s in range(species):
                total = update(
                    diffusion[s], coeffs, state[p + 1, s], state[p, s], state[p + 2, s],
                    below[s, pl.ds(p, 1), :], above[s, pl.ds(p, 1), :], row, lane,
                )
                out[p, s] = total
                low_next[s, pl.ds(p, 1), :] = total[0:1]
                high_next[s, pl.ds(p, 1), :] = total[rows - 1 : rows]
            return carry

        lax.fori_loop(0, 8, advance_plane, 0)
        save(b).start()

        @pl.when(has_up)
        def _():
            row_copy(high_next, below_next, b, 0, up).start()

        @pl.when(has_down)
        def _():
            row_copy(low_next, above_next, b, 1, down).start()

        @pl.when((turn == 0) & has_right)
        def _():
            next_ahead.start()

        @pl.when((turn == 1) & has_left)
        def _():
            next_back.start()

        return carry

    lax.fori_loop(0, blocks, advance_block, 0)

    def settle(b, carry):
        save(b).wait()

        @pl.when(has_down)
        def _():
            row_copy(high_next, below_next, b, 0, up).wait_recv()
            row_copy(low_next, above_next, b, 1, down).wait_send()

        @pl.when(has_up)
        def _():
            row_copy(low_next, above_next, b, 1, down).wait_recv()
            row_copy(high_next, below_next, b, 0, up).wait_send()

        return carry

    lax.fori_loop(0, blocks, settle, 0)

    @pl.when(has_left)
    def _():
        next_ahead.wait_recv()
        next_back.wait_send()
        first_out[...] = first_next[...]

    @pl.when(has_right)
    def _():
        next_back.wait_recv()
        next_ahead.wait_send()
        last_out[...] = last_next[...]

    @pl.when(has_down)
    def _():
        below_out[...] = below_next[...]

    @pl.when(has_up)
    def _():
        above_out[...] = above_next[...]

    @pl.when(me == 0)
    def _():
        first_out[...] = jnp.zeros(first_out.shape, first_out.dtype)

    @pl.when(me == devices - 1)
    def _():
        last_out[...] = jnp.zeros(last_out.shape, last_out.dtype)

    @pl.when(g == 0)
    def _():
        below_out[...] = jnp.zeros(below_out.shape, below_out.dtype)

    @pl.when(g == groups - 1)
    def _():
        above_out[...] = jnp.zeros(above_out.shape, above_out.dtype)


def regrid(cross, sizes, ident, devices, tables, diffusion, fine, coarse, weights, flow):
    inner, stride, depth, hops, base_c, extra_c, step_c, inner_c, stride_c, hops_c = sizes
    planes, species, rows, depth_z = fine.shape
    part = devices // 2
    kept = jax.ShapeDtypeStruct(fine.shape, fine.dtype)
    plane = jax.ShapeDtypeStruct((1,) + fine.shape[1:], fine.dtype)
    edge = jax.ShapeDtypeStruct((species, planes, depth_z), fine.dtype)
    pool = devices * stride + (part - 1) * hops + planes // 2
    pool_c = (devices * stride_c + (part - 1) * hops_c) // 2
    vmem = pl.BlockSpec(memory_space=pltpu.VMEM)
    smem = pl.BlockSpec(memory_space=pltpu.SMEM)
    hbm = pl.BlockSpec(memory_space=pl.ANY)

    def held(count):
        return pltpu.VMEM((count,) + fine.shape[1:], fine.dtype)

    def held_c(count):
        return pltpu.VMEM((count, species, rows // 2, depth_z), fine.dtype)

    def sems(*shape):
        return [pltpu.SemaphoreType.DMA(shape)] * 2

    rim = pltpu.VMEM(edge.shape, edge.dtype)
    passed, passed_c = (part - 1) * hops, (part - 1) * hops_c // 2
    return pl.pallas_call(
        functools.partial(regrid_kernel, cross, sizes),
        out_shape=(kept, plane, plane, edge, edge),
        in_specs=[smem] * 2 + [hbm, hbm, vmem, hbm],
        out_specs=(hbm,) + (vmem,) * 4,
        scratch_shapes=[
            held(planes), pltpu.VMEM(coarse.shape, coarse.dtype), pltpu.VMEM(flow.shape, flow.dtype),
            held(planes), pltpu.SemaphoreType.DMA((3,)), pltpu.SemaphoreType.DMA((planes // 8,)),
            held(devices * stride), held_c(devices * stride_c // 2), held(pool), held_c(pool_c),
            held(devices * depth), held(passed), held_c(passed_c), held(passed), held_c(passed_c),
            held(planes + 2), rim, rim, rim, rim, rim, rim, rim, rim, held(1), held(1),
            *sems(3 * devices), *sems(2 * part), *sems(6), *sems(2, planes // 8),
        ],
        compiler_params=params(collective_id=ident, has_side_effects=True),
        name="regrid",
    )(tables, diffusion, fine, coarse, weights, flow)


def advance_kernel(steps, diffusion, u, before, after, first, last, below, above, flow, out):
    i = pl.program_id(0)
    block, species, rows, depth = u.shape
    row = lax.broadcasted_iota(jnp.int32, (rows, depth), 0)
    lane = lax.broadcasted_iota(jnp.int32, (rows, depth), 1)
    for x in range(block):
        coeffs = coefficients(flow, x)
        for s in range(species):
            if x > 0:
                lo = u[x - 1, s]
            else:
                lo = jnp.where(i == 0, first[0, s], before[0, s])
            if x < block - 1:
                hi = u[x + 1, s]
            else:
                hi = jnp.where(i == steps - 1, last[0, s], after[0, s])
            out[x, s] = update(
                diffusion[s], coeffs, u[x, s], lo, hi,
                below[s, pl.ds(x, 1), :], above[s, pl.ds(x, 1), :], row, lane,
            )


def advance(diffusion, u, first, last, below, above, flow):
    planes, species, rows, depth = u.shape
    block = 16 if planes % 16 == 0 else planes
    steps = planes // block
    edge_spec = pl.BlockSpec((species, block, depth), lambda i: (0, i, 0))
    plane_spec = pl.BlockSpec((1, species, rows, depth), lambda i: (0, 0, 0, 0))
    block_spec = pl.BlockSpec((block, species, rows, depth), lambda i: (i, 0, 0, 0))
    return pl.pallas_call(
        functools.partial(advance_kernel, steps),
        grid=(steps,),
        out_shape=jax.ShapeDtypeStruct(u.shape, u.dtype),
        in_specs=[
            pl.BlockSpec(memory_space=pltpu.SMEM),
            block_spec,
            pl.BlockSpec(
                (1, species, rows, depth), lambda i: (jnp.maximum(i * block - 1, 0), 0, 0, 0)
            ),
            pl.BlockSpec(
                (1, species, rows, depth),
                lambda i: (jnp.minimum(i * block + block, planes - 1), 0, 0, 0),
            ),
            plane_spec,
            plane_spec,
            edge_spec,
            edge_spec,
            pl.BlockSpec((block, 3, rows, depth), lambda i: (i, 0, 0, 0)),
        ],
        out_specs=block_spec,
        compiler_params=params(),
        name="advance",
    )(diffusion, u, u, u, first, last, below, above, flow)


def shift_up(value, axis):
    size = lax.axis_size(axis)
    return lax.ppermute(value, axis, [(i, i + 1) for i in range(size - 1)])


def shift_down(value, axis):
    size = lax.axis_size(axis)
    return lax.ppermute(value, axis, [(i + 1, i) for i in range(size - 1)])


def rims(u):
    rows = u.shape[2]
    below = shift_up(jnp.swapaxes(u[:, :, rows - 1], 0, 1), "grp")
    above = shift_down(jnp.swapaxes(u[:, :, 0], 0, 1), "grp")
    return shift_up(u[-1:], "dev"), shift_down(u[:1], "dev"), below, above


def on_device(old_fine, old_ids, old_coarse, coarse_ids, velocity, diffusion):
    devices = lax.axis_size("dev")
    group_count = lax.axis_size("grp")
    me = lax.axis_index("dev")
    planes = old_fine.shape[0]
    coarse_planes = old_coarse.shape[0]
    capacity = max(2, 2 * planes // devices)
    coarse_capacity = max(2, 2 * coarse_planes // devices)
    both = jnp.concatenate([old_ids[0], coarse_ids[0]])
    relaying = capacity >= 16 and devices % 2 == 0 and planes % 8 == 0 and group_count > 2
    if relaying:
        groups = gather_ids(both, group_count, devices)
    else:
        groups = lax.all_gather(both, ("grp", "dev")).reshape(group_count, devices, -1)
    weights = spread_weights(old_coarse.shape[3])

    def padded(fine, coarse):
        here = (jnp.arange(group_count) == lax.axis_index("grp"))[:, None, None]
        both_all = jnp.max(jnp.where(here, groups, -1), axis=0)
        own = jnp.max(jnp.where((jnp.arange(devices) == me)[:, None], both_all, -1), axis=0)
        coarse_send = send_table(own[planes:], coarse_planes, devices, coarse_capacity)
        coarse_table = receive_table(both_all[:, planes:], coarse_planes, coarse_capacity, me)
        coarse_out = pack_coarse(coarse_send, coarse)
        coarse_in = lax.all_to_all(coarse_out, "dev", split_axis=0, concat_axis=0, tiled=True)
        send = send_table(own[:planes], planes, devices, capacity)
        table = receive_table(both_all[:, :planes], planes, capacity, me)
        arrived = lax.all_to_all(pack_fine(send, fine), "dev", split_axis=0, concat_axis=0, tiled=True)
        interp = refine(coarse_table[None], coarse_in, weights)
        u = assemble(table, arrived, interp)
        u = advance(diffusion, u, *rims(u), velocity)
        return (u,) + rims(u)

    if relaying:
        choices = [capacity * k // 16 for k in CROSS]
        sizes = tuple(capacity * k // 16 for k in FINE) + tuple(coarse_capacity * k // 8 for k in COARSE)
        sizes = sizes[:5] + (1,) + sizes[5:]
        rows = group_count * devices
        flat = groups.reshape(rows, -1)
        place = jnp.stack([lax.axis_index("grp"), me]).astype(jnp.int32)
        tables = plan(
            place, flat[:, :planes], flat[:, planes:], group_count, devices, planes,
            coarse_planes, sizes, choices, capacity * LOOSE // 16,
        )

        def relayed(count, ident, fine, coarse):
            return regrid(
                count, (sizes[0] + (count >= capacity * LOOSE // 16),) + sizes[1:], ident, devices, tables, diffusion, fine, coarse, weights, velocity
            )

        branches = [
            functools.partial(relayed, count, 1 + k) for k, count in enumerate(choices)
        ]
        state = lax.switch(tables[6, 0], branches + [padded], old_fine, old_coarse)
    else:
        state = padded(old_fine, old_coarse)
    return advance(diffusion, *state, velocity)


def solution(mesh):
    in_specs = (
        P("dev", None, "grp", None),
        P("grp", "dev"),
        P("dev", None, "grp", None),
        P("grp", "dev"),
        P("dev", None, "grp", None),
        P(),
    )
    out_specs = P("dev", None, "grp", None)
    return jax.shard_map(
        on_device, mesh=mesh, in_specs=in_specs, out_specs=out_specs, check_vma=False
    )
```

```python
import functools

import jax
import jax.numpy as jnp
import numpy as np
from jax import lax
from jax.experimental import pallas as pl
from jax.experimental.pallas import tpu as pltpu
from jax.sharding import PartitionSpec as P

CROSS = (32, 33, 34, 35, 36, 37, 38, 40, 44)
LOOSE = 40
FINE = (10, 11, 6, 6)
COARSE = (4, 2, 6, 6, 4)
VMEM_LIMIT = 48 * 1024 * 1024
MESH = pl.DeviceIdType.MESH


def params(**more):
    return pltpu.CompilerParams(vmem_limit_bytes=VMEM_LIMIT, **more)


def earlier_count(mask):
    count = mask.shape[-1]
    lower = jnp.arange(count)[None, :] < jnp.arange(count)[:, None]
    return jnp.sum((mask[..., None, :] & lower).astype(jnp.int32), axis=-1)


def send_table(labels, block_len, devices, capacity):
    target = jnp.where(labels >= 0, labels // block_len, -1)
    count = labels.shape[0]
    same = target[None, :] == target[:, None]
    lower = jnp.arange(count)[None, :] < jnp.arange(count)[:, None]
    rank = jnp.sum((same & lower).astype(jnp.int32), axis=1)
    slot = jnp.where(labels >= 0, target * capacity + rank, -1)
    hits = slot[None, :] == jnp.arange(devices * capacity)[:, None]
    return jnp.max(jnp.where(hits, jnp.arange(count)[None, :], 0), axis=1)


def receive_table(labels_all, block_len, capacity, me):
    devices, count = labels_all.shape
    within = labels_all - me * block_len
    valid = (within >= 0) & (within < block_len)
    slot = jnp.arange(devices)[:, None] * capacity + earlier_count(valid)
    flat_within = jnp.where(valid, within, -1).reshape(-1)
    hits = flat_within[None, :] == jnp.arange(block_len)[:, None]
    return jnp.max(jnp.where(hits, slot.reshape(-1)[None, :], -1), axis=1)


def same_dim(a, b, exact=None):
    return lax.dot_general(
        a, b, (((1,), (1,)), ((), ())), precision=exact,
        preferred_element_type=jnp.float32,
    )


def plain_dot(a, b):
    return jnp.dot(a, b, preferred_element_type=jnp.float32)


def as_float(mask):
    return jnp.where(mask, 1.0, 0.0)


def stacked(masks, right):
    out = plain_dot(jnp.concatenate(masks, axis=0), right)
    size = masks[0].shape[0]
    return [out[i * size : (i + 1) * size] for i in range(len(masks))]


def route(owner, devices, base, extra, step, inner, stride, depth, hops):
    shape = owner.shape
    rows, count = shape
    part = devices // 2
    src = lax.rem(lax.broadcasted_iota(jnp.int32, shape, 0), devices)
    home, spot0 = src // part, lax.rem(src, part)
    first = lax.broadcasted_iota(jnp.int32, (count, count), 0)
    second = lax.broadcasted_iota(jnp.int32, (count, count), 1)
    before = as_float(first < second)
    ones = jnp.ones((count, count), jnp.float32)
    masks = [as_float(owner == e) for e in range(devices)]
    ranks = stacked(masks, before)
    counts = [c.astype(jnp.int32) for c in stacked(masks, ones)]
    rank = sum(m * r for m, r in zip(masks, ranks)).astype(jnp.int32)
    caps = []
    for v in range(devices):
        turn = lax.rem(v + part - spot0, part)
        wide = base + jnp.where(turn < extra, step, 0)
        caps.append(jnp.where(home != v // part, wide, inner))
    limit = sum(jnp.where(owner == v, caps[v], 0) for v in range(devices))
    valid = owner >= 0
    over = valid & (rank >= limit)
    side = jnp.where(valid, owner // part, -1)
    orders = stacked([as_float(over & (side == h)) for h in range(2)], before)
    order = jnp.where(side == 0, orders[0], orders[1]).astype(jnp.int32)
    lent_via = jnp.full(shape, -1, jnp.int32)
    lent_spot = jnp.zeros(shape, jnp.int32)
    for h in range(2):
        passed = jnp.zeros(shape, jnp.int32)
        seek = jnp.where(over & (side == h), order, -1)
        for l in range(stride - 1, -1, -1):
            for v in range(h * part, (h + 1) * part):
                free = (counts[v] <= l) & (caps[v] > l)
                hit = free & (seek == passed)
                lent_via = jnp.where(hit, v, lent_via)
                lent_spot = jnp.where(hit, l, lent_spot)
                passed = passed + jnp.where(free, 1, 0)
    via = jnp.where(over, lent_via, owner)
    spot = jnp.where(over, lent_spot, rank)
    relayed = over & (via >= 0) & (via != owner)
    limit_via = sum(jnp.where(via == v, caps[v], 0) for v in range(devices))
    deep = relayed & (spot < limit_via - depth)
    bad = (over & (lent_via < 0)) | deep
    lanes = [
        (v, e) for v in range(devices) for e in range(devices)
        if v != e and v // part == e // part
    ]
    hops_at = [as_float(relayed & (via == v) & (owner == e)) for v, e in lanes]
    inside = stacked(hops_at, before)
    total = stacked(hops_at, jnp.ones((count, 128), jnp.float32))
    lane = lax.broadcasted_iota(jnp.int32, (rows, 128), 1)
    table = sum(jnp.where(lane == i, t, 0.0) for i, t in enumerate(total))
    up = lax.broadcasted_iota(jnp.int32, (rows, rows), 0)
    across = lax.broadcasted_iota(jnp.int32, (rows, rows), 1)
    earlier = as_float((up // devices == across // devices) & (across < up))
    ahead = plain_dot(earlier, table)
    index = jnp.zeros(shape, jnp.float32)
    for i, m in enumerate(hops_at):
        index = index + m * (inside[i] + ahead[:, i : i + 1])
    crowded = jnp.max(ahead + table, axis=(0, 1), keepdims=True) > float(hops)
    fault = jnp.max(as_float(bad), axis=(0, 1), keepdims=True) > 0.0
    broken = jnp.where(crowded | fault, 1, 0)
    return via, spot, relayed, index.astype(jnp.int32), caps, broken


def widest_load(owner, devices):
    part = devices // 2
    src = lax.rem(lax.broadcasted_iota(jnp.int32, owner.shape, 0), devices)
    away = (owner >= 0) & (owner // part != src // part)
    load = jnp.sum(as_float(away), axis=1, keepdims=True)
    return jnp.max(load, axis=0, keepdims=True)


def plan_kernel(
    groups, devices, block_len, coarse_len, sizes, choices, loose,
    place, fine_ids, coarse_ids, out, via_ref, where_ref, kind_ref, owner_ref, inner_ref,
):
    inner, stride, depth, hops, base_c, extra_c, step_c, inner_c, stride_c, hops_c = sizes
    part = devices // 2
    g, me = place[0], place[1]
    fine, coarse = fine_ids[...], coarse_ids[...]
    rows, count = fine.shape
    count_c = coarse.shape[1]
    width = out.shape[1]
    owner = jnp.where(fine >= 0, fine // block_len, -1)
    load = widest_load(owner, devices)
    pick = sum(jnp.where(load > float(c), 1, 0) for c in choices)[0, 0]

    both = jnp.where(fine >= 0, lax.rem(fine, block_len) // 2, -1)
    kind = lax.broadcasted_iota(jnp.int32, (devices, count), 0)
    cell = lax.broadcasted_iota(jnp.int32, (coarse_len, count), 0)
    cell_c = lax.broadcasted_iota(jnp.int32, (coarse_len, count_c), 0)
    kind_c = lax.broadcasted_iota(jnp.int32, (devices, count_c), 0)
    owner_c = coarse // coarse_len
    within_c = lax.rem(coarse, coarse_len)
    needed = []
    for k in range(groups):
        held = jnp.zeros((devices, coarse_len), jnp.float32)
        for s in range(devices):
            r = k * devices + s
            held = held + same_dim(
                as_float(owner[r : r + 1] == kind), as_float(both[r : r + 1] == cell)
            )
        for s in range(devices):
            r = k * devices + s
            seen = plain_dot(held, as_float(within_c[r : r + 1] == cell_c))
            seen = jnp.where(owner_c[r : r + 1] == kind_c, seen, 0.0)
            needed.append(jnp.sum(seen, axis=0, keepdims=True))
    needed = jnp.concatenate(needed, axis=0) < 1.5
    owner_c = jnp.where(needed, owner_c, -1)

    def assign(owner, ids, length, stride, hops, depth, base, extra, step, inner):
        via, spot, relayed, index, caps, broken = route(
            owner, devices, base, extra, step, inner, stride, depth, hops
        )
        n = owner.shape[1]
        src = lax.rem(lax.broadcasted_iota(jnp.int32, owner.shape, 0), devices)
        turn = lax.rem(lax.rem(via, part) + part - lax.rem(src, part), part)
        block = jnp.where(via // part != src // part, turn, part + turn)
        cap = sum(jnp.where(via == v, caps[v], 0) for v in range(devices))
        late = stride - depth
        early = spot >= cap - depth
        flat = jnp.where(
            early, devices * late + block * depth + spot - (cap - depth), block * late + spot
        )
        via_ref[:, 0:n] = jnp.where(relayed, via, -1)
        where_ref[:, 0:n] = jnp.where(via >= 0, flat, -1)
        kind_ref[:, 0:n] = index
        owner_ref[:, 0:n] = owner
        inner_ref[:, 0:n] = ids - me * length
        return broken

    def tables(n, stride, hops, start):
        arrivals = devices * stride
        passed = (part - 1) * hops
        small = max(n, arrivals + passed + 1) <= 256
        exact = None if small else lax.Precision.HIGHEST
        mine = pl.ds(pl.multiple_of(g * devices, devices), devices)
        via_g = via_ref[mine, 0:n]
        flat_g = where_ref[mine, 0:n]
        index_g = kind_ref[mine, 0:n]
        owner_g = owner_ref[mine, 0:n]
        inner_g = inner_ref[mine, 0:n]
        source = lax.broadcasted_iota(jnp.int32, (devices, n), 0)
        own = jnp.max(jnp.where(source == me, flat_g, -1), axis=0, keepdims=True)
        slots = lax.broadcasted_iota(jnp.int32, (width, n), 0)
        place_at = lax.broadcasted_iota(jnp.int32, (devices, n), 1).astype(jnp.float32)
        send = same_dim(place_at, as_float(own == slots), exact)
        seat = lax.rem(me, part)
        lane = lax.rem(owner_g + 2 * part - seat, part) - 1
        handed = jnp.where(via_g == me, lane * hops + index_g, -1)
        back = lax.rem(seat + part - lax.rem(jnp.maximum(via_g, 0), part), part) - 1
        spot_at = jnp.where(via_g >= 0, arrivals + back * hops + index_g, flat_g)
        inside = jnp.where(owner_g == me, inner_g, -1)
        flat_f = flat_g.astype(jnp.float32)
        spot_f = spot_at.astype(jnp.float32) + 1.0
        relay = jnp.zeros((devices, width), jnp.float32)
        final = jnp.zeros((devices, width), jnp.float32)
        for s in range(devices):
            relay = relay + same_dim(
                jnp.broadcast_to(flat_f[s : s + 1], (devices, n)),
                as_float(handed[s : s + 1] == slots), exact,
            )
            final = final + same_dim(
                jnp.broadcast_to(spot_f[s : s + 1], (devices, n)),
                as_float(inside[s : s + 1] == slots), exact,
            )
        at = lax.broadcasted_iota(jnp.int32, (devices, width), 1)
        whole = (final + 0.5).astype(jnp.int32)
        missing = start + (at // 2 if start else 0)
        whole = jnp.where(whole > 0, whole - 1, missing)
        return [(send + 0.5).astype(jnp.int32), (relay + 0.5).astype(jnp.int32), whole]

    broken_c = assign(
        owner_c, coarse, coarse_len, stride_c, hops_c, stride_c, base_c, extra_c, step_c, inner_c,
    )
    parts_c = tables(count_c, stride_c, hops_c, 0)

    def attempt(carry):
        pick, _ = carry
        wide = sum(jnp.where(pick == i, c, 0) for i, c in enumerate(choices))
        broken = assign(
            owner, fine, block_len, stride, hops, depth, wide // part, lax.rem(wide, part), 1,
            inner + jnp.where(wide >= loose, 1, 0),
        )
        return pick + 1, broken[0, 0]

    def again(carry):
        return (carry[1] > 0) & (carry[0] < len(choices))

    after, broken = lax.while_loop(again, attempt, (pick, jnp.int32(1)))
    fill = devices * stride + (part - 1) * hops
    parts = tables(count, stride, hops, fill)
    pick = jnp.where((broken > 0) | (broken_c[0, 0] > 0), len(choices), after - 1)
    parts = parts + parts_c
    for i, value in enumerate(parts):
        out[i : i + 1] = value[0:1]
    out[len(parts) : len(parts) + 1] = jnp.zeros((1, width), jnp.int32) + pick


def plan(place, fine_ids, coarse_ids, groups, devices, block_len, coarse_len, sizes, choices, loose):
    rows, count = fine_ids.shape
    longest = max(devices * sizes[1], devices * sizes[8], count, (devices // 2) * max(sizes[3], sizes[9]))
    width = -(-longest // 128) * 128
    cells = pltpu.VMEM((rows, max(count, coarse_ids.shape[1])), jnp.int32)
    return pl.pallas_call(
        functools.partial(
            plan_kernel, groups, devices, block_len, coarse_len, sizes, choices, loose
        ),
        out_shape=jax.ShapeDtypeStruct((8, width), jnp.int32),
        in_specs=[
            pl.BlockSpec(memory_space=pltpu.SMEM),
            pl.BlockSpec(memory_space=pltpu.VMEM),
            pl.BlockSpec(memory_space=pltpu.VMEM),
        ],
        out_specs=pl.BlockSpec(memory_space=pltpu.VMEM),
        scratch_shapes=[cells] * 5,
        compiler_params=params(),
        name="plan",
    )(place, fine_ids, coarse_ids)


def pack_fine_kernel(table, source, out, sem):
    def send(i, carry):
        pltpu.make_async_copy(source.at[table[i]], out.at[i], sem).start()
        return carry

    lax.fori_loop(0, out.shape[0], send, 0)
    pltpu.make_async_copy(out, out, sem).wait()


def pack_fine(table, fine):
    return pl.pallas_call(
        pack_fine_kernel,
        out_shape=jax.ShapeDtypeStruct((table.shape[0],) + fine.shape[1:], fine.dtype),
        in_specs=[
            pl.BlockSpec(memory_space=pltpu.SMEM),
            pl.BlockSpec(memory_space=pltpu.VMEM),
        ],
        out_specs=pl.BlockSpec(memory_space=pl.ANY),
        scratch_shapes=[pltpu.SemaphoreType.DMA],
        compiler_params=params(),
        name="pack_fine",
    )(table, fine)


def pack_coarse_kernel(table, source, out):
    half = source.shape[-1]

    def step(i, carry):
        out[i, :, :, 0:half] = source[table[2 * i]]
        out[i, :, :, half : 2 * half] = source[table[2 * i + 1]]
        return carry

    lax.fori_loop(0, out.shape[0], step, 0)


def pack_coarse(table, coarse):
    shape = (table.shape[0] // 2,) + coarse.shape[1:3] + (2 * coarse.shape[3],)
    return pl.pallas_call(
        pack_coarse_kernel,
        out_shape=jax.ShapeDtypeStruct(shape, coarse.dtype),
        in_specs=[
            pl.BlockSpec(memory_space=pltpu.SMEM),
            pl.BlockSpec(memory_space=pltpu.VMEM),
        ],
        out_specs=pl.BlockSpec(memory_space=pltpu.VMEM),
        compiler_params=params(),
        name="pack_coarse",
    )(table, coarse)


def refine_into(table, which, pairs, weights, out, offset, count):
    species, rows, depth = pairs.shape[1:]
    half = depth // 2
    lane = lax.broadcasted_iota(jnp.int32, (species * rows, depth), 1)
    row = lax.broadcasted_iota(jnp.int32, (species, rows, depth), 1)

    def step(c, carry):
        slot = jnp.maximum(table[which, c], 0)
        block = pairs[slot // 2].reshape(species * rows, depth)
        odd = slot % 2
        block = jnp.where((lane >= half).astype(jnp.int32) == odd, block, 0.0)
        spread = jnp.dot(
            block, weights[...], precision=lax.Precision.HIGHEST,
            preferred_element_type=jnp.float32,
        )
        plain = spread[:, :depth].reshape(species, rows, depth)
        sloped = spread[:, depth:].reshape(species, rows, depth)
        below = jnp.where(row == 0, plain, pltpu.roll(plain, 1, 1))
        above = jnp.where(row == rows - 1, plain, pltpu.roll(plain, rows - 1, 1))
        slope = 0.125 * (above - below)
        for s in range(species):
            out[offset + c, s, pl.ds(0, rows, 2), :] = sloped[s] - slope[s]
            out[offset + c, s, pl.ds(1, rows, 2), :] = sloped[s] + slope[s]
        return carry

    lax.fori_loop(0, count, step, 0)


def refine_kernel(table, pairs, weights, out):
    refine_into(table, 0, pairs, weights, out, 0, out.shape[0])


def spread_weights(half):
    depth = 2 * half
    coarse = np.arange(half)[:, None]
    fine = np.arange(depth)[None, :]
    centre = (fine // 2 == coarse).astype(np.float32)
    up = (np.minimum(fine // 2 + 1, half - 1) == coarse).astype(np.float32)
    down = (np.maximum(fine // 2 - 1, 0) == coarse).astype(np.float32)
    side = np.where(fine % 2 == 1, 0.125, -0.125).astype(np.float32)
    both = np.concatenate([centre, centre + side * (up - down)], axis=1)
    return np.concatenate([both, both], axis=0)


def refine(table, pairs, weights):
    species, rows, depth = pairs.shape[1:]
    return pl.pallas_call(
        refine_kernel,
        out_shape=jax.ShapeDtypeStruct(
            (table.shape[1], species, 2 * rows, depth), pairs.dtype
        ),
        in_specs=[
            pl.BlockSpec(memory_space=pltpu.SMEM),
            pl.BlockSpec(memory_space=pltpu.VMEM),
            pl.BlockSpec(memory_space=pltpu.VMEM),
        ],
        out_specs=pl.BlockSpec(memory_space=pltpu.VMEM),
        compiler_params=params(),
        cost_estimate=pl.CostEstimate(
            flops=40_000_000, bytes_accessed=30_000_000, transcendentals=0
        ),
        name="refine",
    )(table, pairs, weights)


def assemble_kernel(table, arrived, interp, out, sem):
    def fetch(p, carry):
        slot = table[p]

        @pl.when(slot >= 0)
        def _():
            pltpu.make_async_copy(arrived.at[slot], out.at[p], sem).start()

        @pl.when(slot < 0)
        def _():
            pltpu.make_async_copy(interp.at[p // 2], out.at[p], sem).start()

        return carry

    lax.fori_loop(0, out.shape[0], fetch, 0)
    pltpu.make_async_copy(out, out, sem).wait()


def assemble(table, arrived, interp):
    return pl.pallas_call(
        assemble_kernel,
        out_shape=jax.ShapeDtypeStruct((table.shape[0],) + arrived.shape[1:], arrived.dtype),
        in_specs=[
            pl.BlockSpec(memory_space=pltpu.SMEM),
            pl.BlockSpec(memory_space=pl.ANY),
            pl.BlockSpec(memory_space=pl.ANY),
        ],
        out_specs=pl.BlockSpec(memory_space=pltpu.VMEM),
        scratch_shapes=[pltpu.SemaphoreType.DMA],
        compiler_params=params(),
        name="assemble",
    )(table, arrived, interp)


def gather_kernel(groups, devices, mine, out, send_sems, recv_sems):
    total = groups * devices
    me = lax.axis_index("grp") * devices + lax.axis_index("dev")
    barrier = pltpu.get_barrier_semaphore()

    def place(k):
        to = lax.rem(me + k, total)
        return {"grp": to // devices, "dev": lax.rem(to, devices)}

    def greet(k, carry):
        pl.semaphore_signal(barrier, inc=1, device_id=place(k), device_id_type=MESH)
        return carry

    lax.fori_loop(1, total, greet, 0)
    pl.semaphore_wait(barrier, total - 1)

    def copy(k):
        return pltpu.make_async_remote_copy(
            src_ref=mine,
            dst_ref=out.at[me],
            send_sem=send_sems.at[k],
            recv_sem=recv_sems.at[k],
            device_id=place(k),
            device_id_type=MESH,
        )

    def start(k, carry):
        copy(k).start()
        return carry

    def finish(k, carry):
        copy(k).wait_send()
        source = lax.rem(me + total - k, total)
        pltpu.make_async_remote_copy(
            src_ref=mine,
            dst_ref=out.at[source],
            send_sem=send_sems.at[k],
            recv_sem=recv_sems.at[k],
            device_id=place(k),
            device_id_type=MESH,
        ).wait_recv()
        return carry

    lax.fori_loop(1, total, start, 0)
    out[me] = mine[...]
    lax.fori_loop(1, total, finish, 0)


def gather_ids(both, groups, devices):
    width = both.shape[0]
    padded = -(-width // 128) * 128
    mine = jnp.pad(both, (0, padded - width))[None]
    total = groups * devices
    out = pl.pallas_call(
        functools.partial(gather_kernel, groups, devices),
        out_shape=jax.ShapeDtypeStruct((total, 1, padded), both.dtype),
        in_specs=[pl.BlockSpec(memory_space=pltpu.VMEM)],
        out_specs=pl.BlockSpec(memory_space=pltpu.VMEM),
        scratch_shapes=[
            pltpu.SemaphoreType.DMA((total,)),
            pltpu.SemaphoreType.DMA((total,)),
        ],
        compiler_params=pltpu.CompilerParams(collective_id=0, has_side_effects=True),
        name="gather_ids",
    )(mine)
    return out.reshape(groups, devices, padded)[:, :, :width]


def coefficients(flow, x):
    v = [flow[x, k] for k in range(3)]
    plus = [jnp.maximum(w, 0.0) for w in v]
    minus = [jnp.maximum(-w, 0.0) for w in v]
    rest = 1.0
    for k in range(3):
        rest = rest - plus[k] - minus[k]
    return plus, minus, rest


def update(d, coeffs, c, lo, hi, below, above, row, lane):
    rows, depth = c.shape
    plus, minus, rest = coeffs
    ylo = jnp.where(row == 0, below, pltpu.roll(c, 1, 0))
    yhi = jnp.where(row == rows - 1, above, pltpu.roll(c, rows - 1, 0))
    zlo = jnp.where(lane == 0, c, pltpu.roll(c, 1, 1))
    zhi = jnp.where(lane == depth - 1, c, pltpu.roll(c, depth - 1, 1))
    total = (rest - 6.0 * d) * c
    total = total + (plus[0] + d) * lo + (minus[0] + d) * hi
    total = total + (plus[1] + d) * ylo + (minus[1] + d) * yhi
    return total + (plus[2] + d) * zlo + (minus[2] + d) * zhi


def regrid_kernel(
    cross, sizes, tables, diffusion, fine_hbm, coarse_hbm, weights, flow_hbm,
    out_hbm, first_out, last_out, below_out, above_out,
    fine, coarse, flow, out, load_sems, save_sems, send, send_c, pool, pool_c, near, handed, handed_c, passed_in, passed_c,
    state, low, high, below, above,
    low_next, high_next, below_next, above_next, first_next, last_next,
    send_sems, recv_sems, relay_send, relay_recv, edge_send, edge_recv, row_send, row_recv,
):
    inner, stride, depth, hops, base_c, extra_c, step_c, inner_c, stride_c, hops_c = sizes
    planes, species, rows, depth_z = fine.shape
    half_z = depth_z // 2
    groups, devices = lax.axis_size("grp"), lax.axis_size("dev")
    part = devices // 2
    late = stride - depth
    wide = [cross // part + (1 if k < cross % part else 0) for k in range(part)]
    wide_c = [base_c + (step_c if k < extra_c else 0) for k in range(part)]
    caps = wide + [inner] * part
    caps_c = wide_c + [inner_c] * part
    g, me = lax.axis_index("grp"), lax.axis_index("dev")
    base = (me // part) * part
    other = part - base
    seat = lax.rem(me, part)
    barrier = pltpu.get_barrier_semaphore()
    lane_c = lax.broadcasted_iota(jnp.int32, send_c.shape[1:], 2)

    def target(b):
        if b < part:
            return {"dev": other + lax.rem(seat + b, part)}
        return {"dev": base + lax.rem(seat + b - part, part)}

    def greet(to):
        pl.semaphore_signal(barrier, inc=1, device_id=to, device_id_type=MESH)

    loads = [
        pltpu.make_async_copy(source, into, load_sems.at[i])
        for i, (source, into) in enumerate(((fine_hbm, fine), (coarse_hbm, coarse), (flow_hbm, flow)))
    ]
    for load in loads:
        load.start()
    peers = list(range(part + 1, devices)) + list(range(part))
    for b in peers:
        greet(target(b))
    greet({"grp": lax.rem(g + 1, groups)})
    greet({"grp": lax.rem(g + groups - 1, groups)})
    pl.semaphore_wait(barrier, devices + 1)

    def remote(source, into, sems, at, to):
        return pltpu.make_async_remote_copy(
            src_ref=source,
            dst_ref=into,
            send_sem=sems[0].at[at],
            recv_sem=sems[1].at[at],
            device_id=to,
            device_id_type=MESH,
        )

    def pack(first, count, into, offset):
        def step(k, carry):
            into[offset + k] = fine[tables[0, first + k]]
            return carry

        lax.fori_loop(0, count, step, 0)

    def pack_coarse_pairs(first, count, into):
        def step(k, carry):
            into[first + k, :, :, 0:half_z] = coarse[tables[3, 2 * (first + k)]]
            into[first + k, :, :, half_z:depth_z] = coarse[tables[3, 2 * (first + k) + 1]]
            return carry

        lax.fori_loop(0, count, step, 0)

    sems = (send_sems, recv_sems)
    pairs_c = stride_c // 2
    coarse_moves, early_moves = [], []
    begin = devices * late
    near_by, far = peers[: part - 1], peers[part - 1 :]

    def send_coarse(b):
        count = caps_c[b] // 2
        first = b * pairs_c + pairs_c - count
        pack_coarse_pairs(first, count, send_c)
        cut = pl.ds(first, count)
        coarse_moves.append(remote(send_c.at[cut], pool_c.at[cut], sems, b, target(b)))
        coarse_moves[-1].start()

    def send_early(b):
        pack(begin + b * depth, depth, send, begin + b * depth)
        early_moves.append(
            remote(
                send.at[pl.ds(begin + b * depth, depth)], near.at[pl.ds(b * depth, depth)],
                sems, devices + b, target(b),
            )
        )
        early_moves[-1].start()

    def late_copy(b):
        cut = pl.ds(b * late, caps[b] - depth)
        return remote(send.at[cut], pool.at[cut], sems, 2 * devices + b, target(b))

    loads[0].wait()
    for b in far[:1]:
        send_early(b)
    loads[1].wait()
    for b in far:
        send_coarse(b)
    for b in far[1:]:
        send_early(b)
    for b in near_by:
        send_coarse(b)
        send_early(b)
        pack(b * late, inner - depth, send, b * late)
        late_copy(b).start()
    pack_coarse_pairs(part * pairs_c + pairs_c - inner_c // 2, inner_c // 2, pool_c)
    pack(begin + part * depth, depth, near, part * depth)
    pack(part * late, inner - depth, pool, part * late)
    for move in coarse_moves:
        move.wait_recv()

    def half_of(slot, odd):
        value = pool_c[slot // 2]
        turned = pltpu.roll(value, half_z, 2)
        return jnp.where(slot % 2 == odd, value, turned)

    def relay_coarse(k, carry):
        left = half_of(tables[4, 2 * k], 0)
        right = half_of(tables[4, 2 * k + 1], 1)
        handed_c[k] = jnp.where(lane_c < half_z, left, right)
        return carry

    sends_c = hops_c // 2
    relay_sems = (relay_send, relay_recv)
    lax.fori_loop(0, (part - 1) * sends_c, relay_coarse, 0)
    relays_c = []
    for k in range(1, part):
        cut = pl.ds((k - 1) * sends_c, sends_c)
        relays_c.append(remote(handed_c.at[cut], passed_c.at[cut], relay_sems, k, target(part + k)))
        relays_c[-1].start()
    for b in far:
        pack(b * late, caps[b] - depth, send, b * late)
    outer = (me < part // 2) | (me >= devices - part // 2)

    @pl.when(jnp.logical_not(outer))
    def _():
        for b in far:
            late_copy(b).start()

    for move in early_moves:
        move.wait_recv()

    passed = (part - 1) * hops

    def relay(k, carry):
        handed[k] = near[jnp.maximum(tables[1, k] - begin, 0)]
        return carry

    lax.fori_loop(0, passed, relay, 0)
    relays = []
    for k in range(1, part):
        cut = pl.ds((k - 1) * hops, hops)
        relays.append(
            remote(handed.at[cut], passed_in.at[cut], relay_sems, part + k, target(part + k))
        )
        relays[-1].start()

    @pl.when(outer)
    def _():
        for b in far:
            late_copy(b).start()

    late_moves = [late_copy(b) for b in peers]

    def keep_near(k, carry):
        pool[begin + k] = near[k]
        return carry

    lax.fori_loop(0, devices * depth, keep_near, 0)
    for move in relays_c:
        move.wait_recv()

    def keep_coarse(k, carry):
        pool_c[devices * pairs_c + k] = passed_c[k]
        return carry

    lax.fori_loop(0, (part - 1) * sends_c, keep_coarse, 0)
    arrivals = devices * stride
    refine_into(tables, 5, pool_c, weights, pool, arrivals + passed, coarse.shape[0])
    for move in late_moves + relays:
        move.wait_recv()

    def keep_passed(k, carry):
        pool[arrivals + k] = passed_in[k]
        return carry

    lax.fori_loop(0, passed, keep_passed, 0)

    def edge_copy(source, target, at, to):
        return pltpu.make_async_remote_copy(
            src_ref=source,
            dst_ref=target,
            send_sem=edge_send.at[at],
            recv_sem=edge_recv.at[at],
            device_id=to,
            device_id_type=MESH,
        )

    def row_copy(source, target, b, at, to):
        cut = pl.ds(pl.multiple_of(b * 8, 8), 8)
        return pltpu.make_async_remote_copy(
            src_ref=source.at[:, cut],
            dst_ref=target.at[:, cut],
            send_sem=row_send.at[at, b],
            recv_sem=row_recv.at[at, b],
            device_id=to,
            device_id_type=MESH,
        )

    left, right = {"dev": me - 1}, {"dev": me + 1}
    down, up = {"grp": g - 1}, {"grp": g + 1}
    ahead = edge_copy(state.at[pl.ds(planes, 1)], state.at[pl.ds(0, 1)], 0, right)
    back = edge_copy(state.at[pl.ds(1, 1)], state.at[pl.ds(planes + 1, 1)], 1, left)
    has_left, has_right = me > 0, me < devices - 1
    has_down, has_up = g > 0, g < groups - 1

    blocks = planes // 8

    def assemble_block(turn, carry):
        b = lax.rem(turn + blocks - 1, blocks)

        def assemble(k, carry):
            p = b * 8 + k
            at = tables[2, p]
            for s in range(species):
                value = pool[at, s]
                state[p + 1, s] = value
                low[s, pl.ds(p, 1), :] = value[0:1]
                high[s, pl.ds(p, 1), :] = value[rows - 1 : rows]
            return carry

        lax.fori_loop(0, 8, assemble, 0)

        @pl.when((turn == 0) & has_right)
        def _():
            ahead.start()

        @pl.when((turn == 1) & has_left)
        def _():
            back.start()

        @pl.when(has_up)
        def _():
            row_copy(high, below, b, 2, up).start()

        @pl.when(has_down)
        def _():
            row_copy(low, above, b, 3, down).start()

        return carry

    lax.fori_loop(0, blocks, assemble_block, 0)
    for move in coarse_moves + relays_c + early_moves + late_moves + relays:
        move.wait_send()

    @pl.when(has_left)
    def _():
        ahead.wait_recv()

    @pl.when(has_right)
    def _():
        back.wait_recv()

    @pl.when(has_right)
    def _():
        ahead.wait_send()

    @pl.when(has_left)
    def _():
        back.wait_send()

    @pl.when(me == 0)
    def _():
        state[0] = jnp.zeros(state.shape[1:], state.dtype)

    @pl.when(me == devices - 1)
    def _():
        state[planes + 1] = jnp.zeros(state.shape[1:], state.dtype)

    @pl.when(g == 0)
    def _():
        below[...] = jnp.zeros(below.shape, below.dtype)

    @pl.when(g == groups - 1)
    def _():
        above[...] = jnp.zeros(above.shape, above.dtype)

    row = lax.broadcasted_iota(jnp.int32, (rows, depth_z), 0)
    lane = lax.broadcasted_iota(jnp.int32, (rows, depth_z), 1)


    loads[2].wait()
    next_ahead = edge_copy(out.at[pl.ds(planes - 1, 1)], first_next, 4, right)
    next_back = edge_copy(out.at[pl.ds(0, 1)], last_next, 5, left)

    def save(b):
        cut = pl.ds(b * 8, 8)
        return pltpu.make_async_copy(out.at[cut], out_hbm.at[cut], save_sems.at[b])

    def advance_block(turn, carry):
        b = lax.rem(turn + blocks - 1, blocks)

        @pl.when(has_down)
        def _():
            row_copy(high, below, b, 2, up).wait_recv()

        @pl.when(has_up)
        def _():
            row_copy(low, above, b, 3, down).wait_recv()

        def advance_plane(k, carry):
            p = b * 8 + k
            coeffs = coefficients(flow, p)
            for s in range(species):
                total = update(
                    diffusion[s], coeffs, state[p + 1, s], state[p, s], state[p + 2, s],
                    below[s, pl.ds(p, 1), :], above[s, pl.ds(p, 1), :], row, lane,
                )
                out[p, s] = total
                low_next[s, pl.ds(p, 1), :] = total[0:1]
                high_next[s, pl.ds(p, 1), :] = total[rows - 1 : rows]
            return carry

        lax.fori_loop(0, 8, advance_plane, 0)
        save(b).start()

        @pl.when(has_up)
        def _():
            row_copy(high_next, below_next, b, 0, up).start()

        @pl.when(has_down)
        def _():
            row_copy(low_next, above_next, b, 1, down).start()

        @pl.when((turn == 0) & has_right)
        def _():
            next_ahead.start()

        @pl.when((turn == 1) & has_left)
        def _():
            next_back.start()

        return carry

    lax.fori_loop(0, blocks, advance_block, 0)

    def settle(b, carry):
        save(b).wait()

        @pl.when(has_down)
        def _():
            row_copy(high_next, below_next, b, 0, up).wait_recv()
            row_copy(low_next, above_next, b, 1, down).wait_send()
            row_copy(low, above, b, 3, down).wait_send()

        @pl.when(has_up)
        def _():
            row_copy(low_next, above_next, b, 1, down).wait_recv()
            row_copy(high_next, below_next, b, 0, up).wait_send()
            row_copy(high, below, b, 2, up).wait_send()

        return carry

    lax.fori_loop(0, blocks, settle, 0)

    @pl.when(has_left)
    def _():
        next_ahead.wait_recv()
        next_back.wait_send()
        first_out[...] = first_next[...]

    @pl.when(has_right)
    def _():
        next_back.wait_recv()
        next_ahead.wait_send()
        last_out[...] = last_next[...]

    @pl.when(has_down)
    def _():
        below_out[...] = below_next[...]

    @pl.when(has_up)
    def _():
        above_out[...] = above_next[...]

    @pl.when(me == 0)
    def _():
        first_out[...] = jnp.zeros(first_out.shape, first_out.dtype)

    @pl.when(me == devices - 1)
    def _():
        last_out[...] = jnp.zeros(last_out.shape, last_out.dtype)

    @pl.when(g == 0)
    def _():
        below_out[...] = jnp.zeros(below_out.shape, below_out.dtype)

    @pl.when(g == groups - 1)
    def _():
        above_out[...] = jnp.zeros(above_out.shape, above_out.dtype)


def regrid(cross, sizes, ident, devices, tables, diffusion, fine, coarse, weights, flow):
    inner, stride, depth, hops, base_c, extra_c, step_c, inner_c, stride_c, hops_c = sizes
    planes, species, rows, depth_z = fine.shape
    part = devices // 2
    kept = jax.ShapeDtypeStruct(fine.shape, fine.dtype)
    plane = jax.ShapeDtypeStruct((1,) + fine.shape[1:], fine.dtype)
    edge = jax.ShapeDtypeStruct((species, planes, depth_z), fine.dtype)
    pool = devices * stride + (part - 1) * hops + planes // 2
    pool_c = (devices * stride_c + (part - 1) * hops_c) // 2
    vmem = pl.BlockSpec(memory_space=pltpu.VMEM)
    smem = pl.BlockSpec(memory_space=pltpu.SMEM)
    hbm = pl.BlockSpec(memory_space=pl.ANY)

    def held(count):
        return pltpu.VMEM((count,) + fine.shape[1:], fine.dtype)

    def held_c(count):
        return pltpu.VMEM((count, species, rows // 2, depth_z), fine.dtype)

    def sems(*shape):
        return [pltpu.SemaphoreType.DMA(shape)] * 2

    rim = pltpu.VMEM(edge.shape, edge.dtype)
    passed, passed_c = (part - 1) * hops, (part - 1) * hops_c // 2
    return pl.pallas_call(
        functools.partial(regrid_kernel, cross, sizes),
        out_shape=(kept, plane, plane, edge, edge),
        in_specs=[smem] * 2 + [hbm, hbm, vmem, hbm],
        out_specs=(hbm,) + (vmem,) * 4,
        scratch_shapes=[
            held(planes), pltpu.VMEM(coarse.shape, coarse.dtype), pltpu.VMEM(flow.shape, flow.dtype),
            held(planes), pltpu.SemaphoreType.DMA((3,)), pltpu.SemaphoreType.DMA((planes // 8,)),
            held(devices * stride), held_c(devices * stride_c // 2), held(pool), held_c(pool_c),
            held(devices * depth), held(passed), held_c(passed_c), held(passed), held_c(passed_c),
            held(planes + 2), rim, rim, rim, rim, rim, rim, rim, rim, held(1), held(1),
            *sems(3 * devices), *sems(2 * part), *sems(6), *sems(4, planes // 8),
        ],
        compiler_params=params(collective_id=ident, has_side_effects=True),
        name="regrid",
    )(tables, diffusion, fine, coarse, weights, flow)


def advance_kernel(steps, diffusion, u, before, after, first, last, below, above, flow, out):
    i = pl.program_id(0)
    block, species, rows, depth = u.shape
    row = lax.broadcasted_iota(jnp.int32, (rows, depth), 0)
    lane = lax.broadcasted_iota(jnp.int32, (rows, depth), 1)
    for x in range(block):
        coeffs = coefficients(flow, x)
        for s in range(species):
            if x > 0:
                lo = u[x - 1, s]
            else:
                lo = jnp.where(i == 0, first[0, s], before[0, s])
            if x < block - 1:
                hi = u[x + 1, s]
            else:
                hi = jnp.where(i == steps - 1, last[0, s], after[0, s])
            out[x, s] = update(
                diffusion[s], coeffs, u[x, s], lo, hi,
                below[s, pl.ds(x, 1), :], above[s, pl.ds(x, 1), :], row, lane,
            )


def advance(diffusion, u, first, last, below, above, flow):
    planes, species, rows, depth = u.shape
    block = 16 if planes % 16 == 0 else planes
    steps = planes // block
    edge_spec = pl.BlockSpec((species, block, depth), lambda i: (0, i, 0))
    plane_spec = pl.BlockSpec((1, species, rows, depth), lambda i: (0, 0, 0, 0))
    block_spec = pl.BlockSpec((block, species, rows, depth), lambda i: (i, 0, 0, 0))
    return pl.pallas_call(
        functools.partial(advance_kernel, steps),
        grid=(steps,),
        out_shape=jax.ShapeDtypeStruct(u.shape, u.dtype),
        in_specs=[
            pl.BlockSpec(memory_space=pltpu.SMEM),
            block_spec,
            pl.BlockSpec(
                (1, species, rows, depth), lambda i: (jnp.maximum(i * block - 1, 0), 0, 0, 0)
            ),
            pl.BlockSpec(
                (1, species, rows, depth),
                lambda i: (jnp.minimum(i * block + block, planes - 1), 0, 0, 0),
            ),
            plane_spec,
            plane_spec,
            edge_spec,
            edge_spec,
            pl.BlockSpec((block, 3, rows, depth), lambda i: (i, 0, 0, 0)),
        ],
        out_specs=block_spec,
        compiler_params=params(),
        name="advance",
    )(diffusion, u, u, u, first, last, below, above, flow)


def shift_up(value, axis):
    size = lax.axis_size(axis)
    return lax.ppermute(value, axis, [(i, i + 1) for i in range(size - 1)])


def shift_down(value, axis):
    size = lax.axis_size(axis)
    return lax.ppermute(value, axis, [(i + 1, i) for i in range(size - 1)])


def rims(u):
    rows = u.shape[2]
    below = shift_up(jnp.swapaxes(u[:, :, rows - 1], 0, 1), "grp")
    above = shift_down(jnp.swapaxes(u[:, :, 0], 0, 1), "grp")
    return shift_up(u[-1:], "dev"), shift_down(u[:1], "dev"), below, above


def on_device(old_fine, old_ids, old_coarse, coarse_ids, velocity, diffusion):
    devices = lax.axis_size("dev")
    group_count = lax.axis_size("grp")
    me = lax.axis_index("dev")
    planes = old_fine.shape[0]
    coarse_planes = old_coarse.shape[0]
    capacity = max(2, 2 * planes // devices)
    coarse_capacity = max(2, 2 * coarse_planes // devices)
    both = jnp.concatenate([old_ids[0], coarse_ids[0]])
    relaying = capacity >= 16 and devices % 2 == 0 and planes % 8 == 0 and group_count > 2
    if relaying:
        groups = gather_ids(both, group_count, devices)
    else:
        groups = lax.all_gather(both, ("grp", "dev")).reshape(group_count, devices, -1)
    weights = jnp.asarray(spread_weights(old_coarse.shape[3]))

    def padded(fine, coarse):
        here = (jnp.arange(group_count) == lax.axis_index("grp"))[:, None, None]
        both_all = jnp.max(jnp.where(here, groups, -1), axis=0)
        own = jnp.max(jnp.where((jnp.arange(devices) == me)[:, None], both_all, -1), axis=0)
        coarse_send = send_table(own[planes:], coarse_planes, devices, coarse_capacity)
        coarse_table = receive_table(both_all[:, planes:], coarse_planes, coarse_capacity, me)
        coarse_out = pack_coarse(coarse_send, coarse)
        coarse_in = lax.all_to_all(coarse_out, "dev", split_axis=0, concat_axis=0, tiled=True)
        send = send_table(own[:planes], planes, devices, capacity)
        table = receive_table(both_all[:, :planes], planes, capacity, me)
        arrived = lax.all_to_all(pack_fine(send, fine), "dev", split_axis=0, concat_axis=0, tiled=True)
        interp = refine(coarse_table[None], coarse_in, weights)
        u = assemble(table, arrived, interp)
        u = advance(diffusion, u, *rims(u), velocity)
        return (u,) + rims(u)

    if relaying:
        choices = [capacity * k // 16 for k in CROSS]
        sizes = tuple(capacity * k // 16 for k in FINE) + tuple(coarse_capacity * k // 8 for k in COARSE)
        sizes = sizes[:5] + (1,) + sizes[5:]
        rows = group_count * devices
        flat = groups.reshape(rows, -1)
        place = jnp.stack([lax.axis_index("grp"), me]).astype(jnp.int32)
        tables = plan(
            place, flat[:, :planes], flat[:, planes:], group_count, devices, planes,
            coarse_planes, sizes, choices, capacity * LOOSE // 16,
        )

        def relayed(count, ident, fine, coarse):
            return regrid(
                count, (sizes[0] + (count >= capacity * LOOSE // 16),) + sizes[1:], ident, devices, tables, diffusion, fine, coarse, weights, velocity
            )

        branches = [
            functools.partial(relayed, count, 1 + k) for k, count in enumerate(choices)
        ]
        state = lax.switch(tables[6, 0], branches + [padded], old_fine, old_coarse)
    else:
        state = padded(old_fine, old_coarse)
    return advance(diffusion, *state, velocity)


def solution(mesh):
    in_specs = (
        P("dev", None, "grp", None),
        P("grp", "dev"),
        P("dev", None, "grp", None),
        P("grp", "dev"),
        P("dev", None, "grp", None),
        P(),
    )
    out_specs = P("dev", None, "grp", None)
    return jax.shard_map(
        on_device, mesh=mesh, in_specs=in_specs, out_specs=out_specs, check_vma=False
    )
```
